32 devices in a mesh: zm: 8 (over y, x, core), zv: 4 (over z).
Axes of the slice: x: 2, y: 2, z: 4, core: 2. Of those that a mesh axis runs over, the one named last changes fastest.
Arguments:
- table: float32 [128, 256, 256], P('zm', 'zv'), may hold values from -6 to 6
- refined: float32 [4, 256, 16, 1024], P(None, ('zm', 'zv')), may hold values from -18 to 18
- assign: int32 [4, 32, 8], replicated, may hold values from -1 to 511, as said below
Outputs:
- table_out: float32 [128, 256, 256], P('zm', 'zv')
- block_error: float32 [4, 512], P(None, ('zm', 'zv'))
- worst: float32 [4], replicated
The draws below stay inside these ranges and needn't reach their ends.
Inputs may be any that keep to these rules, and one draw needn't show every extreme that they name: `assign`: devices are numbered d = zm index * 4 + zv index; block b is homed on device b // 16, and its home device has the same zv index as the owner d of the slot. In an iteration no block appears twice, at most 1 block of one home device sit in the slots of one owner (reached in every iteration), and some owner of every zv index has all 8 slots filled.
All inputs are finite; a program needn't handle non-finite values.
Results may differ from the reference program's by a relative error of at most 0.0001.
Values sent between devices are 32-bit elements; how exact they have to be, the bound alone decides.
No kernel may reach another device: no remote copies, remote signals or barrier semaphores. Data moves between devices by JAX's collectives and lax.ppermute only.
A program may use at most 128 MiB of HBM per device.

```python
import jax
import jax.numpy as jnp
from jax import lax

S = 8
NC = 32
BLOCK_Z = 16
BLOCK_V = 16
BLOCK_C = 8
ITERS = 4
CAP = 1
SLOTS = 8
NZ = 128
NV = 256
BLK_DEV = 16
SLOTS_ALL = 256
N_ZM = 8
N_ZV = 4


def draw_assign(key, part):
    planes = []
    for iteration in range(ITERS):
        step_key = jax.random.fold_in(key, 101 + iteration)
        first_key, second_key, third_key, fourth_key = jax.random.split(step_key, 4)
        home_order = jax.vmap(lambda inner: jax.random.permutation(inner, N_ZM))(jax.random.split(first_key, N_ZV))
        picks = jax.vmap(lambda inner: jax.random.permutation(inner, BLK_DEV))(jax.random.split(second_key, N_ZV * N_ZM))
        picks = picks.reshape(N_ZV, N_ZM, BLK_DEV)
        owner_index = jnp.arange(N_ZM)[:, None, None]
        column_index = jnp.arange(N_ZV)[None, :, None]
        slot_index = jnp.arange(SLOTS)[None, None, :]
        position = (owner_index + slot_index // CAP) % N_ZM
        home_zm = home_order[column_index, position]
        local_id = picks[column_index, home_zm, owner_index * CAP + slot_index % CAP]
        full_owner = jax.random.randint(third_key, (1, N_ZV, 1), 0, N_ZM)
        coins = jax.random.randint(fourth_key, (N_ZM, N_ZV, SLOTS), 0, 2)
        live_mask = (coins == 1) | (owner_index == full_owner)
        block_ids = (home_zm * N_ZV + column_index) * BLK_DEV + local_id
        planes.append(jnp.where(live_mask, block_ids, -1).reshape(N_ZM * N_ZV, SLOTS))
    return jnp.stack(planes).astype(jnp.int32)


def draw_refined(key, part):
    shape_all = (ITERS, SLOTS_ALL, BLOCK_Z, BLOCK_V * BLOCK_C * S)
    inner_key = jax.random.fold_in(key, 7)
    base = jnp.clip(jax.random.normal(inner_key, shape_all, jnp.float32), -6.0, 6.0)
    owner_zm = jnp.arange(SLOTS_ALL) // SLOTS // N_ZV
    scale = 1.0 + 2.0 * owner_zm.astype(jnp.float32) / max(N_ZM - 1, 1)
    return base * scale[None, :, None, None]


def level_of(stream_key, dims, pieces, low, largest):
    loudness, own = 1.0, jax.random.fold_in(stream_key, 6)
    for dim, blocks in pieces:
        steps = jnp.exp(jax.random.uniform(jax.random.fold_in(own, dim), (blocks,), jnp.float32, low / len(pieces), largest / len(pieces)))
        loudness = loudness * jnp.repeat(steps, dims[dim] // blocks).reshape([-1 if axis == dim else 1 for axis in range(len(dims))])
    return loudness


def normal_values(key, extent, scale, limit, shards=(), held_as=jnp.bfloat16):
    values = scale * jax.random.normal(key, extent, jnp.float32)
    if shards:
        values = values * level_of(key, extent, shards, -0.22, 0.18)
    return jnp.clip(values, -limit, limit).astype(held_as)


def setup_inputs(seed: int = 0) -> dict:
    keys = jax.random.split(jax.random.key(seed), 4)
    return {
        "table": normal_values(keys[0], (NZ, NV, NC * S), 1.0, 6.0, ((0, 8), (1, 4)), jnp.float32),
        "refined": draw_refined(jax.random.fold_in(keys[3], 71), 0),
        "assign": draw_assign(jax.random.fold_in(keys[3], 71), 0),
    }


def corner_mean(corner_grid):
    summed = corner_grid[:-1, :-1, :-1] + corner_grid[1:, :-1, :-1] + corner_grid[:-1, 1:, :-1] + corner_grid[1:, 1:, :-1]
    summed = summed + corner_grid[:-1, :-1, 1:] + corner_grid[1:, :-1, 1:] + corner_grid[:-1, 1:, 1:] + corner_grid[1:, 1:, 1:]
    return summed * 0.125

def to_blocks(centre):
    size_z, size_v, size_c, size_s = centre.shape
    parts = centre.reshape(size_z // BLOCK_Z, BLOCK_Z, size_v // BLOCK_V, BLOCK_V, size_c // BLOCK_C, BLOCK_C, size_s)
    return parts.transpose(0, 2, 4, 1, 3, 5, 6).reshape(-1, BLOCK_Z * BLOCK_V * BLOCK_C * size_s)

def from_blocks(flat, size_z, size_v, size_c):
    parts = flat.reshape(size_z // BLOCK_Z, size_v // BLOCK_V, size_c // BLOCK_C, BLOCK_Z, BLOCK_V, BLOCK_C, S)
    return parts.transpose(0, 3, 1, 4, 2, 5, 6).reshape(size_z, size_v, size_c * S)

def reference(table, refined, assign):
    size_z, size_v, table_wide = table.shape
    size_c = table_wide // S
    block_cells = BLOCK_Z * BLOCK_V * BLOCK_C * S
    worst_list = []
    error_list = []
    for iteration in range(ITERS):
        corner_grid = table.reshape(size_z, size_v, size_c, S)
        corner_grid = jnp.concatenate([corner_grid, corner_grid[-1:]], 0)
        corner_grid = jnp.concatenate([corner_grid, corner_grid[:, -1:]], 1)
        corner_grid = jnp.concatenate([corner_grid, corner_grid[:, :, -1:]], 2)
        blocks = to_blocks(corner_mean(corner_grid))
        block_ids = assign[iteration].reshape(-1).astype(jnp.int32)
        live_mask = block_ids >= 0
        safe_ids = jnp.where(live_mask, block_ids, 0).astype(jnp.int32)
        target = refined[iteration].reshape(-1, block_cells)
        residual = jnp.where(live_mask[:, None], target - blocks[safe_ids], jnp.float32(0.0))
        total_sq = jnp.sum(residual * residual)
        cell_count = jnp.sum(live_mask.astype(jnp.float32)) * block_cells
        weight = 1.0 / (1.0 + jnp.sqrt(total_sq / cell_count))
        peak_error = lax.optimization_barrier(jnp.max(jnp.abs(residual), axis=1))
        worst_list.append(jnp.max(peak_error))
        errors = jnp.zeros((blocks.shape[0],), jnp.float32).at[safe_ids].max(jnp.where(live_mask, peak_error, jnp.float32(0.0)))
        error_list.append(errors)
        change = jnp.zeros_like(blocks).at[safe_ids].add(weight * residual)
        table = table + from_blocks(change, size_z, size_v, size_c)
    return (table, jnp.stack(error_list), jnp.stack(worst_list))
```

```python
import jax
import jax.numpy as jnp
from jax import lax
from jax.sharding import PartitionSpec as P

S = 8
BLOCK_Z = 16
BLOCK_V = 16
BLOCK_C = 8
ITERS = 4
CAP = 1


precise = lax.Precision.HIGHEST


def shifted(value, axis, steps):
    count = lax.axis_size(axis)
    first, last = (max(0, -steps), min(count, count - steps))
    return lax.ppermute(value, axis, [(source, source + steps) for source in range(first, last)])


def corner_mean(corner_grid):
    summed = (
        corner_grid[:-1, :-1, :-1]
        + corner_grid[1:, :-1, :-1]
        + corner_grid[:-1, 1:, :-1]
        + corner_grid[1:, 1:, :-1]
    )
    summed = (
        summed
        + corner_grid[:-1, :-1, 1:]
        + corner_grid[1:, :-1, 1:]
        + corner_grid[:-1, 1:, 1:]
        + corner_grid[1:, 1:, 1:]
    )
    return summed * 0.125


def global_stats(total_sq, biggest):
    devices = lax.axis_size("zm") * lax.axis_size("zv")
    lane = lax.broadcasted_iota(jnp.int32, (devices, 1, 128), 2)
    mine = jnp.where(lane == 0, total_sq, jnp.where(lane == 1, biggest, 0.0))
    parts = lax.all_to_all(mine, ("zm", "zv"), split_axis=0, concat_axis=0, tiled=True)
    return (jnp.sum(parts[:, 0, 0]), jnp.max(parts[:, 0, 1]))


def shards(table, refined, assign):
    zm_count = lax.axis_size("zm")
    zv_count = lax.axis_size("zv")
    zm_here = lax.axis_index("zm")
    zv_here = lax.axis_index("zv")
    table_depth, table_span, table_wide = table.shape
    channels = table_wide // S
    vary_blocks = table_span // BLOCK_V
    prog_blocks = channels // BLOCK_C
    block_count = vary_blocks * prog_blocks
    block_cells = BLOCK_Z * BLOCK_V * BLOCK_C * S
    slot_total = assign.shape[2]
    device_here = zm_here * zv_count + zv_here
    lane_index = jnp.arange(CAP)
    spot_index = jnp.arange(block_count)
    home_index = jnp.arange(zm_count)
    slot_index = jnp.arange(slot_total)
    worst_list = []
    error_list = []
    for iteration in range(ITERS):
        above_row = shifted(table[:1], "zm", -1)
        above_row = jnp.where(zm_here == zm_count - 1, table[-1:], above_row)
        grown = jnp.concatenate([table, above_row], 0)
        beside = shifted(grown[:, :1], "zv", -1)
        beside = jnp.where(zv_here == zv_count - 1, grown[:, -1:], beside)
        grown = jnp.concatenate([grown, beside], 1)
        corner_grid = grown.reshape(table_depth + 1, table_span + 1, channels, S)
        corner_grid = jnp.concatenate([corner_grid, corner_grid[:, :, -1:]], 2)
        centre = corner_mean(corner_grid)
        view = centre.reshape(BLOCK_Z, vary_blocks, BLOCK_V, prog_blocks, BLOCK_C * S)
        slot_plan = assign[iteration].reshape(zm_count, zv_count, slot_total)
        column = lax.dynamic_index_in_dim(slot_plan, zv_here, 1, False)
        mine_mask = (column >= 0) & (column // block_count == device_here)
        placed = jnp.cumsum(mine_mask.astype(jnp.int32), axis=1) - 1
        local_id = column - device_here * block_count
        pick_place = (mine_mask[:, :, None] & (placed[:, :, None] == lane_index)).astype(
            jnp.float32
        )
        pick_local = (local_id[:, :, None] == spot_index).astype(jnp.float32)
        selector = jnp.einsum("oks,okl->osl", pick_place, pick_local, precision=precise)
        filled = jnp.sum(selector, axis=2) > 0.5
        slot_block = (
            jnp.sum(selector * spot_index.astype(jnp.float32), axis=2).astype(jnp.int32).reshape(-1)
        )
        vary_of = slot_block // prog_blocks
        prog_of = slot_block % prog_blocks
        picked = view[:, vary_of, :, prog_of, :]
        local_blocks = picked.reshape(zm_count, CAP, block_cells)
        wanted = lax.dynamic_index_in_dim(column, zm_here, 0, False)
        live_mask = wanted >= 0
        source = wanted // block_count // zv_count
        earlier = (
            (source[:, None] == source[None, :])
            & live_mask[None, :]
            & (slot_index[None, :] < slot_index[:, None])
        )
        rank_slot = jnp.sum(earlier.astype(jnp.int32), axis=1)
        routing = (
            live_mask[:, None, None]
            & (source[:, None, None] == home_index[None, :, None])
            & (rank_slot[:, None, None] == lane_index)
        ).astype(jnp.float32)
        target = refined[iteration].reshape(slot_total, block_cells)
        cell_count = jnp.sum((slot_plan >= 0).astype(jnp.float32)) * block_cells
        packed = jnp.einsum("khp,kx->hpx", routing, target, precision=precise)
        arrived = lax.all_to_all(packed, "zm", split_axis=0, concat_axis=0, tiled=True)
        residual = jnp.where(filled[:, :, None], arrived - local_blocks, jnp.float32(0.0))
        peak_error = jnp.max(jnp.abs(residual), axis=2)
        total_sq, biggest = global_stats(jnp.sum(residual * residual), jnp.max(peak_error))
        weight = 1.0 / (1.0 + jnp.sqrt(total_sq / cell_count))
        slot_change = weight * residual
        errors = jnp.einsum("opl,op->l", selector, peak_error, precision=precise)
        rows_back = slot_change.reshape(zm_count * CAP, BLOCK_Z, BLOCK_V, BLOCK_C * S)
        change_view = jnp.zeros_like(view).at[:, vary_of, :, prog_of, :].add(rows_back)
        table = table + change_view.reshape(table_depth, table_span, table_wide)
        worst_list.append(biggest)
        error_list.append(errors)
    return (table, jnp.stack(error_list), jnp.stack(worst_list))


def solution(mesh):
    in_specs = (P("zm", "zv", None), P(None, ("zm", "zv"), None, None), P())
    out_specs = (P("zm", "zv", None), P(None, ("zm", "zv")), P())
    return jax.shard_map(shards, mesh=mesh, in_specs=in_specs, out_specs=out_specs, check_vma=False)
```

```python
import functools

import jax
import jax.numpy as jnp
from jax import lax
from jax.experimental import pallas as pl
from jax.experimental.pallas import tpu as pltpu
from jax.sharding import PartitionSpec as P

S = 8
BLOCK_Z = 16
BLOCK_V = 16
BLOCK_C = 8
ITERS = 4
HALF = BLOCK_C * S
PAIRS = BLOCK_V // 2
LANES = 2 * HALF
ROWS = BLOCK_Z * PAIRS
DEEP = BLOCK_Z + ITERS
AXES = ("zm", "zv")
F32 = jnp.float32


def halo_rows(iteration):
    return ITERS - 1 - iteration


def lane_ids():
    return lax.broadcasted_iota(jnp.int32, (PAIRS, LANES), 1)


def sub_ids():
    return lax.broadcasted_iota(jnp.int32, (PAIRS, LANES), 0)


VMEM = pl.BlockSpec(memory_space=pltpu.VMEM)
SMEM = pl.BlockSpec(memory_space=pltpu.SMEM)
ANY = pl.BlockSpec(memory_space=pl.ANY)


def call(body, outs, specs, scratch=(), flops=1000, name=None, limit=24 << 20):
    return pl.pallas_call(
        body,
        out_shape=outs,
        in_specs=specs,
        out_specs=[VMEM] * len(outs),
        scratch_shapes=list(scratch),
        name=name,
        compiler_params=pltpu.CompilerParams(vmem_limit_bytes=limit),
        cost_estimate=pl.CostEstimate(flops=flops, bytes_accessed=1 << 20, transcendentals=0),
    )


def struct(*shape):
    return jax.ShapeDtypeStruct(shape, F32)


class Shape:
    def __init__(self, table, assign, zm_count, zv_count):
        self.zm, self.zv = zm_count, zv_count
        self.span, self.wide = table[1], table[2]
        self.vb = self.span // BLOCK_V
        self.cb = self.wide // HALF
        self.blocks = self.vb * self.cb
        self.fields = self.blocks + 1
        self.slots = assign[2]
        self.cells = BLOCK_Z * BLOCK_V * BLOCK_C * S


def pack_body(g, iteration, assign, refined, out):
    extra = halo_rows(iteration) * PAIRS
    me = lax.axis_index("zm") * g.zv + lax.axis_index("zv")
    for slot in range(g.slots):
        block = assign[iteration, me * g.slots + slot]

        @pl.when(block >= 0)
        def _():
            home = block // (g.blocks * g.zv)
            for zt in range(BLOCK_Z // 8):
                for pair in range(PAIRS):
                    tile = refined[0, slot, zt * 8 : zt * 8 + 8, pair * LANES : (pair + 1) * LANES]
                    out[home, pl.ds(zt * 8 * PAIRS + pair, 8, stride=PAIRS), :] = tile
            if extra:

                @pl.when(home > 0)
                def _():
                    out[jnp.maximum(home - 1, 0), ROWS : ROWS + extra, :] = out[home, 0:extra, :]


def pack(g, iteration, assign, refined):
    rows = ROWS + halo_rows(iteration) * PAIRS
    size = (1,) + refined.shape[1:]
    return pl.pallas_call(
        functools.partial(pack_body, g, iteration),
        grid=(1,),
        out_shape=struct(g.zm, rows, LANES),
        in_specs=[SMEM, pl.BlockSpec(size, lambda i: (iteration, 0, 0, 0))],
        out_specs=pl.BlockSpec((g.zm, rows, LANES), lambda i: (0, 0, 0)),
        name=f"pack{iteration}",
        compiler_params=pltpu.CompilerParams(vmem_limit_bytes=16 << 20),
        cost_estimate=pl.CostEstimate(flops=1000, bytes_accessed=1 << 20, transcendentals=0),
    )(assign, refined)


def to_blocks_body(g, table, below, out, planes):
    left = lane_ids() < HALF

    def put(source, z, target):
        for col in range(g.wide // LANES):
            planes[col] = source[z, :, col * LANES : (col + 1) * LANES]
        for vb in range(g.vb):
            for col in range(g.wide // LANES):
                even = planes[col, pl.ds(vb * BLOCK_V, PAIRS, stride=2), :]
                odd = planes[col, pl.ds(vb * BLOCK_V + 1, PAIRS, stride=2), :]
                first = jnp.where(left, even, pltpu.roll(odd, HALF, 1))
                second = jnp.where(left, pltpu.roll(even, HALF, 1), odd)
                out[vb * g.cb + 2 * col, target] = first
                out[vb * g.cb + 2 * col + 1, target] = second

    @pl.loop(0, BLOCK_Z)
    def _(z):
        put(table, z, z)

    @pl.loop(0, ITERS)
    def _(z):
        put(below, z, BLOCK_Z + z)


def strip_rows(g, get, z):
    sub = sub_ids()
    whole = get(0, z)
    for c in range(1, g.cb):
        whole = jnp.where(sub // 2 == c, pltpu.roll(get(c, z), 2 * c, 0), whole)
    return whole


def owner_of(meta, iteration, z, block, far):
    return meta[iteration, block + jnp.where(z >= BLOCK_Z, far, 0)]


def arrived_tile(g, meta, data, iteration, block, z):
    owner = owner_of(meta, iteration, z, block, g.blocks)
    return data[jnp.maximum(owner, 0), pl.ds(pl.multiple_of(z * PAIRS, PAIRS), PAIRS), :], owner >= 0


def strip_body(g, iteration, with_table, meta, data, *rest):
    out = rest[-1]
    depth = BLOCK_Z + halo_rows(iteration)

    @pl.loop(0, depth)
    def _(z):
        out[z] = strip_rows(g, lambda c, z: arrived_tile(g, meta, data, iteration, c, z)[0], z)

    if with_table:
        nodes = rest[0]

        @pl.loop(0, DEEP)
        def _(z):
            out[depth + z] = strip_rows(g, lambda c, z: nodes[c, z], z)


def stencil(g, get, z, low, edge):
    lane, sub = lane_ids(), sub_ids()
    inner = lane % HALF < HALF - S
    left = lane < HALF
    first = sub == 0
    last = edge & (sub == PAIRS - 1) & (lane >= HALF)
    halo = get(g.blocks, z) + get(g.blocks, low)
    beside = jnp.where(sub >= 2 * (g.cb - 1), halo, pltpu.roll(pltpu.roll(halo, PAIRS - 2, 0), HALF - S, 1))
    halo = halo + jnp.where(inner, pltpu.roll(halo, LANES - S, 1), beside)
    turned = pltpu.roll(halo, HALF, 1)
    result = {g.blocks: 0.125 * (halo + jnp.where(left, turned, pltpu.roll(turned, PAIRS - 1, 0)))}
    after = [pltpu.roll(turned, (PAIRS - 2 * c) % PAIRS, 0) if c else turned for c in range(g.cb)]
    for vb in reversed(range(g.vb)):
        beside = None
        for c in reversed(range(g.cb)):
            block = vb * g.cb + c
            layer = get(block, z) + get(block, low)
            if beside is None:
                shifted = jnp.where(inner, pltpu.roll(layer, LANES - S, 1), layer)
            else:
                shifted = jnp.where(inner, pltpu.roll(layer, LANES - S, 1), pltpu.roll(beside, HALF - S, 1))
            beside = layer
            both = layer + shifted
            turned = pltpu.roll(both, HALF, 1)
            up = pltpu.roll(jnp.where(first, after[c], turned), PAIRS - 1, 0)
            up = jnp.where(left, turned, up)
            if vb == g.vb - 1:
                up = jnp.where(last, both, up)
            result[block] = 0.125 * (both + up)
            after[c] = turned
    return result


def edges(meta):
    return meta[0, 120] == 1, meta[0, 121] == 1


def layer_below(z, edge):
    return jnp.where((z == BLOCK_Z - 1) & edge, z, z + 1)


def halo_live(g, meta, iteration, z):
    sub = sub_ids()
    owner = jnp.zeros((PAIRS, LANES), jnp.int32) - 1
    for c in range(g.cb):
        one = meta[iteration, 2 * g.blocks + c + jnp.where(z >= BLOCK_Z, g.cb, 0)]
        owner = jnp.where(sub // 2 == c, one, owner)
    return owner >= 0


def first_body(g, meta, data, nodes, strip, interp, res, res_interp):
    edge_z, edge_v = edges(meta)
    depth = BLOCK_Z + halo_rows(0)

    def get(block, z):
        return strip[depth + z] if block == g.blocks else nodes[block, z]

    @pl.loop(0, depth)
    def _(z):
        mean = stencil(g, get, z, layer_below(z, edge_z), edge_v)
        for block in range(g.blocks):
            tile, live = arrived_tile(g, meta, data, 0, block, z)
            interp[block, z] = mean[block]
            res[block, z] = jnp.where(live, tile - mean[block], 0.0)
        interp[g.blocks, z] = mean[g.blocks]
        res[g.blocks, z] = jnp.where(halo_live(g, meta, 0, z), strip[z] - mean[g.blocks], 0.0)

    @pl.loop(0, depth - 1)
    def _(z):
        mean = stencil(g, lambda b, z: res[b, z], z, layer_below(z, edge_z), edge_v)
        for block in range(g.fields):
            res_interp[block, z] = mean[block]


def second_body(g, meta, data, strip, interp, res_interp, a_out, b_out, a_interp, b_interp):
    edge_z, edge_v = edges(meta)
    depth = BLOCK_Z + halo_rows(1)

    @pl.loop(0, depth)
    def _(z):
        for block in range(g.blocks):
            tile, live = arrived_tile(g, meta, data, 1, block, z)
            a_out[block, z] = jnp.where(live, tile - interp[block, z], 0.0)
            b_out[block, z] = jnp.where(live, res_interp[block, z], 0.0)
        live = halo_live(g, meta, 1, z)
        a_out[g.blocks, z] = jnp.where(live, strip[z] - interp[g.blocks, z], 0.0)
        b_out[g.blocks, z] = jnp.where(live, res_interp[g.blocks, z], 0.0)

    @pl.loop(0, depth - 1)
    def _(z):
        low = layer_below(z, edge_z)
        mean = stencil(g, lambda b, z: a_out[b, z], z, low, edge_v)
        for block in range(g.fields):
            a_interp[block, z] = mean[block]
        mean = stencil(g, lambda b, z: b_out[b, z], z, low, edge_v)
        for block in range(g.fields):
            b_interp[block, z] = mean[block]


PRODUCTS = 14


def spread_rows(values, count):
    rows = [jnp.sum(value, axis=0, keepdims=True) for value in values]
    rows += [jnp.zeros_like(rows[0])] * (-len(rows) % 8)
    column = jnp.sum(jnp.concatenate(rows, 0), axis=1, keepdims=True)
    lane = lax.broadcasted_iota(jnp.int32, (len(rows), 128), 1)
    row = lax.broadcasted_iota(jnp.int32, (len(rows), 128), 0)
    line = jnp.sum(jnp.where(lane == row, column, 0.0), axis=0, keepdims=True)
    return jnp.broadcast_to(line, (count, 128))


def third_body(g, meta, data, interp, res, res_interp, a_in, b_in, a_interp, b_interp, out, sums):
    sums[...] = jnp.zeros_like(sums)

    @pl.loop(0, g.blocks)
    def _(block):
        @pl.when(meta[0, block] >= 0)
        def _():
            total = jnp.zeros((PAIRS, LANES), F32)
            for z in range(BLOCK_Z):
                value = res[block, z]
                total += value * value
            sums[0] += total

        @pl.when(meta[1, block] >= 0)
        def _():
            totals = [jnp.zeros((PAIRS, LANES), F32)] * 3
            for z in range(BLOCK_Z):
                a, b = a_in[block, z], b_in[block, z]
                totals = [totals[0] + a * a, totals[1] + a * b, totals[2] + b * b]
            for i in range(3):
                sums[1 + i] += totals[i]

        owner = meta[2, block]

        @pl.when(owner >= 0)
        def _():
            totals = [jnp.zeros((PAIRS, LANES), F32)] * 10
            for z in range(BLOCK_Z):
                tile = data[owner, z * PAIRS : (z + 1) * PAIRS, :]
                parts = [tile - interp[block, z], res_interp[block, z], a_interp[block, z], b_interp[block, z]]
                at = 0
                for i in range(4):
                    for j in range(i, 4):
                        totals[at] = totals[at] + parts[i] * parts[j]
                        at += 1
            for i in range(10):
                sums[4 + i] += totals[i]

    out[...] = spread_rows([sums[i] for i in range(PRODUCTS)], out.shape[0])


def weight_of(total, count):
    return 1.0 / (1.0 + jnp.sqrt(jnp.maximum(total, 0.0) / count))


def lane_values(line, count):
    lane = lax.broadcasted_iota(jnp.int32, line.shape, 1)
    return [jnp.sum(jnp.where(lane == i, line, 0.0), axis=1, keepdims=True) for i in range(count)]


def live_cells(g, meta, iteration):
    return jnp.full((1, 1), meta[iteration, 122], jnp.int32).astype(F32) * F32(g.cells)


def three_weights(g, meta, parts):
    q = lane_values(jnp.sum(parts[...], axis=0, keepdims=True), PRODUCTS)
    w0 = weight_of(q[0], live_cells(g, meta, 0))
    w1 = weight_of(q[1] - 2.0 * w0 * q[2] + w0 * w0 * q[3], live_cells(g, meta, 1))
    f = [jnp.ones_like(w0), -w0, -w1, w0 * w1]
    total, at = jnp.zeros_like(w0), 4
    for i in range(4):
        for j in range(i, 4):
            total = total + (1.0 if i == j else 2.0) * f[i] * f[j] * q[at]
            at += 1
    return w0, w1, weight_of(total, live_cells(g, meta, 2))


def fourth_body(g, meta, parts, data2, data3, strip2, nodes, strip0, interp, res, res_interp, a_in, b_in,
                a_interp, b_interp, table_out, last_out, errors, out, grown, peaks):
    edge_z, edge_v = edges(meta)
    w0, w1, w2 = [jnp.broadcast_to(w, (PAIRS, LANES)) for w in three_weights(g, meta, parts)]
    w01 = w0 * w1
    offset = BLOCK_Z + halo_rows(0)

    def grow(z, inside):
        for block in range(g.fields):
            base = interp[block, z] + w0 * res_interp[block, z] + w1 * a_interp[block, z] - w01 * b_interp[block, z]
            if block == g.blocks:
                tile, live, node = strip2[z], halo_live(g, meta, 2, z), strip0[offset + z]
            else:
                tile, live = arrived_tile(g, meta, data2, 2, block, z)
                node = nodes[block, z]
            second = jnp.where(live, tile - base, 0.0)
            zero = res[block, z]
            one = a_in[block, z] - w0 * b_in[block, z]
            grown[block, z] = node + w0 * zero + w1 * one + w2 * second
            if inside and block < g.blocks:
                for i, value in enumerate((zero, one, second)):
                    peaks[i, block] = jnp.maximum(peaks[i, block], jnp.abs(value))

    peaks[...] = jnp.zeros_like(peaks)

    @pl.loop(0, BLOCK_Z)
    def _(z):
        grow(z, True)

    grow(BLOCK_Z, False)

    def step(z, total):
        mean = stencil(g, lambda b, z: grown[b, z], z, layer_below(z, edge_z), edge_v)
        for block in range(g.blocks):
            owner = meta[3, block]
            tile = data3[jnp.maximum(owner, 0), pl.ds(pl.multiple_of(z * PAIRS, PAIRS), PAIRS), :]
            value = jnp.where(owner >= 0, tile - mean[block], 0.0)
            last_out[block, z] = value
            table_out[block, z] = grown[block, z]
            total = total + value * value
            peaks[3, block] = jnp.maximum(peaks[3, block], jnp.abs(value))
        return total

    total = lax.fori_loop(0, BLOCK_Z, step, jnp.zeros((PAIRS, LANES), F32))
    line = spread_rows([total], 1)
    lane = lax.broadcasted_iota(jnp.int32, (1, 128), 1)
    lane_b = lax.broadcasted_iota(jnp.int32, (g.blocks, 128), 1)
    row_b = lax.broadcasted_iota(jnp.int32, (g.blocks, 128), 0)
    for i in range(ITERS):
        rows = [jnp.max(peaks[i, block], axis=0, keepdims=True) for block in range(g.blocks)]
        column = jnp.max(jnp.concatenate(rows, 0), axis=1, keepdims=True)
        errors[i : i + 1, :] = jnp.sum(jnp.where(lane_b == row_b, column, 0.0), axis=0, keepdims=True)
        line = jnp.where(lane == 1 + i, jnp.max(column, axis=0, keepdims=True), line)
    out[...] = jnp.broadcast_to(line, out.shape)


def fifth_body(g, meta, parts, table, last, out, worst, planes):
    left = lane_ids() < HALF
    total = jnp.sum(lane_values(jnp.sum(parts[...], axis=0, keepdims=True), 1)[0], axis=0, keepdims=True)
    w3 = jnp.broadcast_to(weight_of(total, live_cells(g, meta, 3)), (PAIRS, LANES))
    worst[...] = jnp.broadcast_to(jnp.max(parts[...], axis=0, keepdims=True), worst.shape)

    @pl.loop(0, BLOCK_Z)
    def _(z):
        for vb in range(g.vb):
            for col in range(g.wide // LANES):
                block = vb * g.cb + 2 * col
                first = table[block, z] + w3 * last[block, z]
                second = table[block + 1, z] + w3 * last[block + 1, z]
                even = jnp.where(left, first, pltpu.roll(second, HALF, 1))
                odd = jnp.where(left, pltpu.roll(first, HALF, 1), second)
                planes[col, pl.ds(vb * BLOCK_V, PAIRS, stride=2), :] = even
                planes[col, pl.ds(vb * BLOCK_V + 1, PAIRS, stride=2), :] = odd
        for col in range(g.wide // LANES):
            out[z, :, col * LANES : (col + 1) * LANES] = planes[col]


def index_table(g, assign):
    zm_here, zv_here = lax.axis_index("zm"), lax.axis_index("zv")
    me = zm_here * g.zv + zv_here
    slots = assign.reshape(ITERS, -1)
    owner = jnp.arange(slots.shape[1]) // g.slots // g.zv
    column = jnp.arange(2 * g.blocks + 2 * g.cb)
    here = column % g.blocks
    far = jnp.where(column < 2 * g.blocks, column // g.blocks, (column - 2 * g.blocks) // g.cb)
    local = jnp.where(column < 2 * g.blocks, here, (column - 2 * g.blocks) % g.cb)
    side = jnp.where(column < 2 * g.blocks, 0, 1)
    inside = (zm_here + far < g.zm) & (zv_here + side < g.zv)
    target = jnp.where(inside, (me + far * g.zv + side) * g.blocks + local, -2)
    found = jnp.max(jnp.where(slots[:, None, :] == target[None, :, None], owner[None, None, :], -1), axis=2)
    count = jnp.sum((slots >= 0).astype(jnp.int32), axis=1, keepdims=True)
    flags = jnp.stack([zm_here == g.zm - 1, zv_here == g.zv - 1]).astype(jnp.int32)
    gap = jnp.zeros((ITERS, 120 - found.shape[1]), jnp.int32)
    flags = jnp.broadcast_to(flags[None, :], (ITERS, 2))
    return jnp.concatenate([found, gap, flags, count, jnp.zeros((ITERS, 5), jnp.int32)], axis=1)


def to_all(rows):
    count = lax.axis_size("zm") * lax.axis_size("zv")
    return lax.all_to_all(rows.reshape(count, 1, 128), AXES, 0, 0, tiled=True).reshape(count, 128)


def from_next(value, axis):
    count = lax.axis_size(axis)
    return lax.ppermute(value, axis, [(i, i - 1) for i in range(1, count)])


def shards(table, refined, assign):
    g = Shape(table.shape, assign.shape, lax.axis_size("zm"), lax.axis_size("zv"))
    everyone = g.zm * g.zv
    slots = assign.reshape(ITERS, -1)
    below = from_next(table[:ITERS], "zm")
    data = []
    for i in range(ITERS):
        data.append(lax.all_to_all(pack(g, i, slots, refined), "zm", 0, 0, tiled=True))
    meta = index_table(g, assign)
    tile = (PAIRS, LANES)
    layers = [BLOCK_Z + halo_rows(i) for i in range(ITERS)]

    nodes = call(
        functools.partial(to_blocks_body, g), [struct(g.blocks, DEEP, *tile)], [VMEM] * 2,
        [pltpu.VMEM((g.wide // LANES, g.span, LANES), F32)], name="to_blocks",
    )(table, below)[0]
    strips = []
    for i in range(ITERS - 1):
        more = [nodes] if i == 0 else []
        depth = layers[i] + (DEEP if i == 0 else 0)
        made = call(
            functools.partial(strip_body, g, i, i == 0), [struct(depth, *tile)],
            [SMEM] + [VMEM] * (1 + len(more)), name=f"strip{i}",
        )(meta, data[i], *more)[0]
        strips.append(from_next(made, "zv"))
    interp, res, res_interp = call(
        functools.partial(first_body, g),
        [struct(g.fields, layers[0], *tile), struct(g.fields, layers[0], *tile), struct(g.fields, layers[1], *tile)],
        [SMEM] + [VMEM] * 3, name="first",
    )(meta, data[0], nodes, strips[0])
    a_res, b_res, a_interp, b_interp = call(
        functools.partial(second_body, g),
        [struct(g.fields, layers[1], *tile)] * 2 + [struct(g.fields, layers[2], *tile)] * 2,
        [SMEM] + [VMEM] * 4, name="second",
    )(meta, data[1], strips[1], interp, res_interp)
    products = call(
        functools.partial(third_body, g), [struct(everyone, 128)], [SMEM] + [VMEM] * 8,
        [pltpu.VMEM((PRODUCTS,) + tile, F32)], name="third",
    )(meta, data[2], interp, res, res_interp, a_res, b_res, a_interp, b_interp)[0]
    products = to_all(products)
    grown, last, errors, stats = call(
        functools.partial(fourth_body, g),
        [struct(g.blocks, BLOCK_Z, *tile)] * 2 + [struct(ITERS, 128), struct(everyone, 128)],
        [SMEM] + [VMEM] * 13,
        [pltpu.VMEM((g.fields, layers[2], *tile), F32), pltpu.VMEM((ITERS, g.blocks, *tile), F32)], name="fourth",
    )(meta, products, data[2], data[3], strips[2], nodes, strips[0], interp, res, res_interp, a_res, b_res,
      a_interp, b_interp)
    stats = to_all(stats)
    table_out, worst = call(
        functools.partial(fifth_body, g), [struct(*table.shape), struct(8, 128)], [SMEM] + [VMEM] * 3,
        [pltpu.VMEM((g.wide // LANES, g.span, LANES), F32)], name="fifth",
    )(meta, stats, grown, last)
    return (table_out, errors[:, : g.blocks], worst[0, 1 : 1 + ITERS])


def solution(mesh):
    in_specs = (P("zm", "zv", None), P(None, ("zm", "zv"), None, None), P())
    out_specs = (P("zm", "zv", None), P(None, ("zm", "zv")), P())
    return jax.shard_map(shards, mesh=mesh, in_specs=in_specs, out_specs=out_specs, check_vma=False)
```

```python
import functools

import jax
import jax.numpy as jnp
from jax import lax
from jax.experimental import pallas as pl
from jax.experimental.pallas import tpu as pltpu
from jax.sharding import PartitionSpec as P


S = 8
BLOCK_Z = 16
BLOCK_V = 16
BLOCK_C = 8
ITERS = 4
HALF = BLOCK_C * S
PAIRS = BLOCK_V // 2
LANES = 2 * HALF
ROWS = BLOCK_Z * PAIRS
DEEP = BLOCK_Z + ITERS
AXES = ("zm", "zv")
F32 = jnp.float32
TILE = (PAIRS, LANES)


def halo_rows(iteration):
    return ITERS - 1 - iteration


LAYERS = [BLOCK_Z + halo_rows(i) for i in range(ITERS)]
OFFSET = [sum(LAYERS[:i]) * PAIRS for i in range(ITERS)]


def lane_ids():
    return lax.broadcasted_iota(jnp.int32, TILE, 1)


def sub_ids():
    return lax.broadcasted_iota(jnp.int32, TILE, 0)


VMEM = pl.BlockSpec(memory_space=pltpu.VMEM)
SMEM = pl.BlockSpec(memory_space=pltpu.SMEM)
HBM = pl.BlockSpec(memory_space=pltpu.HBM)


def call(body, outs, in_specs, out_specs, scratch, name, flops=200000, limit=24):
    return pl.pallas_call(
        body,
        out_shape=outs,
        in_specs=in_specs,
        out_specs=out_specs,
        scratch_shapes=list(scratch),
        name=name,
        compiler_params=pltpu.CompilerParams(vmem_limit_bytes=limit << 20),
        cost_estimate=pl.CostEstimate(flops=flops, bytes_accessed=1 << 20, transcendentals=0),
    )


def struct(*shape, dtype=F32):
    return jax.ShapeDtypeStruct(shape, dtype)


def dma(count):
    return pltpu.SemaphoreType.DMA((count,))


class Shape:
    def __init__(self, table, assign, zm_count, zv_count):
        self.zm, self.zv = zm_count, zv_count
        self.span, self.wide = table[1], table[2]
        self.vb = self.span // BLOCK_V
        self.cb = self.wide // HALF
        self.blocks = self.vb * self.cb
        self.slots = assign[2]
        self.cells = BLOCK_Z * BLOCK_V * BLOCK_C * S


def fill_inverse(g, iterations, assign, inverse):
    me = lax.axis_index("zm") * g.zv + lax.axis_index("zv")
    for t in iterations:
        for peer in range(g.zm):
            inverse[t, peer] = 0
        for slot in range(g.slots):
            block = assign[t * g.slots + slot, me]

            @pl.when(block >= 0)
            def _():
                inverse[t, block // (g.blocks * g.zv)] = slot


def pack_three_body(g, assign, refined, out, inverse, sems):
    three = range(ITERS - 1)
    fill_inverse(g, three, assign, inverse)

    def copy(t, peer):
        source = refined.at[t * g.slots + inverse[t, peer]]
        return pltpu.make_async_copy(source, out.at[peer, OFFSET[t] : OFFSET[t] + ROWS, :], sems.at[t * g.zm + peer])

    for t in three:
        for peer in range(g.zm):
            copy(t, peer).start()
    for t in three:
        for peer in range(g.zm):
            copy(t, peer).wait()
        for peer in range(g.zm):
            after = min(peer + 1, g.zm - 1)
            for z in range(halo_rows(t)):
                at = OFFSET[t] + ROWS + z * PAIRS
                out[peer, at : at + PAIRS, :] = out[after, pl.ds(OFFSET[t] + z, PAIRS, stride=8), :]


def pack_last_body(g, assign, refined, *rest):
    outs, inverse, sems = rest[: g.zm], rest[-2], rest[-1]
    t = ITERS - 1
    fill_inverse(g, [t], assign, inverse)
    here = lax.axis_index("zm")
    copies = []
    for k in range(g.zm):
        source = refined.at[t * g.slots + inverse[t, here ^ k]]
        copies.append(pltpu.make_async_copy(source, outs[k], sems.at[k]))
    for copy in copies:
        copy.start()
    for copy in copies:
        copy.wait()


def to_blocks_body(g, table, below, out, strip, planes):
    left = lane_ids() < HALF

    def put(source, z, target):
        for col in range(g.wide // LANES):
            planes[col] = source[z, :, col * LANES : (col + 1) * LANES]
        for vb in range(g.vb):
            for col in range(g.wide // LANES):
                even = planes[col, pl.ds(vb * BLOCK_V, PAIRS, stride=2), :]
                odd = planes[col, pl.ds(vb * BLOCK_V + 1, PAIRS, stride=2), :]
                out[target, vb * g.cb + 2 * col] = jnp.where(left, even, pltpu.roll(odd, HALF, 1))
                out[target, vb * g.cb + 2 * col + 1] = jnp.where(left, pltpu.roll(even, HALF, 1), odd)
        strip[target] = strip_rows(g, [out[target, c] for c in range(g.cb)])

    @pl.loop(0, BLOCK_Z)
    def _(z):
        put(table, z, z)

    @pl.loop(0, ITERS)
    def _(z):
        put(below, z, BLOCK_Z + z)


def strip_rows(g, tiles):
    sub = sub_ids()
    whole = tiles[0]
    for c in range(1, g.cb):
        whole = jnp.where(sub // 2 == c, pltpu.roll(tiles[c], 2 * c, 0), whole)
    return whole


def block_row(z):
    return z // 8 * 8 * PAIRS + z % 8


def strip_body(g, meta, data, out, held, sems):
    three = range(ITERS - 1)

    def copies(t, c):
        mine = data.at[jnp.maximum(meta[t, c], 0), OFFSET[t] : OFFSET[t] + ROWS, :]
        far = data.at[jnp.maximum(meta[t, g.blocks + c], 0), OFFSET[t] + ROWS : OFFSET[t] + LAYERS[t] * PAIRS, :]
        at = t * g.cb + c
        return (
            pltpu.make_async_copy(mine, held.at[at, 0:ROWS, :], sems.at[2 * at]),
            pltpu.make_async_copy(far, held.at[at, ROWS : LAYERS[t] * PAIRS, :], sems.at[2 * at + 1]),
        )

    for t in three:
        for c in range(g.cb):
            for copy in copies(t, c):
                copy.start()
    for t in three:
        for c in range(g.cb):
            for copy in copies(t, c):
                copy.wait()
        for z in range(LAYERS[t]):
            tiles = []
            for c in range(g.cb):
                if z < BLOCK_Z:
                    tiles.append(held[t * g.cb + c, pl.ds(block_row(z), PAIRS, stride=8), :])
                else:
                    tiles.append(held[t * g.cb + c, z * PAIRS : (z + 1) * PAIRS, :])
            out[sum(LAYERS[:t]) + z] = strip_rows(g, tiles)


class Stencil:
    def __init__(self, g, edge):
        self.g = g
        lane, sub = lane_ids(), sub_ids()
        self.inner = lane % HALF < HALF - S
        self.left = lane < HALF
        self.first = sub == 0
        self.below = sub >= 2 * (g.cb - 1)
        self.last = edge & (sub == PAIRS - 1) & (lane >= HALF)

    def along_c(self, get, z, low):
        g = self.g
        result = []
        for vb in range(g.vb):
            row = [get(vb * g.cb + c, z) + get(vb * g.cb + c, low) for c in range(g.cb)]
            for c in range(g.cb):
                beside = row[c] if c == g.cb - 1 else pltpu.roll(row[c + 1], HALF - S, 1)
                result.append(row[c] + jnp.where(self.inner, pltpu.roll(row[c], LANES - S, 1), beside))
        halo = get(g.blocks, z) + get(g.blocks, low)
        beside = jnp.where(self.below, halo, pltpu.roll(pltpu.roll(halo, PAIRS - 2, 0), HALF - S, 1))
        result.append(halo + jnp.where(self.inner, pltpu.roll(halo, LANES - S, 1), beside))
        return result

    def along_v(self, sums):
        g = self.g
        turned = [pltpu.roll(value, HALF, 1) for value in sums]
        halo = turned[g.blocks]
        result = []
        for vb in range(g.vb):
            for c in range(g.cb):
                block = vb * g.cb + c
                if vb == g.vb - 1:
                    after = pltpu.roll(halo, PAIRS - 2 * c, 0) if c else halo
                else:
                    after = turned[block + g.cb]
                up = pltpu.roll(jnp.where(self.first, after, turned[block]), PAIRS - 1, 0)
                up = jnp.where(self.left, turned[block], up)
                if vb == g.vb - 1:
                    up = jnp.where(self.last, sums[block], up)
                result.append(0.125 * (sums[block] + up))
        up = jnp.where(self.left, halo, pltpu.roll(halo, PAIRS - 1, 0))
        result.append(0.125 * (sums[g.blocks] + up))
        return result


def edges(meta):
    return meta[0, 120] == 1, meta[0, 121] == 1


def layer_below(z, edge):
    return jnp.where((z == BLOCK_Z - 1) & edge, z, z + 1)


def clip(z, top):
    return jnp.minimum(jnp.maximum(z, 0), top)


def reader(g, main, halo):
    return lambda block, z: halo[z] if block == g.blocks else main[z, block]


def put_all(g, main, halo, z, values):
    for block in range(g.blocks):
        main[z, block] = values[block]
    halo[z] = values[g.blocks]


def halo_live(g, meta, iteration, far):
    sub = sub_ids()
    owner = jnp.zeros(TILE, jnp.int32) - 1
    for c in range(g.cb):
        owner = jnp.where(sub // 2 == c, meta[iteration, 2 * g.blocks + far * g.cb + c], owner)
    return owner >= 0


def interp_body(g, meta, nodes, strip, interp, interp_halo, sums):
    edge_z, edge_v = edges(meta)
    stencil = Stencil(g, edge_v)
    get = reader(g, nodes, strip)
    top = LAYERS[0] - 1

    @pl.loop(0, LAYERS[0] + 1)
    def _(i):
        z = top - i
        before = [sums[jnp.minimum(z + 1, top), b] for b in range(g.blocks + 1)]
        put_all(g, interp, interp_halo, jnp.minimum(z + 1, top), stencil.along_v(before))
        at = jnp.maximum(z, 0)
        for b, value in enumerate(stencil.along_c(get, at, layer_below(at, edge_z))):
            sums[at, b] = value


def local_body(g, meta, data, interp, a0, a1, a2, totals, peaks, held, sems):
    def copy(owner):
        return pltpu.make_async_copy(data.at[owner], held.at[owner], sems.at[owner])

    for owner in range(g.zm):
        copy(owner).start()
    totals[...] = jnp.zeros_like(totals)
    for owner in range(g.zm):
        copy(owner).wait()

    @pl.loop(0, g.blocks)
    def _(block):
        for t, out in ((0, a0), (1, a1), (2, a2)):
            mine, far = meta[t, block], meta[t, g.blocks + block]
            at_mine, at_far = jnp.maximum(mine, 0), jnp.maximum(far, 0)
            total, peak = jnp.zeros(TILE, F32), jnp.zeros(TILE, F32)
            for z in range(LAYERS[t] if t < 2 else BLOCK_Z):
                if z < BLOCK_Z:
                    tile = held[at_mine, pl.ds(OFFSET[t] + block_row(z), PAIRS, stride=8), :]
                    value = jnp.where(mine >= 0, tile - interp[z, block], 0.0)
                    total = total + value * value
                    peak = jnp.maximum(peak, jnp.abs(value))
                else:
                    at = OFFSET[t] + z * PAIRS
                    value = jnp.where(far >= 0, held[at_far, at : at + PAIRS, :] - interp[z, block], 0.0)
                out[z, block] = value
            totals[t] += total
            if t == 0:
                peaks[block] = peak


PRODUCTS = 14


def spread_rows(values, count):
    rows = [jnp.sum(value, axis=0, keepdims=True) for value in values]
    rows += [jnp.zeros_like(rows[0])] * (-len(rows) % 8)
    column = jnp.sum(jnp.concatenate(rows, 0), axis=1, keepdims=True)
    lane = lax.broadcasted_iota(jnp.int32, (len(rows), 128), 1)
    row = lax.broadcasted_iota(jnp.int32, (len(rows), 128), 0)
    line = jnp.sum(jnp.where(lane == row, column, 0.0), axis=0, keepdims=True)
    return jnp.broadcast_to(line, (count, 128))


def products_body(g, meta, strips, interp_halo, a0, a1, a2, totals, out, ca0_out, ca1_out, cb1_out, b1_out, halos_out,
                  a0_halo, a1_halo, b1_halo, b1, ca0, ca1, cb1, halos, sums, sems):
    edge_z, edge_v = edges(meta)
    stencil = Stencil(g, edge_v)
    live0 = [halo_live(g, meta, 0, far) for far in range(2)]
    live1 = [halo_live(g, meta, 1, far) for far in range(2)]
    for z in range(LAYERS[0]):
        a0_halo[z] = jnp.where(live0[z >= BLOCK_Z], strips[z] - interp_halo[z], 0.0)
    for z in range(LAYERS[1]):
        a1_halo[z] = jnp.where(live1[z >= BLOCK_Z], strips[LAYERS[0] + z] - interp_halo[z], 0.0)
    fields = g.blocks + 1
    get0, get1, getb = reader(g, a0, a0_halo), reader(g, a1, a1_halo), reader(g, b1, b1_halo)
    top0, top1 = LAYERS[1] - 1, LAYERS[2] - 1

    def step(i, carry):
        carry = list(carry)
        base = top0 - i
        z = base + 3
        at = clip(z, top1)
        after_a = stencil.along_v([sums[1, at, b] for b in range(fields)])
        after_b = stencil.along_v([sums[2, at, b] for b in range(fields)])
        put_all(g, ca1, halos.at[1], at, after_a)
        put_all(g, cb1, halos.at[2], at, after_b)
        row = jnp.minimum(at, BLOCK_Z - 1)
        counts = (z >= 0) & (z < BLOCK_Z)
        for block in range(g.blocks):
            live = counts & (meta[1, block] >= 0)
            a, b = a1[row, block], jnp.where(live, b1[row, block], 0.0)
            carry[0] = carry[0] + a * b
            carry[1] = carry[1] + b * b
            live = counts & (meta[2, block] >= 0)
            parts = [a2[row, block]] + [
                jnp.where(live, value, 0.0) for value in (ca0[row, block], after_a[block], after_b[block])
            ]
            slot = 2
            for m in range(4):
                for n in range(max(m, 1), 4):
                    carry[slot] = carry[slot] + parts[m] * parts[n]
                    slot += 1
        z = base + 1
        at = clip(z, top0)
        after = stencil.along_v([sums[0, at, b] for b in range(fields)])
        put_all(g, ca0, halos.at[0], at, after)
        far = jnp.where(at >= BLOCK_Z, g.blocks, 0)
        for block in range(g.blocks):
            b1[at, block] = jnp.where(meta[1, far + block] >= 0, after[block], 0.0)
        live = (live1[0] & (at < BLOCK_Z)) | (live1[1] & (at >= BLOCK_Z))
        b1_halo[at] = jnp.where(live, after[g.blocks], 0.0)
        at = clip(base + 2, top1)
        low = layer_below(at, edge_z)
        for b, value in enumerate(stencil.along_c(get1, at, low)):
            sums[1, at, b] = value
        for b, value in enumerate(stencil.along_c(getb, at, low)):
            sums[2, at, b] = value
        at = clip(base, top0)
        for b, value in enumerate(stencil.along_c(get0, at, layer_below(at, edge_z))):
            sums[0, at, b] = value
        return tuple(carry)

    carry = lax.fori_loop(0, LAYERS[1] + 3, step, (jnp.zeros(TILE, F32),) * 11)
    copies = [
        pltpu.make_async_copy(source.at[0 : LAYERS[2]], target, sems.at[i])
        for i, (source, target) in enumerate(((ca0, ca0_out), (ca1, ca1_out), (cb1, cb1_out)))
    ]
    copies.append(pltpu.make_async_copy(b1.at[0:BLOCK_Z], b1_out, sems.at[3]))
    copies.append(pltpu.make_async_copy(halos, halos_out, sems.at[4]))
    for copy in copies:
        copy.start()
    values = [totals[0], totals[1], carry[0], carry[1], totals[2]] + list(carry[2:])
    out[...] = spread_rows(values, out.shape[0])
    for copy in copies:
        copy.wait()


def weight_of(total, count):
    return 1.0 / (1.0 + jnp.sqrt(jnp.maximum(total, 0.0) / count))


def lane_values(line, count):
    lane = lax.broadcasted_iota(jnp.int32, line.shape, 1)
    return [jnp.sum(jnp.where(lane == i, line, 0.0), axis=1, keepdims=True) for i in range(count)]


def live_cells(g, meta, iteration):
    return jnp.full((1, 1), meta[iteration, 122], jnp.int32).astype(F32) * F32(g.cells)


def three_weights(g, meta, parts):
    q = lane_values(jnp.sum(parts[...], axis=0, keepdims=True), PRODUCTS)
    w0 = weight_of(q[0], live_cells(g, meta, 0))
    w1 = weight_of(q[1] - 2.0 * w0 * q[2] + w0 * w0 * q[3], live_cells(g, meta, 1))
    f = [jnp.ones_like(w0), -w0, -w1, w0 * w1]
    total, at = jnp.zeros_like(w0), 4
    for i in range(4):
        for j in range(i, 4):
            total = total + (1.0 if i == j else 2.0) * f[i] * f[j] * q[at]
            at += 1
    return [jnp.broadcast_to(w, TILE) for w in (w0, w1, weight_of(total, live_cells(g, meta, 2)))]


def last_body(g, meta, parts, strips, interp_halo, halos_in, peaks0, data, *rest):
    last_data, rest = rest[: g.zm], rest[g.zm :]
    (interp_in, ca0_in, ca1_in, cb1_in, a1_in, b1_in, r2_out, r3_out, errors, out, weights,
     fields, one_a, one_b, held2, held3, r2, r2_halo, base, sums, peaks, sems) = rest
    depth = LAYERS[2]
    sources = (interp_in, ca0_in, ca1_in, cb1_in)
    copies = []
    for i, source in enumerate(sources):
        copies.append(pltpu.make_async_copy(source.at[0:depth], fields.at[i], sems.at[i]))
    for owner in range(g.zm):
        source = data.at[owner, OFFSET[2] : OFFSET[2] + depth * PAIRS, :]
        copies.append(pltpu.make_async_copy(source, held2.at[owner], sems.at[4 + owner]))
        copies.append(pltpu.make_async_copy(last_data[owner], held3.at[owner], sems.at[4 + g.zm + owner]))
    later = [pltpu.make_async_copy(a1_in.at[0:BLOCK_Z], one_a, sems.at[4 + 2 * g.zm]),
             pltpu.make_async_copy(b1_in, one_b, sems.at[5 + 2 * g.zm])]
    for copy in copies + later:
        copy.start()
    edge_z, edge_v = edges(meta)
    stencil = Stencil(g, edge_v)
    w0, w1, w2 = three_weights(g, meta, parts)
    w01 = w0 * w1
    weights[0], weights[1], weights[2] = w0, w1, w2
    live = [halo_live(g, meta, 2, far) for far in range(2)]
    peaks[...] = jnp.zeros_like(peaks)
    first = sum(LAYERS[:2])
    for z in range(depth):
        value = interp_halo[z] + w0 * halos_in[0, z] + w1 * halos_in[1, z] - w01 * halos_in[2, z]
        r2_halo[z] = jnp.where(live[z >= BLOCK_Z], strips[first + z] - value, 0.0)
    for copy in copies:
        copy.wait()

    @pl.loop(0, g.blocks)
    def _(block):
        mine, far = meta[2, block], meta[2, g.blocks + block]
        at_mine, at_far = jnp.maximum(mine, 0), jnp.maximum(far, 0)
        peak = jnp.zeros(TILE, F32)
        for z in range(depth):
            value = fields[0, z, block] + w0 * fields[1, z, block]
            value = value + w1 * fields[2, z, block] - w01 * fields[3, z, block]
            base[z, block] = value
            if z < BLOCK_Z:
                tile = held2[at_mine, pl.ds(block_row(z), PAIRS, stride=8), :]
                value = jnp.where(mine >= 0, tile - value, 0.0)
                peak = jnp.maximum(peak, jnp.abs(value))
            else:
                value = jnp.where(far >= 0, held2[at_far, z * PAIRS : (z + 1) * PAIRS, :] - value, 0.0)
            r2[z, block] = value
        peaks[1, block] = peak

    get = reader(g, r2, r2_halo)
    fields_count = g.blocks + 1

    def step(i, total):
        base_z = BLOCK_Z - 1 - i
        z = base_z + 1
        at = clip(z, BLOCK_Z - 1)
        after = stencil.along_v([sums[at, b] for b in range(fields_count)])
        counts = (z >= 0) & (z < BLOCK_Z)
        row = at // 8 * 8 * PAIRS + at % 8
        for block in range(g.blocks):
            owner = meta[3, block]
            tile = held3[jnp.maximum(owner, 0), pl.ds(row, PAIRS, stride=8), :]
            value = jnp.where(counts & (owner >= 0), tile - base[at, block] - w2 * after[block], 0.0)
            fields[0, at, block] = value
            total = total + value * value
            peaks[2, block] = jnp.maximum(peaks[2, block], jnp.abs(value))
        at = clip(base_z, BLOCK_Z - 1)
        for b, value in enumerate(stencil.along_c(get, at, layer_below(at, edge_z))):
            sums[at, b] = value
        return total

    total = lax.fori_loop(0, BLOCK_Z + 1, step, jnp.zeros(TILE, F32))
    writes = [pltpu.make_async_copy(r2.at[0:BLOCK_Z], r2_out, sems.at[0]),
              pltpu.make_async_copy(fields.at[0, 0:BLOCK_Z], r3_out, sems.at[1])]
    for copy in later:
        copy.wait()
    for copy in writes:
        copy.start()

    @pl.loop(0, g.blocks)
    def _(block):
        peak = jnp.zeros(TILE, F32)
        for z in range(BLOCK_Z):
            peak = jnp.maximum(peak, jnp.abs(one_a[z, block] - w0 * one_b[z, block]))
        peaks[0, block] = peak

    line = spread_rows([total], 1)
    lane = lax.broadcasted_iota(jnp.int32, (1, 128), 1)
    lane_b = lax.broadcasted_iota(jnp.int32, (g.blocks, 128), 1)
    row_b = lax.broadcasted_iota(jnp.int32, (g.blocks, 128), 0)
    for i in range(ITERS):
        tiles = [peaks0[block] if i == 0 else peaks[i - 1, block] for block in range(g.blocks)]
        rows = [jnp.max(tile, axis=0, keepdims=True) for tile in tiles]
        column = jnp.max(jnp.concatenate(rows, 0), axis=1, keepdims=True)
        errors[i : i + 1, :] = jnp.sum(jnp.where(lane_b == row_b, column, 0.0), axis=0, keepdims=True)
        line = jnp.where(lane == 1 + i, jnp.max(column, axis=0, keepdims=True), line)
    out[...] = jnp.broadcast_to(line, out.shape)
    for copy in writes:
        copy.wait()


def assemble_body(g, table, weights, a0_in, a1_in, b1_in, r2_in, r3_in, grown, last, held, planes, sems):
    left = lane_ids() < HALF
    copies = [
        pltpu.make_async_copy(source.at[0:BLOCK_Z], held.at[i], sems.at[i])
        for i, source in enumerate((a0_in, a1_in, b1_in, r2_in, r3_in))
    ]
    for copy in copies:
        copy.start()
    w0, w1, w2 = weights[0], weights[1], weights[2]
    w01 = w0 * w1
    for copy in copies:
        copy.wait()

    @pl.loop(0, BLOCK_Z)
    def _(z):
        for vb in range(g.vb):
            for col in range(g.wide // LANES):
                pair = []
                for block in (vb * g.cb + 2 * col, vb * g.cb + 2 * col + 1):
                    change = w0 * held[0, z, block] + w1 * held[1, z, block]
                    change = change - w01 * held[2, z, block] + w2 * held[3, z, block]
                    pair.append((change, held[4, z, block]))
                for i in range(2):
                    first, second = pair[0][i], pair[1][i]
                    even = jnp.where(left, first, pltpu.roll(second, HALF, 1))
                    odd = jnp.where(left, pltpu.roll(first, HALF, 1), second)
                    planes[i, col, pl.ds(vb * BLOCK_V, PAIRS, stride=2), :] = even
                    planes[i, col, pl.ds(vb * BLOCK_V + 1, PAIRS, stride=2), :] = odd
        for col in range(g.wide // LANES):
            lanes = slice(col * LANES, (col + 1) * LANES)
            grown[z, :, lanes] = table[z, :, lanes] + planes[0, col]
            last[z, :, lanes] = planes[1, col]


def finish_body(g, meta, parts, grown, last, out, worst):
    total = lane_values(jnp.sum(parts[...], axis=0, keepdims=True), 1)[0]
    weight = weight_of(total, live_cells(g, meta, 3))
    worst[...] = jnp.broadcast_to(jnp.max(parts[...], axis=0, keepdims=True), worst.shape)
    w3 = jnp.broadcast_to(weight, (8, g.wide))
    for z in range(BLOCK_Z):
        for at in range(0, g.span, 8):
            out[z, at : at + 8, :] = grown[z, at : at + 8, :] + w3 * last[z, at : at + 8, :]


def index_table(g, assign):
    zm_here, zv_here = lax.axis_index("zm"), lax.axis_index("zv")
    me = zm_here * g.zv + zv_here
    slots = assign.reshape(ITERS, -1)
    owner = jnp.arange(slots.shape[1]) // g.slots // g.zv
    owner = jnp.where(jnp.arange(ITERS)[:, None] == ITERS - 1, owner ^ zm_here, owner)
    column = jnp.arange(2 * g.blocks + 2 * g.cb)
    here = column % g.blocks
    far = jnp.where(column < 2 * g.blocks, column // g.blocks, (column - 2 * g.blocks) // g.cb)
    local = jnp.where(column < 2 * g.blocks, here, (column - 2 * g.blocks) % g.cb)
    side = jnp.where(column < 2 * g.blocks, 0, 1)
    inside = (zm_here + far < g.zm) & (zv_here + side < g.zv)
    target = jnp.where(inside, (me + far * g.zv + side) * g.blocks + local, -2)
    found = jnp.max(jnp.where(slots[:, None, :] == target[None, :, None], owner[:, None, :], -1), axis=2)
    count = jnp.sum((slots >= 0).astype(jnp.int32), axis=1, keepdims=True)
    flags = jnp.stack([zm_here == g.zm - 1, zv_here == g.zv - 1]).astype(jnp.int32)
    gap = jnp.zeros((ITERS, 120 - found.shape[1]), jnp.int32)
    flags = jnp.broadcast_to(flags[None, :], (ITERS, 2))
    return jnp.concatenate([found, gap, flags, count, jnp.zeros((ITERS, 5), jnp.int32)], axis=1)


def to_all(rows):
    count = lax.axis_size("zm") * lax.axis_size("zv")
    return lax.all_to_all(rows.reshape(count, 1, 128), AXES, 0, 0, tiled=True).reshape(count, 128)


def from_next(value, axis):
    count = lax.axis_size(axis)
    return lax.ppermute(value, axis, [(i, i - 1) for i in range(1, count)])


def shards(table, refined, assign):
    g = Shape(table.shape, assign.shape, lax.axis_size("zm"), lax.axis_size("zv"))
    everyone = g.zm * g.zv
    part = functools.partial
    fields = g.blocks + 1
    columns = g.wide // LANES
    slots = assign.transpose(0, 2, 1).reshape(ITERS * g.slots, -1)
    views = refined.reshape(ITERS * g.slots, BLOCK_Z // 8, 8, PAIRS, LANES).transpose(0, 1, 3, 2, 4)
    views = views.reshape(ITERS * g.slots, ROWS, LANES)

    below = from_next(table[:ITERS], "zm")
    packed = call(
        part(pack_three_body, g), struct(g.zm, OFFSET[3], LANES), [SMEM, HBM], VMEM,
        [pltpu.SMEM((ITERS, g.zm), jnp.int32), dma(3 * g.zm)], "pack_three",
    )(slots, views)
    data = lax.all_to_all(packed, "zm", 0, 0, tiled=True)
    packed = call(
        part(pack_last_body, g), [struct(ROWS, LANES)] * g.zm, [SMEM, HBM], [VMEM] * g.zm,
        [pltpu.SMEM((ITERS, g.zm), jnp.int32), dma(g.zm)], "pack_last",
    )(slots, views)
    last_data = [packed[0]]
    for k in range(1, g.zm):
        last_data.append(lax.ppermute(packed[k], "zm", [(i, i ^ k) for i in range(g.zm)]))
    meta = index_table(g, assign)

    nodes, strip = call(
        part(to_blocks_body, g), [struct(DEEP, g.blocks, *TILE), struct(DEEP, *TILE)], [VMEM] * 2, [VMEM] * 2,
        [pltpu.VMEM((columns, g.span, LANES), F32)], "to_blocks",
    )(table, below)
    strip = from_next(strip, "zv")
    interp, interp_halo = call(
        part(interp_body, g), [struct(LAYERS[0], g.blocks, *TILE), struct(LAYERS[0], *TILE)],
        [SMEM, VMEM, VMEM], [VMEM] * 2, [pltpu.VMEM((LAYERS[0], fields, *TILE), F32)], "interp",
    )(meta, nodes, strip)

    strips = call(
        part(strip_body, g), struct(sum(LAYERS[:3]), *TILE), [SMEM, HBM], VMEM,
        [pltpu.VMEM((3 * g.cb, LAYERS[0] * PAIRS, LANES), F32), dma(6 * g.cb)], "strips",
    )(meta, data)
    strips = from_next(strips, "zv")
    a0, a1, a2, totals, peaks0 = call(
        part(local_body, g),
        [struct(LAYERS[0], g.blocks, *TILE), struct(LAYERS[1], g.blocks, *TILE), struct(BLOCK_Z, g.blocks, *TILE),
         struct(3, *TILE), struct(g.blocks, *TILE)],
        [SMEM, HBM, VMEM], [VMEM] * 5, [pltpu.VMEM(data.shape, F32), dma(g.zm)], "local",
    )(meta, data, interp)
    main = [struct(LAYERS[2], g.blocks, *TILE)] * 3
    products, ca0, ca1, cb1, b1, halos = call(
        part(products_body, g),
        [struct(everyone, 128)] + main + [struct(BLOCK_Z, g.blocks, *TILE), struct(3, LAYERS[1], *TILE)],
        [SMEM] + [VMEM] * 6, [VMEM] + [HBM] * 5,
        [pltpu.VMEM((LAYERS[0] + 1, *TILE), F32)] * 3
        + [pltpu.VMEM((LAYERS[1] + 1, g.blocks, *TILE), F32)] * 4
        + [pltpu.VMEM((3, LAYERS[1], *TILE), F32), pltpu.VMEM((3, LAYERS[1], fields, *TILE), F32), dma(5)],
        "products",
    )(meta, strips, interp_halo, a0, a1, a2, totals)
    products = to_all(products)
    own = struct(BLOCK_Z, g.blocks, *TILE)
    r2, r3, errors, stats, weights = call(
        part(last_body, g), [own, own, struct(ITERS, 128), struct(everyone, 128), struct(3, *TILE)],
        [SMEM] + [VMEM] * 5 + [HBM] * (1 + g.zm + 6), [HBM] * 2 + [VMEM] * 3,
        [pltpu.VMEM((4, LAYERS[2], g.blocks, *TILE), F32)] + [pltpu.VMEM(own.shape, F32)] * 2
        + [pltpu.VMEM((g.zm, LAYERS[2] * PAIRS, LANES), F32), pltpu.VMEM((g.zm, ROWS, LANES), F32)]
        + [pltpu.VMEM((LAYERS[2], g.blocks, *TILE), F32), pltpu.VMEM((LAYERS[2], *TILE), F32)]
        + [pltpu.VMEM((LAYERS[2], g.blocks, *TILE), F32), pltpu.VMEM((BLOCK_Z, fields, *TILE), F32)]
        + [pltpu.VMEM((3, g.blocks, *TILE), F32), dma(6 + 2 * g.zm)],
        "last",
    )(meta, products, strips, interp_halo, halos, peaks0, data, *last_data, interp, ca0, ca1, cb1, a1, b1)
    stats = to_all(stats)
    grown, last = call(
        part(assemble_body, g), [struct(*table.shape)] * 2, [VMEM] * 2 + [HBM] * 5, [VMEM] * 2,
        [pltpu.VMEM((5, BLOCK_Z, g.blocks, *TILE), F32), pltpu.VMEM((2, columns, g.span, LANES), F32), dma(5)],
        "assemble",
    )(table, weights, a0, a1, b1, r2, r3)
    table_out, worst = call(
        part(finish_body, g), [struct(*table.shape), struct(8, 128)], [SMEM] + [VMEM] * 3, [VMEM] * 2, [], "finish",
    )(meta, stats, grown, last)
    return (table_out, errors[:, : g.blocks], worst[0, 1 : 1 + ITERS])


def solution(mesh):
    in_specs = (P("zm", "zv", None), P(None, ("zm", "zv"), None, None), P())
    out_specs = (P("zm", "zv", None), P(None, ("zm", "zv")), P())
    return jax.shard_map(shards, mesh=mesh, in_specs=in_specs, out_specs=out_specs, check_vma=False)
```

```python
import functools

import jax
import jax.numpy as jnp
from jax import lax
from jax.experimental import pallas as pl
from jax.experimental.pallas import tpu as pltpu
from jax.sharding import PartitionSpec as P


S = 8
BLOCK_Z = 16
BLOCK_V = 16
BLOCK_C = 8
ITERS = 4
HALF = BLOCK_C * S
PAIRS = BLOCK_V // 2
LANES = 2 * HALF
ROWS = BLOCK_Z * PAIRS
DEEP = BLOCK_Z + ITERS
AXES = ("zm", "zv")
F32 = jnp.float32
TILE = (PAIRS, LANES)


def halo_rows(iteration):
    return ITERS - 1 - iteration


LAYERS = [BLOCK_Z + halo_rows(i) for i in range(ITERS)]
OFFSET = [sum(LAYERS[:i]) * PAIRS for i in range(ITERS)]


def lane_ids():
    return lax.broadcasted_iota(jnp.int32, TILE, 1)


def sub_ids():
    return lax.broadcasted_iota(jnp.int32, TILE, 0)


VMEM = pl.BlockSpec(memory_space=pltpu.VMEM)
SMEM = pl.BlockSpec(memory_space=pltpu.SMEM)
HBM = pl.BlockSpec(memory_space=pltpu.HBM)
WHOLE = 60
PART = 24


def call(body, outs, in_specs, out_specs, scratch, name, limit, flops=2000000):
    return pl.pallas_call(
        body,
        out_shape=outs,
        in_specs=in_specs,
        out_specs=out_specs,
        scratch_shapes=list(scratch),
        name=name,
        compiler_params=pltpu.CompilerParams(vmem_limit_bytes=limit << 20),
        cost_estimate=pl.CostEstimate(flops=flops, bytes_accessed=1 << 20, transcendentals=0),
    )


def struct(*shape, dtype=F32):
    return jax.ShapeDtypeStruct(shape, dtype)


def dma(count):
    return pltpu.SemaphoreType.DMA((count,))


class Shape:
    def __init__(self, table, assign, zm_count, zv_count):
        self.zm, self.zv = zm_count, zv_count
        self.span, self.wide = table[1], table[2]
        self.vb = self.span // BLOCK_V
        self.cb = self.wide // HALF
        self.vt = self.span // 8
        self.ct = self.wide // LANES
        self.blocks = self.vb * self.cb
        self.pairs = self.vb * self.ct
        self.slots = assign[2]
        self.cells = BLOCK_Z * BLOCK_V * BLOCK_C * S

    def main(self, layers):
        return (self.ct, layers, self.span, LANES)

    def halo(self, layers):
        return (self.ct, layers, 8, LANES)


def fill_inverse(g, iterations, assign, inverse):
    me = lax.axis_index("zm") * g.zv + lax.axis_index("zv")
    for t in iterations:
        for peer in range(g.zm):
            inverse[t, peer] = 0
        for slot in range(g.slots):
            block = assign[t * g.slots + slot, me]

            @pl.when(block >= 0)
            def _():
                inverse[t, block // (g.blocks * g.zv)] = slot


def pack_three_body(g, assign, refined, out, inverse, held, sems, out_sems):
    three = range(ITERS - 1)
    fill_inverse(g, three, assign, inverse)

    def copy(t, peer):
        source = refined.at[t * g.slots + inverse[t, peer]]
        return pltpu.make_async_copy(source, held.at[peer, OFFSET[t] : OFFSET[t] + ROWS, :], sems.at[t * g.zm + peer])

    writes = []
    for t in three:
        for peer in range(g.zm):
            copy(t, peer).start()
    for t in three:
        for peer in range(g.zm):
            copy(t, peer).wait()
        for peer in range(g.zm):
            after = min(peer + 1, g.zm - 1)
            for z in range(halo_rows(t)):
                at = OFFSET[t] + ROWS + z * PAIRS
                held[peer, at : at + PAIRS, :] = held[after, pl.ds(OFFSET[t] + z, PAIRS, stride=8), :]
        rows = slice(OFFSET[t], OFFSET[t + 1])
        writes.append(pltpu.make_async_copy(held.at[:, rows, :], out.at[:, rows, :], out_sems.at[t]))
        writes[-1].start()
    for write in writes:
        write.wait()


def pack_last_body(g, assign, refined, *rest):
    outs, inverse, sems = rest[: g.zm], rest[-2], rest[-1]
    t = ITERS - 1
    fill_inverse(g, [t], assign, inverse)
    here = lax.axis_index("zm")
    copies = []
    for k in range(g.zm):
        source = refined.at[t * g.slots + inverse[t, here ^ k]]
        copies.append(pltpu.make_async_copy(source, outs[k], sems.at[k]))
    for copy in copies:
        copy.start()
    for copy in copies:
        copy.wait()


def block_row(z):
    return z // 8 * 8 * PAIRS + z % 8


def pair_tiles(left, first, second):
    even = jnp.where(left, first, pltpu.roll(second, HALF, 1))
    odd = jnp.where(left, pltpu.roll(first, HALF, 1), second)
    return even, odd


def pair_live(meta, iteration, column, left):
    first, second = meta[iteration, column] >= 0, meta[iteration, column + 1] >= 0
    return (left & first) | (~left & second)


def strip_body(g, meta, data, unused_a, unused_b, out, held, planes, sems):
    three = range(ITERS - 1)
    left, sub = lane_ids() < HALF, sub_ids()

    def copies(t, c):
        mine = data.at[jnp.maximum(meta[t, c], 0), OFFSET[t] : OFFSET[t] + ROWS, :]
        far = data.at[jnp.maximum(meta[t, g.blocks + c], 0), OFFSET[t] + ROWS : OFFSET[t] + LAYERS[t] * PAIRS, :]
        at = t * g.cb + c
        return (
            pltpu.make_async_copy(mine, held.at[at, 0:ROWS, :], sems.at[2 * at]),
            pltpu.make_async_copy(far, held.at[at, ROWS : LAYERS[t] * PAIRS, :], sems.at[2 * at + 1]),
        )

    for t in three:
        for c in range(g.cb):
            for copy in copies(t, c):
                copy.start()
    for t in three:
        for c in range(g.cb):
            for copy in copies(t, c):
                copy.wait()
        first = sum(LAYERS[:t])
        for z in range(LAYERS[t]):
            for col in range(g.ct):
                tiles = []
                for c in (2 * col, 2 * col + 1):
                    if z < BLOCK_Z:
                        tiles.append(held[t * g.cb + c, pl.ds(block_row(z), PAIRS, stride=8), :])
                    else:
                        tiles.append(held[t * g.cb + c, z * PAIRS : (z + 1) * PAIRS, :])
                even, odd = pair_tiles(left, *tiles)
                planes[col, first + z, pl.ds(0, PAIRS, stride=2), :] = even
                planes[col, first + z, pl.ds(1, PAIRS, stride=2), :] = odd
        for z in range(first, first + LAYERS[t]):
            out[z] = jnp.where(sub < 4, planes[0, z, 0:8, :], pltpu.roll(planes[1, z, 0:8, :], 4, 0))


def strip_tile(strips, z, col):
    return strips[z] if col == 0 else pltpu.roll(strips[z], 4, 0)


class Stencil:
    def __init__(self, g, edge):
        self.g = g
        lane, sub = lane_ids(), sub_ids()
        self.inner = lane < LANES - S
        self.above = sub < 7
        self.last = edge & (sub == 7)

    def __call__(self, get, z, low):
        g = self.g
        sums, turned = {}, {}
        for vt in range(g.vt + 1):
            for col in range(g.ct):
                sums[col, vt] = get(col, vt, z) + get(col, vt, low)
                turned[col, vt] = pltpu.roll(sums[col, vt], LANES - S, 1)
        both, up = {}, {}
        for vt in range(g.vt + 1):
            for col in range(g.ct):
                beside = sums[col, vt] if col == g.ct - 1 else turned[col + 1, vt]
                both[col, vt] = sums[col, vt] + jnp.where(self.inner, turned[col, vt], beside)
                up[col, vt] = pltpu.roll(both[col, vt], 7, 0)
        result = {}
        for vt in range(g.vt + 1):
            for col in range(g.ct):
                value = up[col, vt]
                if vt < g.vt:
                    value = jnp.where(self.above, value, up[col, vt + 1])
                if vt == g.vt - 1:
                    value = jnp.where(self.last, both[col, vt], value)
                result[col, vt] = 0.125 * (both[col, vt] + value)
        return result


def edges(meta):
    return meta[0, 120] == 1, meta[0, 121] == 1


def layer_below(z, edge):
    return jnp.where((z == BLOCK_Z - 1) & edge, z, z + 1)


def clip(z, top):
    return jnp.minimum(jnp.maximum(z, 0), top)


def tile_rows(vt):
    return slice(vt * 8, vt * 8 + 8)


def reader(g, main, halo):
    return lambda col, vt, z: halo[col, z] if vt == g.vt else main[col, z, tile_rows(vt), :]


def put(g, main, halo, z, values):
    for (col, vt), value in values.items():
        if vt == g.vt:
            halo[col, z] = value
        else:
            main[col, z, tile_rows(vt), :] = value


def interp_body(g, meta, table, below, strip, interp, interp_halo, nodes, nodes_halo):
    edge_z, edge_v = edges(meta)
    stencil = Stencil(g, edge_v)

    def take(source, z, target):
        for col in range(g.ct):
            lanes = slice(col * LANES, (col + 1) * LANES)
            nodes[col, target] = source[z, :, lanes]
            nodes_halo[col, target] = strip[target, :, lanes]

    @pl.loop(0, BLOCK_Z)
    def _(z):
        take(table, z, z)

    @pl.loop(0, ITERS)
    def _(z):
        take(below, z, BLOCK_Z + z)

    get = reader(g, nodes, nodes_halo)

    @pl.loop(0, LAYERS[0])
    def _(z):
        put(g, interp, interp_halo, z, stencil(get, z, layer_below(z, edge_z)))


def fill_local(g, meta, t, layers, pick, interp, out, pair, left):
    vb, col = pair // g.ct, pair % g.ct
    column = vb * g.cb + 2 * col
    live = [pair_live(meta, t, column + far * g.blocks, left) for far in range(2)]
    row = pl.multiple_of(vb * BLOCK_V, BLOCK_V)
    for z in range(layers):
        even, odd = pair_tiles(left, *pick(column, z))
        out[col, z, pl.ds(row, PAIRS, stride=2), :] = even
        out[col, z, pl.ds(row + 1, PAIRS, stride=2), :] = odd
    total, peak = jnp.zeros(TILE, F32), jnp.zeros(TILE, F32)
    for z in range(layers):
        for half in range(2):
            rows = pl.ds(row + 8 * half, 8)
            value = jnp.where(live[z >= BLOCK_Z], out[col, z, rows, :] - interp[col, z, rows, :], 0.0)
            out[col, z, rows, :] = value
            if z < BLOCK_Z:
                total = total + value * value
                peak = jnp.maximum(peak, jnp.abs(value))
    return total, peak


def local_body(g, meta, data, interp_in, a0, a1, a2, totals, peaks, held, interp, sems):
    copies = [pltpu.make_async_copy(data.at[owner], held.at[owner], sems.at[owner]) for owner in range(g.zm)]
    copies.append(pltpu.make_async_copy(interp_in, interp, sems.at[g.zm]))
    for copy in copies:
        copy.start()
    totals[...] = jnp.zeros_like(totals)
    left = lane_ids() < HALF
    for copy in copies:
        copy.wait()

    @pl.loop(0, g.pairs)
    def _(pair):
        for t, out in ((0, a0), (1, a1), (2, a2)):

            def pick(column, z):
                tiles = []
                for block in (column, column + 1):
                    if z < BLOCK_Z:
                        owner = jnp.maximum(meta[t, block], 0)
                        tiles.append(held[owner, pl.ds(OFFSET[t] + block_row(z), PAIRS, stride=8), :])
                    else:
                        owner = jnp.maximum(meta[t, g.blocks + block], 0)
                        at = OFFSET[t] + z * PAIRS
                        tiles.append(held[owner, at : at + PAIRS, :])
                return tiles

            total, peak = fill_local(g, meta, t, LAYERS[t], pick, interp, out, pair, left)
            totals[t] += total
            if t == 0:
                peaks[pair] = peak


def local_last_body(g, meta, interp_in, *rest):
    data, (a3_out, a3, held, interp, sems) = rest[: g.zm], rest[g.zm :]
    t = ITERS - 1
    copies = [pltpu.make_async_copy(data[k], held.at[k], sems.at[k]) for k in range(g.zm)]
    for col in range(g.ct):
        copies.append(pltpu.make_async_copy(interp_in.at[col, 0:BLOCK_Z], interp.at[col], sems.at[g.zm + col]))
    for copy in copies:
        copy.start()
    left = lane_ids() < HALF
    for copy in copies:
        copy.wait()

    @pl.loop(0, g.pairs)
    def _(pair):
        def pick(column, z):
            owners = [jnp.maximum(meta[t, block], 0) for block in (column, column + 1)]
            return [held[owner, pl.ds(block_row(z), PAIRS, stride=8), :] for owner in owners]

        fill_local(g, meta, t, BLOCK_Z, pick, interp, a3, pair, left)

    write = pltpu.make_async_copy(a3, a3_out, sems.at[0])
    write.start()
    write.wait()


PRODUCTS = 14


def spread_rows(values, count):
    rows = [jnp.sum(value, axis=0, keepdims=True) for value in values]
    rows += [jnp.zeros_like(rows[0])] * (-len(rows) % 8)
    column = jnp.sum(jnp.concatenate(rows, 0), axis=1, keepdims=True)
    lane = lax.broadcasted_iota(jnp.int32, (len(rows), 128), 1)
    row = lax.broadcasted_iota(jnp.int32, (len(rows), 128), 0)
    line = jnp.sum(jnp.where(lane == row, column, 0.0), axis=0, keepdims=True)
    return jnp.broadcast_to(line, (count, 128))


def fill_masks(g, meta, masks, iterations, left):
    for at, t in enumerate(iterations):
        for far in range(2):
            for pair in range(g.pairs):
                column = pair // g.ct * g.cb + pair % g.ct * 2 + far * g.blocks
                masks[at, far, pair] = jnp.where(pair_live(meta, t, column, left), 1.0, 0.0)


def halo_live(g, meta, iteration, left):
    first = 2 * g.blocks
    return [[pair_live(meta, iteration, first + far * g.cb + 2 * col, left) for col in range(g.ct)] for far in range(2)]


def segments(top, counts):
    result, high = [], top
    for count in counts:
        result.append((high - count + 1, high))
        high -= count
    return result


def products_body(g, meta, strips, interp_halo, a0, a1, a2, totals, out, ca0_out, ca1_out, cb1_out, halos,
                  a0_halo, a1_halo, b1_halo, b1, ca0, ca1, cb1, masks, sems):
    edge_z, edge_v = edges(meta)
    stencil = Stencil(g, edge_v)
    left = lane_ids() < HALF
    live0, live1 = halo_live(g, meta, 0, left), halo_live(g, meta, 1, left)
    fill_masks(g, meta, masks, (1, 2), left)
    for col in range(g.ct):
        for z in range(LAYERS[0]):
            value = strip_tile(strips, z, col) - interp_halo[col, z]
            a0_halo[col, z] = jnp.where(live0[z >= BLOCK_Z][col], value, 0.0)
        for z in range(LAYERS[1]):
            value = strip_tile(strips, LAYERS[0] + z, col) - interp_halo[col, z]
            a1_halo[col, z] = jnp.where(live1[z >= BLOCK_Z][col], value, 0.0)
    get0, get1, getb = reader(g, a0, a0_halo), reader(g, a1, a1_halo), reader(g, b1, b1_halo)
    top0, top1 = LAYERS[1] - 1, LAYERS[2] - 1

    def step(i, carry):
        carry = list(carry)
        base = top0 - i
        z = base + 1
        at = clip(z, top1)
        low = layer_below(at, edge_z)
        after_a = stencil(get1, at, low)
        after_b = stencil(getb, at, low)
        put(g, ca1, halos.at[1], at, after_a)
        put(g, cb1, halos.at[2], at, after_b)
        row = jnp.minimum(at, BLOCK_Z - 1)
        counts = jnp.where((z >= 0) & (z < BLOCK_Z), 1.0, 0.0)
        for pair in range(g.pairs):
            col = pair % g.ct
            live = masks[1, 0, pair] * counts > 0.5
            live1_here = counts > 0.5
            for vt in (pair // g.ct * 2, pair // g.ct * 2 + 1):
                rows = tile_rows(vt)
                a, b = a1[col, row, rows, :], jnp.where(live1_here, b1[col, row, rows, :], 0.0)
                carry[0] = carry[0] + a * b
                carry[1] = carry[1] + b * b
                parts = [a2[col, row, rows, :]] + [
                    jnp.where(live, value, 0.0) for value in (ca0[col, row, rows, :], after_a[col, vt], after_b[col, vt])
                ]
                slot = 2
                for m in range(4):
                    for n in range(max(m, 1), 4):
                        carry[slot] = carry[slot] + parts[m] * parts[n]
                        slot += 1
        at = clip(base, top0)
        after = stencil(get0, at, layer_below(at, edge_z))
        put(g, ca0, halos.at[0], at, after)
        far = jnp.where(at >= BLOCK_Z, 1, 0)
        for (col, vt), value in after.items():
            if vt == g.vt:
                live = (live1[0][col] & (at < BLOCK_Z)) | (live1[1][col] & (at >= BLOCK_Z))
                b1_halo[col, at] = jnp.where(live, value, 0.0)
            else:
                mask = masks[0, far, vt // 2 * g.ct + col]
                b1[col, at, tile_rows(vt), :] = jnp.where(mask > 0.5, value, 0.0)
        return tuple(carry)

    carry = (jnp.zeros(TILE, F32),) * 11
    writes = []
    start = 0
    for index, (lowest, highest) in enumerate(segments(top1, (5, 6, 6))):
        stop = top0 - (lowest - 1) + 1
        carry = lax.fori_loop(start, stop, step, carry)
        start = stop
        for which, (source, target) in enumerate(((ca0, ca0_out), (ca1, ca1_out), (cb1, cb1_out))):
            for col in range(g.ct):
                layers = slice(lowest, highest + 1)
                sem = sems.at[(index * 3 + which) * g.ct + col]
                writes.append(pltpu.make_async_copy(source.at[col, layers], target.at[col, layers], sem))
                writes[-1].start()
    values = [totals[0], totals[1], carry[0], carry[1], totals[2]] + list(carry[2:])
    out[...] = spread_rows(values, out.shape[0])
    for write in writes:
        write.wait()


def weight_of(total, count):
    return 1.0 / (1.0 + jnp.sqrt(jnp.maximum(total, 0.0) / count))


def lane_values(line, count):
    lane = lax.broadcasted_iota(jnp.int32, line.shape, 1)
    return [jnp.sum(jnp.where(lane == i, line, 0.0), axis=1, keepdims=True) for i in range(count)]


def live_cells(g, meta, iteration):
    return jnp.full((1, 1), meta[iteration, 122], jnp.int32).astype(F32) * F32(g.cells)


def three_weights(g, meta, parts):
    q = lane_values(jnp.sum(parts[...], axis=0, keepdims=True), PRODUCTS)
    w0 = weight_of(q[0], live_cells(g, meta, 0))
    w1 = weight_of(q[1] - 2.0 * w0 * q[2] + w0 * w0 * q[3], live_cells(g, meta, 1))
    f = [jnp.ones_like(w0), -w0, -w1, w0 * w1]
    total, at = jnp.zeros_like(w0), 4
    for i in range(4):
        for j in range(i, 4):
            total = total + (1.0 if i == j else 2.0) * f[i] * f[j] * q[at]
            at += 1
    return [jnp.broadcast_to(w, TILE) for w in (w0, w1, weight_of(total, live_cells(g, meta, 2)))]


def last_body(g, meta, parts, strips, interp_halo, halos_in, peaks0, a1_in, a2_in, a3_in, ca0_in, ca1_in, cb1_in,
              r2_out, r3_out, errors, out, weights,
              a1, a2, a3, ca0, ca1, cb1, r2, r2_halo, change, r3, masks, peaks, sems, out_sems):
    top = LAYERS[2] - 1
    chunks = segments(top, (5, 4, 4, 4))
    reads, at = [], 0
    for lowest, highest in chunks:
        group = []
        for source, target, layers in ((a1_in, a1, BLOCK_Z), (a2_in, a2, BLOCK_Z + 1), (a3_in, a3, BLOCK_Z),
                                       (ca0_in, ca0, BLOCK_Z + 1), (ca1_in, ca1, BLOCK_Z + 1), (cb1_in, cb1, BLOCK_Z + 1)):
            for col in range(g.ct):
                span = slice(lowest, min(highest + 1, layers))
                group.append(pltpu.make_async_copy(source.at[col, span], target.at[col, span], sems.at[at]))
                at += 1
        reads.append(group)
    for group in reads:
        for copy in group:
            copy.start()
    edge_z, edge_v = edges(meta)
    stencil = Stencil(g, edge_v)
    left = lane_ids() < HALF
    fill_masks(g, meta, masks, (1, 2, 3), left)
    w0, w1, w2 = three_weights(g, meta, parts)
    w01 = w0 * w1
    weights[0], weights[1], weights[2] = w0, w1, w2
    live = halo_live(g, meta, 2, left)
    peaks[...] = jnp.zeros_like(peaks)
    first = sum(LAYERS[:2])
    for col in range(g.ct):
        for z in range(LAYERS[2]):
            value = interp_halo[col, z] + w0 * halos_in[0, col, z] + w1 * halos_in[1, col, z] - w01 * halos_in[2, col, z]
            r2_halo[col, z] = jnp.where(live[z >= BLOCK_Z][col], strip_tile(strips, first + z, col) - value, 0.0)
    get = reader(g, r2, r2_halo)

    def step(i, total):
        base = top - i
        z = base + 1
        at = clip(z, BLOCK_Z - 1)
        counts = jnp.where((z >= 0) & (z < BLOCK_Z), 1.0, 0.0)
        after = stencil(get, at, layer_below(at, edge_z))
        for pair in range(g.pairs):
            col = pair % g.ct
            mask = masks[2, 0, pair] > 0.5
            peak = peaks[2, pair]
            for vt in (pair // g.ct * 2, pair // g.ct * 2 + 1):
                rows = tile_rows(vt)
                value = jnp.where(mask, change[col, at, rows, :] + w2 * after[col, vt], 0.0)
                value = jnp.where(counts > 0.5, a3[col, at, rows, :] - value, 0.0)
                r3[col, at, rows, :] = value
                total = total + value * value
                peak = jnp.maximum(peak, jnp.abs(value))
            peaks[2, pair] = peak
        at = clip(base, top)
        far = jnp.where(at >= BLOCK_Z, 1, 0)
        own = jnp.minimum(at, BLOCK_Z - 1)
        counts = jnp.where(at < BLOCK_Z, 1.0, 0.0)
        for pair in range(g.pairs):
            col = pair % g.ct
            mask1, mask2 = masks[0, 0, pair] > 0.5, masks[1, far, pair] > 0.5
            peak1, peak2 = peaks[0, pair], peaks[1, pair]
            for vt in (pair // g.ct * 2, pair // g.ct * 2 + 1):
                rows = tile_rows(vt)
                zero = w0 * ca0[col, at, rows, :]
                whole = zero + w1 * ca1[col, at, rows, :] - w01 * cb1[col, at, rows, :]
                change[col, at, rows, :] = whole
                value = a2[col, at, rows, :] - jnp.where(mask2, whole, 0.0)
                r2[col, at, rows, :] = value
                peak2 = jnp.maximum(peak2, jnp.where(counts > 0.5, jnp.abs(value), 0.0))
                value = a1[col, own, rows, :] - jnp.where(mask1, zero, 0.0)
                peak1 = jnp.maximum(peak1, jnp.where(counts > 0.5, jnp.abs(value), 0.0))
            peaks[0, pair] = peak1
            peaks[1, pair] = peak2
        return total

    total, start, writes = jnp.zeros(TILE, F32), 0, []
    for index, (lowest, highest) in enumerate(chunks):
        for copy in reads[index]:
            copy.wait()
        stop = top - lowest + 1 + (1 if lowest == 0 else 0)
        total = lax.fori_loop(start, stop, step, total)
        start = stop
        below = lowest + 1 if lowest else 0
        above = min((chunks[index - 1][0] if index else BLOCK_Z - 1), BLOCK_Z - 1)
        for which, (source, target, layers) in enumerate(
            ((r2, r2_out, slice(lowest, min(highest, BLOCK_Z - 1) + 1)), (r3, r3_out, slice(below, above + 1)))
        ):
            for col in range(g.ct):
                sem = out_sems.at[(index * 2 + which) * g.ct + col]
                writes.append(pltpu.make_async_copy(source.at[col, layers], target.at[col, layers], sem))
                writes[-1].start()

    line = spread_rows([total], 1)
    lane = lax.broadcasted_iota(jnp.int32, (1, 128), 1)
    lane_p = lax.broadcasted_iota(jnp.int32, (g.pairs, 128), 1)
    row_p = lax.broadcasted_iota(jnp.int32, (g.pairs, 128), 0)
    for i in range(ITERS):
        tiles = [peaks0[pair] if i == 0 else peaks[i - 1, pair] for pair in range(g.pairs)]
        rows = jnp.concatenate([jnp.max(tile, axis=0, keepdims=True) for tile in tiles], 0)
        found = jnp.zeros((1, 128), F32)
        for half in range(2):
            inside = lane_p // HALF == half
            column = jnp.max(jnp.where(inside, rows, 0.0), axis=1, keepdims=True)
            place = row_p // g.ct * g.cb + row_p % g.ct * 2 + half
            found = found + jnp.sum(jnp.where(lane_p == place, column, 0.0), axis=0, keepdims=True)
        errors[i : i + 1, :] = found
        line = jnp.where(lane == 1 + i, jnp.max(found, axis=1, keepdims=True), line)
    out[...] = jnp.broadcast_to(line, out.shape)
    for write in writes:
        write.wait()


def assemble_body(g, meta, weights, table_in, a0_in, a1_in, ca0_in, r2_in, grown_out,
                  table, a0, a1, ca0, r2, grown, masks, sems):
    copies = [pltpu.make_async_copy(table_in, table, sems.at[0])]
    for i, (source, target) in enumerate(((a0_in, a0), (a1_in, a1), (ca0_in, ca0), (r2_in, r2))):
        for col in range(g.ct):
            copies.append(pltpu.make_async_copy(source.at[col, 0:BLOCK_Z], target.at[col], sems.at[1 + i * g.ct + col]))
    for copy in copies:
        copy.start()
    fill_masks(g, meta, masks, (1,), lane_ids() < HALF)
    w0, w1, w2 = weights[0], weights[1], weights[2]
    w01 = w0 * w1
    for copy in copies:
        copy.wait()

    @pl.loop(0, BLOCK_Z)
    def _(z):
        for pair in range(g.pairs):
            col = pair % g.ct
            lanes = slice(col * LANES, (col + 1) * LANES)
            mask = masks[0, 0, pair] > 0.5
            for vt in (pair // g.ct * 2, pair // g.ct * 2 + 1):
                rows = tile_rows(vt)
                value = w0 * a0[col, z, rows, :] + w1 * a1[col, z, rows, :] + w2 * r2[col, z, rows, :]
                value = value - jnp.where(mask, w01 * ca0[col, z, rows, :], 0.0)
                grown[z, rows, lanes] = table[z, rows, lanes] + value

    write = pltpu.make_async_copy(grown, grown_out, sems.at[0])
    write.start()
    write.wait()


def finish_body(g, meta, parts, grown_in, r3_in, out_hbm, worst, grown, r3, out, sems, out_sems):
    quarter = BLOCK_Z // 4
    reads, at = [], 0
    for part in range(4):
        layers = slice(part * quarter, (part + 1) * quarter)
        group = [pltpu.make_async_copy(grown_in.at[layers], grown.at[layers], sems.at[at])]
        for col in range(g.ct):
            group.append(pltpu.make_async_copy(r3_in.at[col, layers], r3.at[col, layers], sems.at[at + 1 + col]))
        at += 1 + g.ct
        reads.append(group)
    for group in reads:
        for copy in group:
            copy.start()
    total = lane_values(jnp.sum(parts[...], axis=0, keepdims=True), 1)[0]
    w3 = jnp.broadcast_to(weight_of(total, live_cells(g, meta, 3)), TILE)
    line = jnp.max(parts[...], axis=0, keepdims=True)
    for i, value in enumerate(lane_values(line, 1 + ITERS)[1:]):
        worst[i] = jnp.max(value)
    writes = []
    for part in range(4):
        for copy in reads[part]:
            copy.wait()
        layers = slice(part * quarter, (part + 1) * quarter)
        for z in range(part * quarter, (part + 1) * quarter):
            for col in range(g.ct):
                lanes = slice(col * LANES, (col + 1) * LANES)
                for vt in range(g.vt):
                    rows = tile_rows(vt)
                    out[z, rows, lanes] = grown[z, rows, lanes] + w3 * r3[col, z, rows, :]
        writes.append(pltpu.make_async_copy(out.at[layers], out_hbm.at[layers], out_sems.at[part]))
        writes[-1].start()
    for write in writes:
        write.wait()


def index_table(g, assign):
    zm_here, zv_here = lax.axis_index("zm"), lax.axis_index("zv")
    me = zm_here * g.zv + zv_here
    slots = assign.reshape(ITERS, -1)
    owner = jnp.arange(slots.shape[1]) // g.slots // g.zv
    owner = jnp.where(jnp.arange(ITERS)[:, None] == ITERS - 1, owner ^ zm_here, owner)
    column = jnp.arange(2 * g.blocks + 2 * g.cb)
    here = column % g.blocks
    far = jnp.where(column < 2 * g.blocks, column // g.blocks, (column - 2 * g.blocks) // g.cb)
    local = jnp.where(column < 2 * g.blocks, here, (column - 2 * g.blocks) % g.cb)
    side = jnp.where(column < 2 * g.blocks, 0, 1)
    inside = (zm_here + far < g.zm) & (zv_here + side < g.zv)
    target = jnp.where(inside, (me + far * g.zv + side) * g.blocks + local, -2)
    found = jnp.max(jnp.where(slots[:, None, :] == target[None, :, None], owner[:, None, :], -1), axis=2)
    count = jnp.sum((slots >= 0).astype(jnp.int32), axis=1, keepdims=True)
    flags = jnp.stack([zm_here == g.zm - 1, zv_here == g.zv - 1]).astype(jnp.int32)
    gap = jnp.zeros((ITERS, 120 - found.shape[1]), jnp.int32)
    flags = jnp.broadcast_to(flags[None, :], (ITERS, 2))
    return jnp.concatenate([found, gap, flags, count, jnp.zeros((ITERS, 5), jnp.int32)], axis=1)


def to_all(rows):
    count = lax.axis_size("zm") * lax.axis_size("zv")
    return lax.all_to_all(rows.reshape(count, 1, 128), AXES, 0, 0, tiled=True).reshape(count, 128)


def from_next(value, axis):
    count = lax.axis_size(axis)
    return lax.ppermute(value, axis, [(i, i - 1) for i in range(1, count)])


def shards(table, refined, assign):
    g = Shape(table.shape, assign.shape, lax.axis_size("zm"), lax.axis_size("zv"))
    everyone = g.zm * g.zv
    part = functools.partial
    slots = assign.transpose(0, 2, 1).reshape(ITERS * g.slots, -1)
    views = refined.reshape(ITERS * g.slots, BLOCK_Z // 8, 8, PAIRS, LANES).transpose(0, 1, 3, 2, 4)
    views = views.reshape(ITERS * g.slots, ROWS, LANES)
    vmem = lambda *shape: pltpu.VMEM(shape, F32)
    main, halo = g.main, g.halo

    packed = call(
        part(pack_three_body, g), struct(g.zm, OFFSET[3], LANES), [SMEM, HBM], HBM,
        [pltpu.SMEM((ITERS, g.zm), jnp.int32), vmem(g.zm, OFFSET[3], LANES), dma(3 * g.zm), dma(3)], "pack_three", WHOLE,
    )(slots, views)
    data = lax.all_to_all(packed, "zm", 0, 0, tiled=True)
    below = from_next(table[:ITERS], "zm")
    strip = from_next(jnp.concatenate([table[:, :8], below[:, :8]], 0), "zv")
    packed = call(
        part(pack_last_body, g), [struct(ROWS, LANES)] * g.zm, [SMEM, HBM], [VMEM] * g.zm,
        [pltpu.SMEM((ITERS, g.zm), jnp.int32), dma(g.zm)], "pack_last", PART,
    )(slots, views)
    last_data = [packed[0]]
    for k in range(1, g.zm):
        last_data.append(lax.ppermute(packed[k], "zm", [(i, i ^ k) for i in range(g.zm)]))
    meta = index_table(g, assign)
    interp, interp_halo = call(
        part(interp_body, g), [struct(*main(LAYERS[0])), struct(*halo(LAYERS[0]))],
        [SMEM] + [VMEM] * 3, [VMEM] * 2, [vmem(*main(DEEP)), vmem(*halo(DEEP))], "interp", PART,
    )(meta, table, below, strip)

    strips = call(
        part(strip_body, g), struct(sum(LAYERS[:3]), *TILE), [SMEM] + [HBM] * 3, VMEM,
        [vmem(3 * g.cb, LAYERS[0] * PAIRS, LANES), vmem(g.ct, sum(LAYERS[:3]), BLOCK_V, LANES), dma(6 * g.cb)],
        "strips", PART,
    )(meta, data, interp_halo, packed[0])
    strips = from_next(strips, "zv")
    a0, a1, a2, totals, peaks0 = call(
        part(local_body, g), [struct(*main(LAYERS[t])) for t in range(3)] + [struct(3, *TILE), struct(g.pairs, *TILE)],
        [SMEM] + [HBM] * 2, [VMEM] * 5, [vmem(*data.shape), vmem(*main(LAYERS[0])), dma(g.zm + 1)], "local", PART,
    )(meta, data, interp)
    products, ca0, ca1, cb1, halos = call(
        part(products_body, g),
        [struct(everyone, 128)] + [struct(*main(LAYERS[2]))] * 3 + [struct(3, *halo(LAYERS[1]))],
        [SMEM] + [VMEM] * 6, [VMEM] + [HBM] * 3 + [VMEM],
        [vmem(*halo(LAYERS[0] + 1)), vmem(*halo(LAYERS[1] + 1)), vmem(*halo(LAYERS[1] + 1))]
        + [vmem(*main(LAYERS[1] + 1))] * 4 + [vmem(2, 2, g.pairs, *TILE), dma(9 * g.ct)],
        "products", PART,
    )(meta, strips, interp_halo, a0, a1, a2, totals)
    products = to_all(products)
    own = struct(*main(BLOCK_Z))
    a3 = call(
        part(local_last_body, g), own, [SMEM] + [HBM] * (1 + g.zm), HBM,
        [vmem(*main(BLOCK_Z)), vmem(g.zm, ROWS, LANES), vmem(*main(BLOCK_Z)), dma(g.zm + g.ct)], "local_last", WHOLE,
    )(meta, interp, *last_data)
    r2, r3, errors, stats, weights = call(
        part(last_body, g), [own, own, struct(ITERS, 128), struct(everyone, 128), struct(3, *TILE)],
        [SMEM] + [VMEM] * 5 + [HBM] * 6, [HBM] * 2 + [VMEM] * 3,
        [vmem(*main(BLOCK_Z)), vmem(*main(LAYERS[2])), vmem(*main(BLOCK_Z))] + [vmem(*main(LAYERS[2]))] * 4
        + [vmem(*halo(LAYERS[2])), vmem(*main(LAYERS[2])), vmem(*main(BLOCK_Z)), vmem(3, 2, g.pairs, *TILE),
           vmem(3, g.pairs, *TILE), dma(24 * g.ct), dma(8 * g.ct)],
        "last", WHOLE,
    )(meta, products, strips, interp_halo, halos, peaks0, a1, a2, a3, ca0, ca1, cb1)
    stats = to_all(stats)
    grown = call(
        part(assemble_body, g), struct(*table.shape), [SMEM, VMEM] + [HBM] * 5, HBM,
        [vmem(*table.shape)] + [vmem(*main(BLOCK_Z))] * 4 + [vmem(*table.shape), vmem(1, 2, g.pairs, *TILE), dma(1 + 4 * g.ct)],
        "assemble", WHOLE,
    )(meta, weights, table, a0, a1, ca0, r2)
    table_out, worst = call(
        part(finish_body, g), [struct(*table.shape), struct(ITERS)], [SMEM, VMEM] + [HBM] * 2, [HBM, SMEM],
        [vmem(*table.shape), vmem(*main(BLOCK_Z)), vmem(*table.shape), dma(4 * (1 + g.ct)), dma(4)], "finish", WHOLE,
    )(meta, stats, grown, r3)
    return (table_out, errors[:, : g.blocks], worst)


def solution(mesh):
    in_specs = (P("zm", "zv", None), P(None, ("zm", "zv"), None, None), P())
    out_specs = (P("zm", "zv", None), P(None, ("zm", "zv")), P())
    return jax.shard_map(shards, mesh=mesh, in_specs=in_specs, out_specs=out_specs, check_vma=False)
```

```python
import functools

import jax
import jax.numpy as jnp
from jax import lax
from jax.experimental import pallas as pl
from jax.experimental.pallas import tpu as pltpu
from jax.sharding import PartitionSpec as P


S = 8
BLOCK_Z = 16
BLOCK_V = 16
BLOCK_C = 8
ITERS = 4
HALF = BLOCK_C * S
PAIRS = BLOCK_V // 2
LANES = 2 * HALF
ROWS = BLOCK_Z * PAIRS
DEEP = BLOCK_Z + ITERS
AXES = ("zm", "zv")
F32 = jnp.float32
TILE = (PAIRS, LANES)


def halo_rows(iteration):
    return ITERS - 1 - iteration


LAYERS = [BLOCK_Z + halo_rows(i) for i in range(ITERS)]
OFFSET = [sum(LAYERS[:i]) * PAIRS for i in range(ITERS)]


def lane_ids():
    return lax.broadcasted_iota(jnp.int32, TILE, 1)


def sub_ids():
    return lax.broadcasted_iota(jnp.int32, TILE, 0)


VMEM = pl.BlockSpec(memory_space=pltpu.VMEM)
SMEM = pl.BlockSpec(memory_space=pltpu.SMEM)
HBM = pl.BlockSpec(memory_space=pltpu.HBM)
WHOLE = 60
PART = 24


def call(body, outs, in_specs, out_specs, scratch, limit, flops=2000000):
    return pl.pallas_call(
        body,
        out_shape=outs,
        in_specs=in_specs,
        out_specs=out_specs,
        scratch_shapes=list(scratch),
        compiler_params=pltpu.CompilerParams(vmem_limit_bytes=limit << 20),
        cost_estimate=pl.CostEstimate(flops=flops, bytes_accessed=1 << 20, transcendentals=0),
    )


def struct(*shape, dtype=F32):
    return jax.ShapeDtypeStruct(shape, dtype)


def dma(count):
    return pltpu.SemaphoreType.DMA((count,))


class Shape:
    def __init__(self, table, assign, zm_count, zv_count):
        self.zm, self.zv = zm_count, zv_count
        self.span, self.wide = table[1], table[2]
        self.vb = self.span // BLOCK_V
        self.cb = self.wide // HALF
        self.vt = self.span // 8
        self.ct = self.wide // LANES
        self.blocks = self.vb * self.cb
        self.pairs = self.vb * self.ct
        self.slots = assign[2]
        self.cells = BLOCK_Z * BLOCK_V * BLOCK_C * S

    def main(self, layers):
        return (self.ct, layers, self.span, LANES)

    def halo(self, layers):
        return (self.ct, layers, 8, LANES)


def fill_inverse(g, iterations, assign, inverse):
    me = lax.axis_index("zm") * g.zv + lax.axis_index("zv")
    for t in iterations:
        for peer in range(g.zm):
            inverse[t, peer] = 0
        for slot in range(g.slots):
            block = assign[t * g.slots + slot, me]

            @pl.when(block >= 0)
            def _():
                inverse[t, block // (g.blocks * g.zv)] = slot


def pack_three_body(g, assign, refined, out, inverse, held, sems, out_sems):
    three = range(ITERS - 1)
    fill_inverse(g, three, assign, inverse)
    reads, writes = {}, []
    for t in three:
        for peer in range(g.zm):
            rows = slice(OFFSET[t], OFFSET[t] + ROWS)
            source = refined.at[t * g.slots + inverse[t, peer]]
            reads[t, peer] = pltpu.make_async_copy(source, held.at[peer, rows, :], sems.at[t * g.zm + peer])
            reads[t, peer].start()
    for t in three:
        for peer in range(g.zm):
            rows = slice(OFFSET[t], OFFSET[t] + ROWS)
            reads[t, peer].wait()
            sem = out_sems.at[t * g.zm + peer]
            writes.append(pltpu.make_async_copy(held.at[peer, rows, :], out.at[peer, rows, :], sem))
            writes[-1].start()
        for peer in range(g.zm):
            after = min(peer + 1, g.zm - 1)
            for z in range(halo_rows(t)):
                at = OFFSET[t] + ROWS + z * PAIRS
                held[peer, at : at + PAIRS, :] = held[after, pl.ds(OFFSET[t] + z, PAIRS, stride=8), :]
        rows = slice(OFFSET[t] + ROWS, OFFSET[t + 1])
        writes.append(pltpu.make_async_copy(held.at[:, rows, :], out.at[:, rows, :], out_sems.at[3 * g.zm + t]))
        writes[-1].start()
    for write in writes:
        write.wait()


def pack_last_body(g, assign, refined, *rest):
    outs, inverse, sems = rest[: g.zm], rest[-2], rest[-1]
    t = ITERS - 1
    fill_inverse(g, [t], assign, inverse)
    here = lax.axis_index("zm")
    copies = []
    for k in range(g.zm):
        source = refined.at[t * g.slots + inverse[t, here ^ k]]
        copies.append(pltpu.make_async_copy(source, outs[k], sems.at[k]))
    for copy in copies:
        copy.start()
    for copy in copies:
        copy.wait()


def block_row(z):
    return z // 8 * 8 * PAIRS + z % 8


def pair_tiles(left, first, second):
    even = jnp.where(left, first, pltpu.roll(second, HALF, 1))
    odd = jnp.where(left, pltpu.roll(first, HALF, 1), second)
    return even, odd


def pair_live(meta, iteration, column, left):
    first, second = meta[iteration, column] >= 0, meta[iteration, column + 1] >= 0
    return (left & first) | (~left & second)


def strip_body(g, meta, data, unused_a, unused_b, out, held, planes, sems):
    three = range(ITERS - 1)
    left, sub = lane_ids() < HALF, sub_ids()

    def copies(t, c):
        mine = data.at[jnp.maximum(meta[t, c], 0), OFFSET[t] : OFFSET[t] + ROWS, :]
        far = data.at[jnp.maximum(meta[t, g.blocks + c], 0), OFFSET[t] + ROWS : OFFSET[t] + LAYERS[t] * PAIRS, :]
        at = t * g.cb + c
        return (
            pltpu.make_async_copy(mine, held.at[at, 0:ROWS, :], sems.at[2 * at]),
            pltpu.make_async_copy(far, held.at[at, ROWS : LAYERS[t] * PAIRS, :], sems.at[2 * at + 1]),
        )

    for t in three:
        for c in range(g.cb):
            for copy in copies(t, c):
                copy.start()
    for t in three:
        for c in range(g.cb):
            for copy in copies(t, c):
                copy.wait()
        first = sum(LAYERS[:t])
        for z in range(LAYERS[t]):
            for col in range(g.ct):
                tiles = []
                for c in (2 * col, 2 * col + 1):
                    if z < BLOCK_Z:
                        tiles.append(held[t * g.cb + c, pl.ds(block_row(z), PAIRS, stride=8), :])
                    else:
                        tiles.append(held[t * g.cb + c, z * PAIRS : (z + 1) * PAIRS, :])
                even, odd = pair_tiles(left, *tiles)
                planes[col, first + z, pl.ds(0, PAIRS, stride=2), :] = even
                planes[col, first + z, pl.ds(1, PAIRS, stride=2), :] = odd
        for z in range(first, first + LAYERS[t]):
            out[z] = jnp.where(sub < 4, planes[0, z, 0:8, :], pltpu.roll(planes[1, z, 0:8, :], 4, 0))


def strip_tile(strips, z, col):
    return strips[z] if col == 0 else pltpu.roll(strips[z], 4, 0)


class Stencil:
    def __init__(self, g, edge):
        self.g = g
        lane, sub = lane_ids(), sub_ids()
        self.inner = lane < LANES - S
        self.above = sub < 7
        self.last = edge & (sub == 7)

    def __call__(self, get, z, low):
        g = self.g
        sums, turned = {}, {}
        for vt in range(g.vt + 1):
            for col in range(g.ct):
                sums[col, vt] = get(col, vt, z) + get(col, vt, low)
                turned[col, vt] = pltpu.roll(sums[col, vt], LANES - S, 1)
        both, up = {}, {}
        for vt in range(g.vt + 1):
            for col in range(g.ct):
                beside = sums[col, vt] if col == g.ct - 1 else turned[col + 1, vt]
                both[col, vt] = sums[col, vt] + jnp.where(self.inner, turned[col, vt], beside)
                up[col, vt] = pltpu.roll(both[col, vt], 7, 0)
        result = {}
        for vt in range(g.vt + 1):
            for col in range(g.ct):
                value = up[col, vt]
                if vt < g.vt:
                    value = jnp.where(self.above, value, up[col, vt + 1])
                if vt == g.vt - 1:
                    value = jnp.where(self.last, both[col, vt], value)
                result[col, vt] = 0.125 * (both[col, vt] + value)
        return result


def edges(meta):
    return meta[0, 120] == 1, meta[0, 121] == 1


def layer_below(z, edge):
    return jnp.where((z == BLOCK_Z - 1) & edge, z, z + 1)


def clip(z, top):
    return jnp.minimum(jnp.maximum(z, 0), top)


def tile_rows(vt):
    return slice(vt * 8, vt * 8 + 8)


def reader(g, main, halo):
    return lambda col, vt, z: halo[col, z] if vt == g.vt else main[col, z, tile_rows(vt), :]


def put(g, main, halo, z, values):
    for (col, vt), value in values.items():
        if vt == g.vt:
            halo[col, z] = value
        else:
            main[col, z, tile_rows(vt), :] = value


def interp_body(g, meta, table, below, strip, interp, interp_halo, nodes, nodes_halo):
    edge_z, edge_v = edges(meta)
    stencil = Stencil(g, edge_v)

    def take(source, z, target):
        for col in range(g.ct):
            lanes = slice(col * LANES, (col + 1) * LANES)
            nodes[col, target] = source[z, :, lanes]
            nodes_halo[col, target] = strip[target, :, lanes]

    @pl.loop(0, BLOCK_Z)
    def _(z):
        take(table, z, z)

    @pl.loop(0, ITERS)
    def _(z):
        take(below, z, BLOCK_Z + z)

    get = reader(g, nodes, nodes_halo)

    @pl.loop(0, LAYERS[0])
    def _(z):
        put(g, interp, interp_halo, z, stencil(get, z, layer_below(z, edge_z)))


PRODUCTS = 14


def spread_rows(values, count):
    rows = [jnp.sum(value, axis=0, keepdims=True) for value in values]
    rows += [jnp.zeros_like(rows[0])] * (-len(rows) % 8)
    column = jnp.sum(jnp.concatenate(rows, 0), axis=1, keepdims=True)
    lane = lax.broadcasted_iota(jnp.int32, (len(rows), 128), 1)
    row = lax.broadcasted_iota(jnp.int32, (len(rows), 128), 0)
    line = jnp.sum(jnp.where(lane == row, column, 0.0), axis=0, keepdims=True)
    return jnp.broadcast_to(line, (count, 128))


def fill_masks(g, meta, masks, iterations, left):
    for at, t in enumerate(iterations):
        for far in range(2):
            for pair in range(g.pairs):
                column = pair // g.ct * g.cb + pair % g.ct * 2 + far * g.blocks
                masks[at, far, pair] = jnp.where(pair_live(meta, t, column, left), 1.0, 0.0)


def halo_live(g, meta, iteration, left):
    first = 2 * g.blocks
    return [[pair_live(meta, iteration, first + far * g.cb + 2 * col, left) for col in range(g.ct)] for far in range(2)]


def segments(top, counts):
    result, high = [], top
    for count in counts:
        result.append((high - count + 1, high))
        high -= count
    return result


def convert(g, meta, t, held, offset, z, out, left):
    row = offset + z // 8 * 8 * PAIRS + z % 8
    for pair in range(g.pairs):
        vb, col = pair // g.ct, pair % g.ct
        tiles = []
        for half in range(2):
            owner = jnp.maximum(meta[t, vb * g.cb + 2 * col + half], 0)
            tiles.append(held[owner, pl.ds(row, PAIRS, stride=8), :])
        even, odd = pair_tiles(left, *tiles)
        out[col, z, pl.ds(vb * BLOCK_V, PAIRS, stride=2), :] = even
        out[col, z, pl.ds(vb * BLOCK_V + 1, PAIRS, stride=2), :] = odd


def between(z):
    return jnp.where((z >= 0) & (z < BLOCK_Z), 1.0, 0.0)


def pair_tile_rows(g, pair):
    return [tile_rows(vt) for vt in (pair // g.ct * 2, pair // g.ct * 2 + 1)]


def middle_body(g, meta, strips, interp_halo, data, interp_in,
                out, a0_out, a1_out, a2_out, ca0_out, ca1_out, cb1_out, halos, peaks,
                held, interp, f0, f1, f2, a0, a1, a2, b1, ca0, ca1, cb1, a0_halo, a1_halo, b1_halo, masks, sems, out_sems):
    f, a = (f0, f1, f2), (a0, a1, a2)
    split = BLOCK_Z // 2
    groups = ([], [])
    for t in range(3):
        first, middle, end = OFFSET[t], OFFSET[t] + ROWS // 2, OFFSET[t + 1]
        for group, rows in ((0, slice(middle, end)), (1, slice(first, middle))):
            groups[group].append(pltpu.make_async_copy(data.at[:, rows, :], held.at[:, rows, :], sems.at[2 * t + group]))
    for col in range(g.ct):
        for group, layers in ((0, slice(split, LAYERS[0])), (1, slice(0, split))):
            sem = sems.at[6 + 2 * col + group]
            groups[group].append(pltpu.make_async_copy(interp_in.at[col, layers], interp.at[col, layers], sem))
    for group in groups:
        for copy in group:
            copy.start()
    edge_z, edge_v = edges(meta)
    stencil = Stencil(g, edge_v)
    left = lane_ids() < HALF
    live0, live1 = halo_live(g, meta, 0, left), halo_live(g, meta, 1, left)
    fill_masks(g, meta, masks, (0, 1, 2), left)
    for col in range(g.ct):
        for z in range(LAYERS[0]):
            value = strip_tile(strips, z, col) - interp_halo[col, z]
            a0_halo[col, z] = jnp.where(live0[z >= BLOCK_Z][col], value, 0.0)
        for z in range(LAYERS[1]):
            value = strip_tile(strips, LAYERS[0] + z, col) - interp_halo[col, z]
            a1_halo[col, z] = jnp.where(live1[z >= BLOCK_Z][col], value, 0.0)
    peaks[...] = jnp.zeros_like(peaks)
    get0, get1, getb = reader(g, a0, a0_halo), reader(g, a1, a1_halo), reader(g, b1, b1_halo)
    top0, top1 = LAYERS[1] - 1, LAYERS[2] - 1
    for copy in groups[0]:
        copy.wait()

    @pl.loop(0, g.pairs)
    def _(pair):
        vb, col = pair // g.ct, pair % g.ct
        row = pl.multiple_of(vb * BLOCK_V, BLOCK_V)
        column = g.blocks + vb * g.cb + 2 * col
        for t in range(3):
            owners = [jnp.maximum(meta[t, column + half], 0) for half in range(2)]
            for z in range(BLOCK_Z, LAYERS[t]):
                at = OFFSET[t] + z * PAIRS
                even, odd = pair_tiles(left, *[held[owner, at : at + PAIRS, :] for owner in owners])
                f[t][col, z, pl.ds(row, PAIRS, stride=2), :] = even
                f[t][col, z, pl.ds(row + 1, PAIRS, stride=2), :] = odd
        for t in range(3):
            live = masks[t, 1, pair] > 0.5
            for z in range(BLOCK_Z, LAYERS[t]):
                for half in range(2):
                    rows = pl.ds(row + 8 * half, 8)
                    value = f[t][col, z, rows, :] - interp[col, z, rows, :]
                    a[t][col, z, rows, :] = jnp.where(live, value, 0.0)

    def step(i, carry):
        carry = list(carry)
        base = BLOCK_Z - 1 - i
        z = base + 3
        at = clip(z, top1)
        low = layer_below(at, edge_z)
        after_a = stencil(get1, at, low)
        after_b = stencil(getb, at, low)
        put(g, ca1, halos.at[1], at, after_a)
        put(g, cb1, halos.at[2], at, after_b)
        row = jnp.minimum(at, BLOCK_Z - 1)
        counts = between(z)
        inside = jnp.full(TILE, counts, F32) > 0.5
        for pair in range(g.pairs):
            col = pair % g.ct
            live = masks[2, 0, pair] * counts > 0.5
            for half, rows in enumerate(pair_tile_rows(g, pair)):
                vt = pair // g.ct * 2 + half
                one, two = a1[col, row, rows, :], jnp.where(inside, b1[col, row, rows, :], 0.0)
                carry[3] = carry[3] + one * two
                carry[4] = carry[4] + two * two
                parts = [a2[col, row, rows, :]] + [
                    jnp.where(live, value, 0.0) for value in (ca0[col, row, rows, :], after_a[col, vt], after_b[col, vt])
                ]
                slot = 5
                for m in range(4):
                    for n in range(max(m, 1), 4):
                        carry[slot] = carry[slot] + parts[m] * parts[n]
                        slot += 1
        at = clip(base + 2, top0)
        after = stencil(get0, at, layer_below(at, edge_z))
        put(g, ca0, halos.at[0], at, after)
        far = jnp.where(at >= BLOCK_Z, 1, 0)
        for (col, vt), value in after.items():
            if vt == g.vt:
                live = (live1[0][col] & (at < BLOCK_Z)) | (live1[1][col] & (at >= BLOCK_Z))
                b1_halo[col, at] = jnp.where(live, value, 0.0)
            else:
                mask = masks[1, far, vt // 2 * g.ct + col]
                b1[col, at, tile_rows(vt), :] = jnp.where(mask > 0.5, value, 0.0)
        at = clip(base + 1, BLOCK_Z - 1)
        counts = between(base + 1)
        for pair in range(g.pairs):
            col = pair % g.ct
            peak = peaks[pair]
            for rows in pair_tile_rows(g, pair):
                mean = interp[col, at, rows, :]
                for t in range(3):
                    value = jnp.where(masks[t, 0, pair] > 0.5, f[t][col, at, rows, :] - mean, 0.0)
                    a[t][col, at, rows, :] = value
                    counted = jnp.where(masks[t, 0, pair] * counts > 0.5, value, 0.0)
                    carry[t] = carry[t] + counted * counted
                    if t == 0:
                        peak = jnp.maximum(peak, jnp.abs(counted))
            peaks[pair] = peak
        at = clip(base, BLOCK_Z - 1)
        for t in range(3):
            convert(g, meta, t, held, OFFSET[t], at, f[t], left)
        return tuple(carry)

    carry = (jnp.zeros(TILE, F32),) * (3 + 11)
    writes = []
    outs = ((a0, a0_out, BLOCK_Z), (a1, a1_out, BLOCK_Z), (a2, a2_out, BLOCK_Z + 1),
            (ca0, ca0_out, BLOCK_Z + 1), (ca1, ca1_out, BLOCK_Z + 1), (cb1, cb1_out, BLOCK_Z + 1))
    bounds = (0, split, split + 5, BLOCK_Z + 3)
    for index in range(3):
        if index == 1:
            for copy in groups[1]:
                copy.wait()
        carry = lax.fori_loop(bounds[index], bounds[index + 1], step, carry)
        lowest = BLOCK_Z - bounds[index + 1] + 3
        highest = BLOCK_Z - bounds[index] + 2 if index else top1
        for which, (source, target, layers) in enumerate(outs):
            for col in range(g.ct):
                span = slice(lowest, min(highest + 1, layers))
                sem = out_sems.at[(index * 6 + which) * g.ct + col]
                writes.append(pltpu.make_async_copy(source.at[col, span], target.at[col, span], sem))
                writes[-1].start()
    values = [carry[0], carry[1], carry[3], carry[4], carry[2]] + list(carry[5:])
    out[...] = spread_rows(values, out.shape[0])
    for write in writes:
        write.wait()


def weight_of(total, count):
    return 1.0 / (1.0 + jnp.sqrt(jnp.maximum(total, 0.0) / count))


def lane_values(line, count):
    lane = lax.broadcasted_iota(jnp.int32, line.shape, 1)
    return [jnp.sum(jnp.where(lane == i, line, 0.0), axis=1, keepdims=True) for i in range(count)]


def live_cells(g, meta, iteration):
    return jnp.full((1, 1), meta[iteration, 122], jnp.int32).astype(F32) * F32(g.cells)


def three_weights(g, meta, parts):
    q = lane_values(jnp.sum(parts[...], axis=0, keepdims=True), PRODUCTS)
    w0 = weight_of(q[0], live_cells(g, meta, 0))
    w1 = weight_of(q[1] - 2.0 * w0 * q[2] + w0 * w0 * q[3], live_cells(g, meta, 1))
    f = [jnp.ones_like(w0), -w0, -w1, w0 * w1]
    total, at = jnp.zeros_like(w0), 4
    for i in range(4):
        for j in range(i, 4):
            total = total + (1.0 if i == j else 2.0) * f[i] * f[j] * q[at]
            at += 1
    return [jnp.broadcast_to(w, TILE) for w in (w0, w1, weight_of(total, live_cells(g, meta, 2)))]


def last_body(g, meta, parts, strips, interp_halo, halos_in, peaks0, a1_in, a2_in, interp_in, ca0_in, ca1_in, cb1_in,
              *rest):
    data, rest = rest[: g.zm], rest[g.zm :]
    (r2_out, r3_out, errors, out, weights,
     held, f3, a1, a2, interp, ca0, ca1, cb1, r2, r2_halo, change, r3, masks, peaks, sems, out_sems) = rest
    top = LAYERS[2] - 1
    chunks = segments(top, (5, 4, 4, 4))
    reads, at = [], 0
    for lowest, highest in chunks:
        group = []
        if not reads:
            for k in range(g.zm):
                group.append(pltpu.make_async_copy(data[k], held.at[k], sems.at[at]))
                at += 1
        for source, target, layers in ((ca0_in, ca0, BLOCK_Z + 1), (ca1_in, ca1, BLOCK_Z + 1), (cb1_in, cb1, BLOCK_Z + 1),
                                       (a1_in, a1, BLOCK_Z), (a2_in, a2, BLOCK_Z + 1), (interp_in, interp, BLOCK_Z)):
            for col in range(g.ct):
                span = slice(lowest, min(highest + 1, layers))
                group.append(pltpu.make_async_copy(source.at[col, span], target.at[col, span], sems.at[at]))
                at += 1
        reads.append(group)
    for group in reads:
        for copy in group:
            copy.start()
    edge_z, edge_v = edges(meta)
    stencil = Stencil(g, edge_v)
    left = lane_ids() < HALF
    fill_masks(g, meta, masks, (1, 2, 3), left)
    w0, w1, w2 = three_weights(g, meta, parts)
    w01 = w0 * w1
    weights[0], weights[1], weights[2] = w0, w1, w2
    live = halo_live(g, meta, 2, left)
    peaks[...] = jnp.zeros_like(peaks)
    first = sum(LAYERS[:2])
    for col in range(g.ct):
        for z in range(LAYERS[2]):
            value = interp_halo[col, z] + w0 * halos_in[0, col, z] + w1 * halos_in[1, col, z] - w01 * halos_in[2, col, z]
            r2_halo[col, z] = jnp.where(live[z >= BLOCK_Z][col], strip_tile(strips, first + z, col) - value, 0.0)
    get = reader(g, r2, r2_halo)

    def step(i, total):
        base = top - i
        z = base + 1
        at = clip(z, BLOCK_Z - 1)
        counts = between(z)
        after = stencil(get, at, layer_below(at, edge_z))
        for pair in range(g.pairs):
            col = pair % g.ct
            mask = masks[2, 0, pair] * counts > 0.5
            peak = peaks[2, pair]
            for half, rows in enumerate(pair_tile_rows(g, pair)):
                value = f3[col, at, rows, :] - interp[col, at, rows, :] - change[col, at, rows, :]
                value = jnp.where(mask, value - w2 * after[col, pair // g.ct * 2 + half], 0.0)
                r3[col, at, rows, :] = value
                total = total + value * value
                peak = jnp.maximum(peak, jnp.abs(value))
            peaks[2, pair] = peak
        at = clip(base, top)
        far = jnp.where(at >= BLOCK_Z, 1, 0)
        own = jnp.minimum(at, BLOCK_Z - 1)
        inside = jnp.full(TILE, between(at), F32) > 0.5
        for pair in range(g.pairs):
            col = pair % g.ct
            mask1, mask2 = masks[0, 0, pair] > 0.5, masks[1, far, pair] > 0.5
            peak1, peak2 = peaks[0, pair], peaks[1, pair]
            for rows in pair_tile_rows(g, pair):
                zero = w0 * ca0[col, at, rows, :]
                whole = zero + w1 * ca1[col, at, rows, :] - w01 * cb1[col, at, rows, :]
                change[col, at, rows, :] = whole
                value = a2[col, at, rows, :] - jnp.where(mask2, whole, 0.0)
                r2[col, at, rows, :] = value
                peak2 = jnp.maximum(peak2, jnp.where(inside, jnp.abs(value), 0.0))
                value = a1[col, own, rows, :] - jnp.where(mask1, zero, 0.0)
                peak1 = jnp.maximum(peak1, jnp.where(inside, jnp.abs(value), 0.0))
            peaks[0, pair] = peak1
            peaks[1, pair] = peak2
        convert(g, meta, ITERS - 1, held, 0, own, f3, left)
        return total

    total, start, writes = jnp.zeros(TILE, F32), 0, []
    for index, (lowest, highest) in enumerate(chunks):
        for copy in reads[index]:
            copy.wait()
        stop = top - lowest + 1 + (1 if lowest == 0 else 0)
        total = lax.fori_loop(start, stop, step, total)
        start = stop
        below = lowest + 1 if lowest else 0
        above = min((chunks[index - 1][0] if index else BLOCK_Z - 1), BLOCK_Z - 1)
        for which, (source, target, layers) in enumerate(
            ((r2, r2_out, slice(lowest, min(highest, BLOCK_Z - 1) + 1)), (r3, r3_out, slice(below, above + 1)))
        ):
            for col in range(g.ct):
                sem = out_sems.at[(index * 2 + which) * g.ct + col]
                writes.append(pltpu.make_async_copy(source.at[col, layers], target.at[col, layers], sem))
                writes[-1].start()

    line = spread_rows([total], 1)
    lane = lax.broadcasted_iota(jnp.int32, (1, 128), 1)
    lane_p = lax.broadcasted_iota(jnp.int32, (g.pairs, 128), 1)
    row_p = lax.broadcasted_iota(jnp.int32, (g.pairs, 128), 0)
    for i in range(ITERS):
        tiles = [peaks0[pair] if i == 0 else peaks[i - 1, pair] for pair in range(g.pairs)]
        rows = jnp.concatenate([jnp.max(tile, axis=0, keepdims=True) for tile in tiles], 0)
        found = jnp.zeros((1, 128), F32)
        for half in range(2):
            inside = lane_p // HALF == half
            column = jnp.max(jnp.where(inside, rows, 0.0), axis=1, keepdims=True)
            place = row_p // g.ct * g.cb + row_p % g.ct * 2 + half
            found = found + jnp.sum(jnp.where(lane_p == place, column, 0.0), axis=0, keepdims=True)
        errors[i : i + 1, :] = found
        line = jnp.where(lane == 1 + i, jnp.max(found, axis=1, keepdims=True), line)
    out[...] = jnp.broadcast_to(line, out.shape)
    for write in writes:
        write.wait()


def assemble_body(g, meta, weights, table_in, a0_in, a1_in, ca0_in, r2_in, grown_out,
                  table, a0, a1, ca0, r2, grown, masks, sems):
    copies = [pltpu.make_async_copy(table_in, table, sems.at[0])]
    for i, (source, target) in enumerate(((a0_in, a0), (a1_in, a1), (ca0_in, ca0), (r2_in, r2))):
        for col in range(g.ct):
            copies.append(pltpu.make_async_copy(source.at[col, 0:BLOCK_Z], target.at[col], sems.at[1 + i * g.ct + col]))
    for copy in copies:
        copy.start()
    fill_masks(g, meta, masks, (1,), lane_ids() < HALF)
    w0, w1, w2 = weights[0], weights[1], weights[2]
    w01 = w0 * w1
    for copy in copies:
        copy.wait()

    @pl.loop(0, BLOCK_Z)
    def _(z):
        for pair in range(g.pairs):
            col = pair % g.ct
            lanes = slice(col * LANES, (col + 1) * LANES)
            mask = masks[0, 0, pair] > 0.5
            for vt in (pair // g.ct * 2, pair // g.ct * 2 + 1):
                rows = tile_rows(vt)
                value = w0 * a0[col, z, rows, :] + w1 * a1[col, z, rows, :] + w2 * r2[col, z, rows, :]
                value = value - jnp.where(mask, w01 * ca0[col, z, rows, :], 0.0)
                grown[z, rows, lanes] = table[z, rows, lanes] + value

    write = pltpu.make_async_copy(grown, grown_out, sems.at[0])
    write.start()
    write.wait()


def finish_body(g, meta, parts, grown_in, r3_in, out_hbm, worst, grown, r3, out, sems, out_sems):
    quarter = BLOCK_Z // 4
    reads, at = [], 0
    for part in range(4):
        layers = slice(part * quarter, (part + 1) * quarter)
        group = [pltpu.make_async_copy(grown_in.at[layers], grown.at[layers], sems.at[at])]
        for col in range(g.ct):
            group.append(pltpu.make_async_copy(r3_in.at[col, layers], r3.at[col, layers], sems.at[at + 1 + col]))
        at += 1 + g.ct
        reads.append(group)
    for group in reads:
        for copy in group:
            copy.start()
    total = lane_values(jnp.sum(parts[...], axis=0, keepdims=True), 1)[0]
    w3 = jnp.broadcast_to(weight_of(total, live_cells(g, meta, 3)), TILE)
    line = jnp.max(parts[...], axis=0, keepdims=True)
    for i, value in enumerate(lane_values(line, 1 + ITERS)[1:]):
        worst[i] = jnp.max(value)
    writes = []
    for part in range(4):
        for copy in reads[part]:
            copy.wait()
        layers = slice(part * quarter, (part + 1) * quarter)
        for z in range(part * quarter, (part + 1) * quarter):
            for col in range(g.ct):
                lanes = slice(col * LANES, (col + 1) * LANES)
                for vt in range(g.vt):
                    rows = tile_rows(vt)
                    out[z, rows, lanes] = grown[z, rows, lanes] + w3 * r3[col, z, rows, :]
        writes.append(pltpu.make_async_copy(out.at[layers], out_hbm.at[layers], out_sems.at[part]))
        writes[-1].start()
    for write in writes:
        write.wait()


def index_table(g, assign):
    zm_here, zv_here = lax.axis_index("zm"), lax.axis_index("zv")
    me = zm_here * g.zv + zv_here
    slots = assign.reshape(ITERS, -1)
    owner = jnp.arange(slots.shape[1]) // g.slots // g.zv
    owner = jnp.where(jnp.arange(ITERS)[:, None] == ITERS - 1, owner ^ zm_here, owner)
    column = jnp.arange(2 * g.blocks + 2 * g.cb)
    here = column % g.blocks
    far = jnp.where(column < 2 * g.blocks, column // g.blocks, (column - 2 * g.blocks) // g.cb)
    local = jnp.where(column < 2 * g.blocks, here, (column - 2 * g.blocks) % g.cb)
    side = jnp.where(column < 2 * g.blocks, 0, 1)
    inside = (zm_here + far < g.zm) & (zv_here + side < g.zv)
    target = jnp.where(inside, (me + far * g.zv + side) * g.blocks + local, -2)
    found = jnp.max(jnp.where(slots[:, None, :] == target[None, :, None], owner[:, None, :], -1), axis=2)
    count = jnp.sum((slots >= 0).astype(jnp.int32), axis=1, keepdims=True)
    flags = jnp.stack([zm_here == g.zm - 1, zv_here == g.zv - 1]).astype(jnp.int32)
    gap = jnp.zeros((ITERS, 120 - found.shape[1]), jnp.int32)
    flags = jnp.broadcast_to(flags[None, :], (ITERS, 2))
    return jnp.concatenate([found, gap, flags, count, jnp.zeros((ITERS, 5), jnp.int32)], axis=1)


def to_all(rows):
    count = lax.axis_size("zm") * lax.axis_size("zv")
    return lax.all_to_all(rows.reshape(count, 1, 128), AXES, 0, 0, tiled=True).reshape(count, 128)


def from_next(value, axis):
    count = lax.axis_size(axis)
    return lax.ppermute(value, axis, [(i, i - 1) for i in range(1, count)])


def shards(table, refined, assign):
    g = Shape(table.shape, assign.shape, lax.axis_size("zm"), lax.axis_size("zv"))
    everyone = g.zm * g.zv
    part = functools.partial
    slots = assign.transpose(0, 2, 1).reshape(ITERS * g.slots, -1)
    views = refined.reshape(ITERS * g.slots, BLOCK_Z // 8, 8, PAIRS, LANES).transpose(0, 1, 3, 2, 4)
    views = views.reshape(ITERS * g.slots, ROWS, LANES)
    vmem = lambda *shape: pltpu.VMEM(shape, F32)
    main, halo = g.main, g.halo

    below = from_next(table[:ITERS], "zm")
    packed = call(
        part(pack_three_body, g), struct(g.zm, OFFSET[3], LANES), [SMEM, HBM], HBM,
        [pltpu.SMEM((ITERS, g.zm), jnp.int32), vmem(g.zm, OFFSET[3], LANES), dma(3 * g.zm), dma(3 * g.zm + 3)],
        WHOLE,
    )(slots, views)
    data = lax.all_to_all(packed, "zm", 0, 0, tiled=True)
    strip = from_next(jnp.concatenate([table[:, :8], below[:, :8]], 0), "zv")
    packed = call(
        part(pack_last_body, g), [struct(ROWS, LANES)] * g.zm, [SMEM, HBM], [VMEM] * g.zm,
        [pltpu.SMEM((ITERS, g.zm), jnp.int32), dma(g.zm)], PART,
    )(slots, views)
    last_data = [packed[0]]
    for k in range(1, g.zm):
        last_data.append(lax.ppermute(packed[k], "zm", [(i, i ^ k) for i in range(g.zm)]))
    meta = index_table(g, assign)
    interp, interp_halo = call(
        part(interp_body, g), [struct(*main(LAYERS[0])), struct(*halo(LAYERS[0]))],
        [SMEM] + [VMEM] * 3, [VMEM] * 2, [vmem(*main(DEEP)), vmem(*halo(DEEP))], PART,
    )(meta, table, below, strip)

    strips = call(
        part(strip_body, g), struct(sum(LAYERS[:3]), *TILE), [SMEM] + [HBM] * 3, VMEM,
        [vmem(3 * g.cb, LAYERS[0] * PAIRS, LANES), vmem(g.ct, sum(LAYERS[:3]), BLOCK_V, LANES), dma(6 * g.cb)],
        PART,
    )(meta, data, interp_halo, packed[0])
    strips = from_next(strips, "zv")
    own, more = struct(*main(BLOCK_Z)), struct(*main(LAYERS[2]))
    products, a0, a1, a2, ca0, ca1, cb1, halos, peaks0 = call(
        part(middle_body, g),
        [struct(everyone, 128), own, own, more, more, more, more, struct(3, *halo(LAYERS[1])), struct(g.pairs, *TILE)],
        [SMEM] + [VMEM] * 2 + [HBM] * 2, [VMEM] + [HBM] * 6 + [VMEM] * 2,
        [vmem(*data.shape), vmem(*main(LAYERS[0]))] + [vmem(*main(LAYERS[0] + 1))] * 10
        + [vmem(*halo(LAYERS[0] + 1))] * 3 + [vmem(3, 2, g.pairs, *TILE), dma(6 + 2 * g.ct), dma(18 * g.ct)],
        WHOLE,
    )(meta, strips, interp_halo, data, interp)
    products = to_all(products)
    r2, r3, errors, stats, weights = call(
        part(last_body, g), [own, own, struct(ITERS, 128), struct(everyone, 128), struct(3, *TILE)],
        [SMEM] + [VMEM] * 5 + [HBM] * (6 + g.zm), [HBM] * 2 + [VMEM] * 3,
        [vmem(g.zm, ROWS, LANES), vmem(*main(BLOCK_Z)), vmem(*main(BLOCK_Z)), vmem(*main(LAYERS[2])), vmem(*main(BLOCK_Z))]
        + [vmem(*main(LAYERS[2]))] * 4 + [vmem(*halo(LAYERS[2])), vmem(*main(LAYERS[2])), vmem(*main(BLOCK_Z)),
           vmem(3, 2, g.pairs, *TILE), vmem(3, g.pairs, *TILE), dma(g.zm + 24 * g.ct), dma(8 * g.ct)],
        WHOLE,
    )(meta, products, strips, interp_halo, halos, peaks0, a1, a2, interp, ca0, ca1, cb1, *last_data)
    stats = to_all(stats)
    grown = call(
        part(assemble_body, g), struct(*table.shape), [SMEM, VMEM] + [HBM] * 5, HBM,
        [vmem(*table.shape)] + [vmem(*main(BLOCK_Z))] * 4 + [vmem(*table.shape), vmem(1, 2, g.pairs, *TILE), dma(1 + 4 * g.ct)],
        WHOLE,
    )(meta, weights, table, a0, a1, ca0, r2)
    table_out, worst = call(
        part(finish_body, g), [struct(*table.shape), struct(ITERS)], [SMEM, VMEM] + [HBM] * 2, [HBM, SMEM],
        [vmem(*table.shape), vmem(*main(BLOCK_Z)), vmem(*table.shape), dma(4 * (1 + g.ct)), dma(4)], WHOLE,
    )(meta, stats, grown, r3)
    return (table_out, errors[:, : g.blocks], worst)


def solution(mesh):
    in_specs = (P("zm", "zv", None), P(None, ("zm", "zv"), None, None), P())
    out_specs = (P("zm", "zv", None), P(None, ("zm", "zv")), P())

    return jax.shard_map(shards, mesh=mesh, in_specs=in_specs, out_specs=out_specs, check_vma=False)
```

```python
import functools

import jax
import jax.numpy as jnp
from jax import lax
from jax.experimental import pallas as pl
from jax.experimental.pallas import tpu as pltpu
from jax.sharding import PartitionSpec as P


S = 8
BLOCK_Z = 16
BLOCK_V = 16
BLOCK_C = 8
ITERS = 4
HALF = BLOCK_C * S
PAIRS = BLOCK_V // 2
LANES = 2 * HALF
ROWS = BLOCK_Z * PAIRS
DEEP = BLOCK_Z + ITERS
AXES = ("zm", "zv")
F32 = jnp.float32
TILE = (PAIRS, LANES)


def halo_rows(iteration):
    return ITERS - 1 - iteration


LAYERS = [BLOCK_Z + halo_rows(i) for i in range(ITERS)]
OFFSET = [sum(LAYERS[:i]) * PAIRS for i in range(ITERS)]


def lane_ids():
    return lax.broadcasted_iota(jnp.int32, TILE, 1)


def sub_ids():
    return lax.broadcasted_iota(jnp.int32, TILE, 0)


VMEM = pl.BlockSpec(memory_space=pltpu.VMEM)
SMEM = pl.BlockSpec(memory_space=pltpu.SMEM)
HBM = pl.BlockSpec(memory_space=pltpu.HBM)
WHOLE = 60
PART = 24


def call(body, outs, in_specs, out_specs, scratch, limit, flops=2000000):
    return pl.pallas_call(
        body,
        out_shape=outs,
        in_specs=in_specs,
        out_specs=out_specs,
        scratch_shapes=list(scratch),
        compiler_params=pltpu.CompilerParams(vmem_limit_bytes=limit << 20),
        cost_estimate=pl.CostEstimate(flops=flops, bytes_accessed=1 << 20, transcendentals=0),
    )


def struct(*shape, dtype=F32):
    return jax.ShapeDtypeStruct(shape, dtype)


def dma(count):
    return pltpu.SemaphoreType.DMA((count,))


class Shape:
    def __init__(self, table, assign, zm_count, zv_count):
        self.zm, self.zv = zm_count, zv_count
        self.span, self.wide = table[1], table[2]
        self.vb = self.span // BLOCK_V
        self.cb = self.wide // HALF
        self.vt = self.span // 8
        self.ct = self.wide // LANES
        self.blocks = self.vb * self.cb
        self.pairs = self.vb * self.ct
        self.slots = assign[2]
        self.cells = BLOCK_Z * BLOCK_V * BLOCK_C * S

    def main(self, layers):
        return (self.ct, layers, self.span, LANES)

    def halo(self, layers):
        return (self.ct, layers, 8, LANES)


def fill_inverse(g, iterations, assign, inverse):
    me = lax.axis_index("zm") * g.zv + lax.axis_index("zv")
    for t in iterations:
        for peer in range(g.zm):
            inverse[t, peer] = 0
        for slot in range(g.slots):
            block = assign[t * g.slots + slot, me]

            @pl.when(block >= 0)
            def _():
                inverse[t, block // (g.blocks * g.zv)] = slot


def pack_three_body(g, assign, refined, table, out, top, inverse, held, extras, rows_held, sems, out_sems):
    three = range(ITERS - 1)
    reads = [
        pltpu.make_async_copy(refined.at[i], held.at[i], sems.at[i]) for i in range(3 * g.slots)
    ]
    rows_in = pltpu.make_async_copy(table.at[0:ITERS], rows_held, sems.at[3 * g.slots])
    rows_out = pltpu.make_async_copy(rows_held, top, out_sems.at[3 * g.zm + 3])
    rows_in.start()
    for read in reads:
        read.start()
    fill_inverse(g, three, assign, inverse)
    rows_in.wait()
    rows_out.start()
    writes = []
    for t in three:
        for slot in range(g.slots):
            reads[t * g.slots + slot].wait()
        for peer in range(g.zm):
            source = held.at[t * g.slots + inverse[t, peer]]
            target = out.at[peer, OFFSET[t] : OFFSET[t] + ROWS, :]
            writes.append(pltpu.make_async_copy(source, target, out_sems.at[t * g.zm + peer]))
            writes[-1].start()
    for t in three:
        first = OFFSET[t] - t * ROWS
        for peer in range(g.zm):
            after = t * g.slots + inverse[t, min(peer + 1, g.zm - 1)]
            for z in range(halo_rows(t)):
                at = first + z * PAIRS
                extras[peer, at : at + PAIRS, :] = held[after, pl.ds(z, PAIRS, stride=8), :]
        count = halo_rows(t) * PAIRS
        target = out.at[:, OFFSET[t] + ROWS : OFFSET[t + 1], :]
        writes.append(pltpu.make_async_copy(extras.at[:, first : first + count, :], target, out_sems.at[3 * g.zm + t]))
        writes[-1].start()
    for write in writes:
        write.wait()
    rows_out.wait()


def pack_last_body(g, assign, refined, *rest):
    outs, inverse, sems = rest[: g.zm], rest[-2], rest[-1]
    t = ITERS - 1
    fill_inverse(g, [t], assign, inverse)
    here = lax.axis_index("zm")
    copies = []
    for k in range(g.zm):
        source = refined.at[t * g.slots + inverse[t, here ^ k]]
        copies.append(pltpu.make_async_copy(source, outs[k], sems.at[k]))
    for copy in copies:
        copy.start()
    for copy in copies:
        copy.wait()


def pair_tiles(left, first, second):
    even = jnp.where(left, first, pltpu.roll(second, HALF, 1))
    odd = jnp.where(left, pltpu.roll(first, HALF, 1), second)
    return even, odd


def pair_live(meta, iteration, column, left):
    first, second = meta[iteration, column] >= 0, meta[iteration, column + 1] >= 0
    return (left & first) | (~left & second)


def strip_body(g, meta, data, unused_a, unused_b, out, held, planes, sems):
    three = range(ITERS - 1)
    left, sub = lane_ids() < HALF, sub_ids()
    two = 2 * 8

    def copies(t, c):
        at, mine = t * g.cb + c, jnp.maximum(meta[t, c], 0)
        far = data.at[jnp.maximum(meta[t, g.blocks + c], 0), OFFSET[t] + ROWS : OFFSET[t] + LAYERS[t] * PAIRS, :]
        result = [pltpu.make_async_copy(far, held.at[at, 2 * two : 2 * two + halo_rows(t) * PAIRS, :], sems.at[3 * at])]
        for zt in range(2):
            first = OFFSET[t] + zt * 8 * PAIRS
            source = data.at[mine, first : first + two, :]
            result.append(pltpu.make_async_copy(source, held.at[at, zt * two : zt * two + two, :], sems.at[3 * at + 1 + zt]))
        return result

    for t in three:
        for c in range(g.cb):
            for copy in copies(t, c):
                copy.start()
    for t in three:
        for c in range(g.cb):
            for copy in copies(t, c):
                copy.wait()
        first = sum(LAYERS[:t])
        for z in range(LAYERS[t]):
            for col in range(g.ct):
                tiles = []
                for c in (2 * col, 2 * col + 1):
                    if z < BLOCK_Z:
                        tiles.append(held[t * g.cb + c, pl.ds(z // 8 * two + z % 8, PAIRS, stride=8), :])
                    else:
                        at = 2 * two + (z - BLOCK_Z) * PAIRS
                        tiles.append(held[t * g.cb + c, at : at + PAIRS, :])
                even, odd = pair_tiles(left, *tiles)
                planes[col, first + z, pl.ds(0, PAIRS, stride=2), :] = even
                planes[col, first + z, pl.ds(1, PAIRS, stride=2), :] = odd
        if t == 0:
            for z in range(LAYERS[0]):
                out[z] = jnp.where(sub < 4, planes[0, z, 0:8, :], pltpu.roll(planes[1, z, 0:8, :], 4, 0))
    for z in range(LAYERS[1]):
        one, two_at = LAYERS[0] + z, LAYERS[0] + LAYERS[1] + min(z, LAYERS[2] - 1)
        low = jnp.where(sub < 2, planes[0, one, 0:8, :], pltpu.roll(planes[1, one, 0:8, :], 2, 0))
        high = pltpu.roll(planes[0, two_at, 0:8, :], 4, 0)
        high = jnp.where(sub < 6, high, pltpu.roll(planes[1, two_at, 0:8, :], 6, 0))
        out[LAYERS[0] + z] = jnp.where(sub < 4, low, high)


def strip_tile(strips, t, z, col):
    tile = strips[z] if t == 0 else strips[LAYERS[0] + z]
    shift = (4 * col, 2 * col, 4 + 2 * col)[t]
    return pltpu.roll(tile, 8 - shift, 0) if shift else tile


class Stencil:
    def __init__(self, g, edge):
        self.g = g
        lane, sub = lane_ids(), sub_ids()
        self.inner = lane < LANES - S
        self.above = sub < 7
        self.last = edge & (sub == 7)

    def __call__(self, get, z, low):
        g = self.g
        sums, turned = {}, {}
        for vt in range(g.vt + 1):
            for col in range(g.ct):
                sums[col, vt] = get(col, vt, z) + get(col, vt, low)
                turned[col, vt] = pltpu.roll(sums[col, vt], LANES - S, 1)
        both, up = {}, {}
        for vt in range(g.vt + 1):
            for col in range(g.ct):
                beside = sums[col, vt] if col == g.ct - 1 else turned[col + 1, vt]
                both[col, vt] = sums[col, vt] + jnp.where(self.inner, turned[col, vt], beside)
                up[col, vt] = pltpu.roll(both[col, vt], 7, 0)
        result = {}
        for vt in range(g.vt + 1):
            for col in range(g.ct):
                value = up[col, vt]
                if vt < g.vt:
                    value = jnp.where(self.above, value, up[col, vt + 1])
                if vt == g.vt - 1:
                    value = jnp.where(self.last, both[col, vt], value)
                result[col, vt] = 0.125 * (both[col, vt] + value)
        return result


def edges(meta):
    return meta[0, 120] == 1, meta[0, 121] == 1


def layer_below(z, edge):
    return jnp.where((z == BLOCK_Z - 1) & edge, z, z + 1)


def clip(z, top):
    return jnp.minimum(jnp.maximum(z, 0), top)


def tile_rows(vt):
    return slice(vt * 8, vt * 8 + 8)


def reader(g, main, halo):
    return lambda col, vt, z: halo[col, z] if vt == g.vt else main[col, z, tile_rows(vt), :]


def put(g, main, halo, z, values):
    for (col, vt), value in values.items():
        if vt == g.vt:
            halo[col, z] = value
        else:
            main[col, z, tile_rows(vt), :] = value


def interp_body(g, meta, table, below, strip, interp, interp_halo, nodes, nodes_halo):
    edge_z, edge_v = edges(meta)
    stencil = Stencil(g, edge_v)

    def take(source, z, target):
        for col in range(g.ct):
            lanes = slice(col * LANES, (col + 1) * LANES)
            nodes[col, target] = source[z, :, lanes]
            nodes_halo[col, target] = strip[target, :, lanes]

    @pl.loop(0, BLOCK_Z)
    def _(z):
        take(table, z, z)

    @pl.loop(0, ITERS)
    def _(z):
        take(below, z, BLOCK_Z + z)

    get = reader(g, nodes, nodes_halo)

    @pl.loop(0, LAYERS[0])
    def _(z):
        put(g, interp, interp_halo, z, stencil(get, z, layer_below(z, edge_z)))


PRODUCTS = 14


def spread_rows(values, count):
    rows = [jnp.sum(value, axis=0, keepdims=True) for value in values]
    rows += [jnp.zeros_like(rows[0])] * (-len(rows) % 8)
    column = jnp.sum(jnp.concatenate(rows, 0), axis=1, keepdims=True)
    lane = lax.broadcasted_iota(jnp.int32, (len(rows), 128), 1)
    row = lax.broadcasted_iota(jnp.int32, (len(rows), 128), 0)
    line = jnp.sum(jnp.where(lane == row, column, 0.0), axis=0, keepdims=True)
    return jnp.broadcast_to(line, (count, 128))


def fill_masks(g, meta, masks, iterations, left):
    for at, t in enumerate(iterations):
        for far in range(2):
            for pair in range(g.pairs):
                column = pair // g.ct * g.cb + pair % g.ct * 2 + far * g.blocks
                masks[at, far, pair] = jnp.where(pair_live(meta, t, column, left), 1.0, 0.0)


def halo_live(g, meta, iteration, left):
    first = 2 * g.blocks
    return [[pair_live(meta, iteration, first + far * g.cb + 2 * col, left) for col in range(g.ct)] for far in range(2)]


def segments(top, counts):
    result, high = [], top
    for count in counts:
        result.append((high - count + 1, high))
        high -= count
    return result


def convert(g, meta, t, held, offset, z, out, left):
    row = offset + z // 8 * 8 * PAIRS + z % 8
    for pair in range(g.pairs):
        vb, col = pair // g.ct, pair % g.ct
        tiles = []
        for half in range(2):
            owner = jnp.maximum(meta[t, vb * g.cb + 2 * col + half], 0)
            tiles.append(held[owner, pl.ds(row, PAIRS, stride=8), :])
        even, odd = pair_tiles(left, *tiles)
        out[col, z, pl.ds(vb * BLOCK_V, PAIRS, stride=2), :] = even
        out[col, z, pl.ds(vb * BLOCK_V + 1, PAIRS, stride=2), :] = odd


def between(z):
    return jnp.where((z >= 0) & (z < BLOCK_Z), 1.0, 0.0)


def pair_tile_rows(g, pair):
    return [tile_rows(vt) for vt in (pair // g.ct * 2, pair // g.ct * 2 + 1)]


def local_body(g, meta, data, interp_in, a0_out, a1_out, a2_out, totals, peaks,
               held, interp, f0, f1, f2, a0, a1, a2, masks, sems, out_sems):
    f, a, outs = (f0, f1, f2), (a0, a1, a2), (a0_out, a1_out, a2_out)
    split = BLOCK_Z // 2
    groups = ([], [])
    for t in range(3):
        first, middle, end = OFFSET[t], OFFSET[t] + ROWS // 2, OFFSET[t + 1]
        for group, rows in ((0, slice(middle, end)), (1, slice(first, middle))):
            groups[group].append(pltpu.make_async_copy(data.at[:, rows, :], held.at[:, rows, :], sems.at[2 * t + group]))
    for col in range(g.ct):
        for group, layers in ((0, slice(split, LAYERS[0])), (1, slice(0, split))):
            sem = sems.at[6 + 2 * col + group]
            groups[group].append(pltpu.make_async_copy(interp_in.at[col, layers], interp.at[col, layers], sem))
    for group in groups:
        for copy in group:
            copy.start()
    left = lane_ids() < HALF
    fill_masks(g, meta, masks, (0, 1, 2), left)
    peaks[...] = jnp.zeros_like(peaks)
    for copy in groups[0]:
        copy.wait()

    @pl.loop(0, g.pairs)
    def _(pair):
        vb, col = pair // g.ct, pair % g.ct
        row = pl.multiple_of(vb * BLOCK_V, BLOCK_V)
        column = g.blocks + vb * g.cb + 2 * col
        for t in range(3):
            owners = [jnp.maximum(meta[t, column + half], 0) for half in range(2)]
            for z in range(BLOCK_Z, LAYERS[t]):
                at = OFFSET[t] + z * PAIRS
                even, odd = pair_tiles(left, *[held[owner, at : at + PAIRS, :] for owner in owners])
                f[t][col, z, pl.ds(row, PAIRS, stride=2), :] = even
                f[t][col, z, pl.ds(row + 1, PAIRS, stride=2), :] = odd
        for t in range(3):
            live = masks[t, 1, pair] > 0.5
            for z in range(BLOCK_Z, LAYERS[t]):
                for half in range(2):
                    rows = pl.ds(row + 8 * half, 8)
                    value = f[t][col, z, rows, :] - interp[col, z, rows, :]
                    a[t][col, z, rows, :] = jnp.where(live, value, 0.0)

    def step(i, carry):
        carry = list(carry)
        base = BLOCK_Z - 1 - i
        at = clip(base + 1, BLOCK_Z - 1)
        inside = jnp.full(TILE, between(base + 1), F32) > 0.5
        for pair in range(g.pairs):
            col = pair % g.ct
            peak = peaks[pair]
            for rows in pair_tile_rows(g, pair):
                mean = interp[col, at, rows, :]
                for t in range(3):
                    live = (masks[t, 0, pair] > 0.5) & inside
                    value = jnp.where(live, f[t][col, at, rows, :] - mean, 0.0)
                    a[t][col, at, rows, :] = value
                    carry[t] = carry[t] + value * value
                    if t == 0:
                        peak = jnp.maximum(peak, jnp.abs(value))
            peaks[pair] = peak
        at = clip(base, BLOCK_Z - 1)
        for t in range(3):
            convert(g, meta, t, held, OFFSET[t], at, f[t], left)
        return tuple(carry)

    carry = (jnp.zeros(TILE, F32),) * 3
    writes, bounds = [], (0, split, split + 5, BLOCK_Z + 1)
    for index in range(3):
        if index == 1:
            for copy in groups[1]:
                copy.wait()
        carry = lax.fori_loop(bounds[index], bounds[index + 1], step, carry)
        lowest = BLOCK_Z - bounds[index + 1] + 1
        for t in range(3):
            highest = BLOCK_Z - bounds[index] if index else LAYERS[t] - 1
            for col in range(g.ct):
                span = slice(lowest, highest + 1)
                sem = out_sems.at[(index * 3 + t) * g.ct + col]
                writes.append(pltpu.make_async_copy(a[t].at[col, span], outs[t].at[col, span], sem))
                writes[-1].start()
    for t in range(3):
        totals[t] = carry[t]
    for write in writes:
        write.wait()


def middle_body(g, meta, strips, interp_halo, totals, a0_in, a1_in, a2_in,
                out, ca0_out, ca1_out, cb1_out, halos,
                a0, a1, a2, b1, ca0, ca1, cb1, a0_halo, a1_halo, b1_halo, masks, sems, out_sems):
    split = BLOCK_Z // 2
    groups, at = ([], []), 0
    for source, target, layers in ((a0_in, a0, LAYERS[0]), (a1_in, a1, LAYERS[1]), (a2_in, a2, BLOCK_Z)):
        for col in range(g.ct):
            for group, span in ((0, slice(split, layers)), (1, slice(0, split))):
                groups[group].append(pltpu.make_async_copy(source.at[col, span], target.at[col, span], sems.at[at]))
                at += 1
    for group in groups:
        for copy in group:
            copy.start()
    edge_z, edge_v = edges(meta)
    stencil = Stencil(g, edge_v)
    left = lane_ids() < HALF
    live0, live1 = halo_live(g, meta, 0, left), halo_live(g, meta, 1, left)
    fill_masks(g, meta, masks, (1, 2), left)
    for pair in range(g.pairs):
        masks[1, 1, pair] = jnp.zeros(TILE, F32)
    for col in range(g.ct):
        for z in range(LAYERS[0]):
            value = strip_tile(strips, 0, z, col) - interp_halo[col, z]
            a0_halo[col, z] = jnp.where(live0[z >= BLOCK_Z][col], value, 0.0)
        for z in range(LAYERS[1]):
            value = strip_tile(strips, 1, z, col) - interp_halo[col, z]
            a1_halo[col, z] = jnp.where(live1[z >= BLOCK_Z][col], value, 0.0)
    get0, get1, getb = reader(g, a0, a0_halo), reader(g, a1, a1_halo), reader(g, b1, b1_halo)
    top0, top1 = LAYERS[1] - 1, LAYERS[2] - 1
    none = LAYERS[0]
    for col in range(g.ct):
        for field in (a1, a2, b1, ca0):
            field[col, none] = jnp.zeros((g.span, LANES), F32)
    for copy in groups[0]:
        copy.wait()

    def step(i, carry):
        carry = list(carry)
        base = top0 - i
        z = base + 1
        at = clip(z, top1)
        low = layer_below(at, edge_z)
        after_a = stencil(get1, at, low)
        after_b = stencil(getb, at, low)
        put(g, ca1, halos.at[1], at, after_a)
        put(g, cb1, halos.at[2], at, after_b)
        own = (z >= 0) & (z < BLOCK_Z)
        row, kind = jnp.where(own, z, none), jnp.where(own, 0, 1)
        for pair in range(g.pairs):
            col = pair % g.ct
            live = masks[1, kind, pair] > 0.5
            for half, rows in enumerate(pair_tile_rows(g, pair)):
                vt = pair // g.ct * 2 + half
                one, two = a1[col, row, rows, :], b1[col, row, rows, :]
                carry[0] = carry[0] + one * two
                carry[1] = carry[1] + two * two
                parts = [a2[col, row, rows, :]] + [
                    jnp.where(live, value, 0.0) for value in (ca0[col, row, rows, :], after_a[col, vt], after_b[col, vt])
                ]
                slot = 2
                for m in range(4):
                    for n in range(max(m, 1), 4):
                        carry[slot] = carry[slot] + parts[m] * parts[n]
                        slot += 1
        at = clip(base, top0)
        after = stencil(get0, at, layer_below(at, edge_z))
        put(g, ca0, halos.at[0], at, after)
        far = jnp.where(at >= BLOCK_Z, 1, 0)
        for (col, vt), value in after.items():
            if vt == g.vt:
                live = (live1[0][col] & (at < BLOCK_Z)) | (live1[1][col] & (at >= BLOCK_Z))
                b1_halo[col, at] = jnp.where(live, value, 0.0)
            else:
                mask = masks[0, far, vt // 2 * g.ct + col]
                b1[col, at, tile_rows(vt), :] = jnp.where(mask > 0.5, value, 0.0)
        return tuple(carry)

    carry = (jnp.zeros(TILE, F32),) * 11
    writes = []
    bounds = (0, top0 - split + 1, top0 - split + 6, top0 + 2)
    for index in range(3):
        if index == 1:
            for copy in groups[1]:
                copy.wait()
        carry = lax.fori_loop(bounds[index], bounds[index + 1], step, carry)
        lowest = top0 - bounds[index + 1] + 2
        highest = top0 - bounds[index] + 1 if index else top1
        for which, (source, target) in enumerate(((ca0, ca0_out), (ca1, ca1_out), (cb1, cb1_out))):
            for col in range(g.ct):
                span = slice(lowest, highest + 1)
                sem = out_sems.at[(index * 3 + which) * g.ct + col]
                writes.append(pltpu.make_async_copy(source.at[col, span], target.at[col, span], sem))
                writes[-1].start()
    values = [totals[0], totals[1], carry[0], carry[1], totals[2]] + list(carry[2:])
    out[...] = spread_rows(values, out.shape[0])
    for write in writes:
        write.wait()


def weight_of(total, count):
    return 1.0 / (1.0 + jnp.sqrt(jnp.maximum(total, 0.0) / count))


def lane_values(line, count):
    lane = lax.broadcasted_iota(jnp.int32, line.shape, 1)
    return [jnp.sum(jnp.where(lane == i, line, 0.0), axis=1, keepdims=True) for i in range(count)]


def live_cells(g, meta, iteration):
    return jnp.full((1, 1), meta[iteration, 122], jnp.int32).astype(F32) * F32(g.cells)


def three_weights(g, meta, parts):
    q = lane_values(jnp.sum(parts[...], axis=0, keepdims=True), PRODUCTS)
    w0 = weight_of(q[0], live_cells(g, meta, 0))
    w1 = weight_of(q[1] - 2.0 * w0 * q[2] + w0 * w0 * q[3], live_cells(g, meta, 1))
    f = [jnp.ones_like(w0), -w0, -w1, w0 * w1]
    total, at = jnp.zeros_like(w0), 4
    for i in range(4):
        for j in range(i, 4):
            total = total + (1.0 if i == j else 2.0) * f[i] * f[j] * q[at]
            at += 1
    return [jnp.broadcast_to(w, TILE) for w in (w0, w1, weight_of(total, live_cells(g, meta, 2)))]


def last_body(g, meta, parts, strips, interp_halo, halos_in, peaks0, a0_in, a1_in, a2_in, interp_in, ca0_in, ca1_in, cb1_in,
              *rest):
    data, rest = rest[: g.zm], rest[g.zm :]
    (sum_hbm, r3_hbm, errors, out,
     held, f3, a0, a1, a2, interp, ca0, ca1, cb1, r2, r2_halo, change, sum_out, r3, masks, peaks, sems, out_sems) = rest
    top = LAYERS[2] - 1
    chunks = segments(top, (5, 4, 4, 4))
    reads, at = [], 0
    for lowest, highest in chunks:
        group = []
        if not reads:
            for k in range(g.zm):
                group.append(pltpu.make_async_copy(data[k], held.at[k], sems.at[at]))
                at += 1
        for source, target, layers in ((ca0_in, ca0, BLOCK_Z + 1), (ca1_in, ca1, BLOCK_Z + 1), (cb1_in, cb1, BLOCK_Z + 1),
                                       (a0_in, a0, BLOCK_Z), (a1_in, a1, BLOCK_Z), (a2_in, a2, BLOCK_Z + 1),
                                       (interp_in, interp, BLOCK_Z)):
            for col in range(g.ct):
                span = slice(lowest, min(highest + 1, layers))
                group.append(pltpu.make_async_copy(source.at[col, span], target.at[col, span], sems.at[at]))
                at += 1
        reads.append(group)
    for group in reads:
        for copy in group:
            copy.start()
    edge_z, edge_v = edges(meta)
    stencil = Stencil(g, edge_v)
    left = lane_ids() < HALF
    fill_masks(g, meta, masks, (1, 2, 3), left)
    w0, w1, w2 = three_weights(g, meta, parts)
    w01 = w0 * w1
    live = halo_live(g, meta, 2, left)
    peaks[...] = jnp.zeros_like(peaks)
    for col in range(g.ct):
        for z in range(LAYERS[2]):
            value = interp_halo[col, z] + w0 * halos_in[0, col, z] + w1 * halos_in[1, col, z] - w01 * halos_in[2, col, z]
            r2_halo[col, z] = jnp.where(live[z >= BLOCK_Z][col], strip_tile(strips, 2, z, col) - value, 0.0)
    get = reader(g, r2, r2_halo)

    def step(i, total):
        base = top - i
        z = base + 1
        at = clip(z, BLOCK_Z - 1)
        counts = between(z)
        after = stencil(get, at, layer_below(at, edge_z))
        for pair in range(g.pairs):
            col = pair % g.ct
            mask = masks[2, 0, pair] * counts > 0.5
            peak = peaks[2, pair]
            for half, rows in enumerate(pair_tile_rows(g, pair)):
                value = f3[col, at, rows, :] - interp[col, at, rows, :] - change[col, at, rows, :]
                value = jnp.where(mask, value - w2 * after[col, pair // g.ct * 2 + half], 0.0)
                r3[col, at, rows, :] = value
                total = total + value * value
                peak = jnp.maximum(peak, jnp.abs(value))
            peaks[2, pair] = peak
        at = clip(base, top)
        far = jnp.where(at >= BLOCK_Z, 1, 0)
        own = jnp.minimum(at, BLOCK_Z - 1)
        inside = jnp.full(TILE, between(at), F32) > 0.5
        for pair in range(g.pairs):
            col = pair % g.ct
            mask1, mask2 = masks[0, 0, pair] > 0.5, masks[1, far, pair] > 0.5
            peak1, peak2 = peaks[0, pair], peaks[1, pair]
            for rows in pair_tile_rows(g, pair):
                zero = w0 * ca0[col, at, rows, :]
                whole = zero + w1 * ca1[col, at, rows, :] - w01 * cb1[col, at, rows, :]
                change[col, at, rows, :] = whole
                value = a2[col, at, rows, :] - jnp.where(mask2, whole, 0.0)
                r2[col, at, rows, :] = value
                peak2 = jnp.maximum(peak2, jnp.where(inside, jnp.abs(value), 0.0))
                one = a1[col, own, rows, :] - jnp.where(mask1, zero, 0.0)
                peak1 = jnp.maximum(peak1, jnp.where(inside, jnp.abs(one), 0.0))
                sum_out[col, own, rows, :] = w0 * a0[col, own, rows, :] + w1 * one + w2 * value
            peaks[0, pair] = peak1
            peaks[1, pair] = peak2
        convert(g, meta, ITERS - 1, held, 0, own, f3, left)
        return total

    total, start, writes = jnp.zeros(TILE, F32), 0, []
    for index, (lowest, highest) in enumerate(chunks):
        for copy in reads[index]:
            copy.wait()
        stop = top - lowest + 1 + (1 if lowest == 0 else 0)
        total = lax.fori_loop(start, stop, step, total)
        start = stop
        below = lowest + 1 if lowest else 0
        above = min((chunks[index - 1][0] if index else BLOCK_Z - 1), BLOCK_Z - 1)
        for which, (source, target, layers) in enumerate(
            ((sum_out, sum_hbm, slice(lowest, min(highest, BLOCK_Z - 1) + 1)), (r3, r3_hbm, slice(below, above + 1)))
        ):
            for col in range(g.ct):
                sem = out_sems.at[(index * 2 + which) * g.ct + col]
                writes.append(pltpu.make_async_copy(source.at[col, layers], target.at[col, layers], sem))
                writes[-1].start()

    line = spread_rows([total], 1)
    lane = lax.broadcasted_iota(jnp.int32, (1, 128), 1)
    lane_p = lax.broadcasted_iota(jnp.int32, (g.pairs, 128), 1)
    row_p = lax.broadcasted_iota(jnp.int32, (g.pairs, 128), 0)
    for i in range(ITERS):
        tiles = [peaks0[pair] if i == 0 else peaks[i - 1, pair] for pair in range(g.pairs)]
        rows = jnp.concatenate([jnp.max(tile, axis=0, keepdims=True) for tile in tiles], 0)
        found = jnp.zeros((1, 128), F32)
        for half in range(2):
            inside = lane_p // HALF == half
            column = jnp.max(jnp.where(inside, rows, 0.0), axis=1, keepdims=True)
            place = row_p // g.ct * g.cb + row_p % g.ct * 2 + half
            found = found + jnp.sum(jnp.where(lane_p == place, column, 0.0), axis=0, keepdims=True)
        errors[i : i + 1, :] = found
        line = jnp.where(lane == 1 + i, jnp.max(found, axis=1, keepdims=True), line)
    out[...] = jnp.broadcast_to(line, out.shape)
    for write in writes:
        write.wait()


def finish_body(g, meta, parts, table_in, change_in, r3_in, out_hbm, worst, table, change, r3, out, sems, out_sems):
    quarter = BLOCK_Z // 4
    spans = [slice(part * quarter, (part + 1) * quarter) for part in range(4)]
    reads = []
    for part, span in enumerate(spans):
        at = part * (1 + 2 * g.ct)
        group = [pltpu.make_async_copy(table_in.at[span], table.at[span], sems.at[at])]
        for col in range(g.ct):
            at += 2
            group.append(pltpu.make_async_copy(change_in.at[col, span], change.at[col, span], sems.at[at - 1]))
            group.append(pltpu.make_async_copy(r3_in.at[col, span], r3.at[col, span], sems.at[at]))
        reads.append(group)
    for group in reads:
        for read in group:
            read.start()
    total = lane_values(jnp.sum(parts[...], axis=0, keepdims=True), 1)[0]
    w3 = jnp.broadcast_to(weight_of(total, live_cells(g, meta, 3)), TILE)
    writes = []
    for part, span in enumerate(spans):
        for read in reads[part]:
            read.wait()
        for z in range(part * quarter, (part + 1) * quarter):
            for col in range(g.ct):
                lanes = slice(col * LANES, (col + 1) * LANES)
                for vt in range(g.vt):
                    rows = tile_rows(vt)
                    out[z, rows, lanes] = table[z, rows, lanes] + (change[col, z, rows, :] + w3 * r3[col, z, rows, :])
        writes.append(pltpu.make_async_copy(out.at[span], out_hbm.at[span], out_sems.at[part]))
        writes[-1].start()
    line = jnp.max(parts[...], axis=0, keepdims=True)
    for i, value in enumerate(lane_values(line, 1 + ITERS)[1:]):
        worst[i] = jnp.max(value)
    for write in writes:
        write.wait()


def index_table(g, assign):
    zm_here, zv_here = lax.axis_index("zm"), lax.axis_index("zv")
    me = zm_here * g.zv + zv_here
    slots = assign.reshape(ITERS, -1)
    owner = jnp.arange(slots.shape[1]) // g.slots // g.zv
    owner = jnp.where(jnp.arange(ITERS)[:, None] == ITERS - 1, owner ^ zm_here, owner)
    column = jnp.arange(2 * g.blocks + 2 * g.cb)
    here = column % g.blocks
    far = jnp.where(column < 2 * g.blocks, column // g.blocks, (column - 2 * g.blocks) // g.cb)
    local = jnp.where(column < 2 * g.blocks, here, (column - 2 * g.blocks) % g.cb)
    side = jnp.where(column < 2 * g.blocks, 0, 1)
    inside = (zm_here + far < g.zm) & (zv_here + side < g.zv)
    target = jnp.where(inside, (me + far * g.zv + side) * g.blocks + local, -2)
    found = jnp.max(jnp.where(slots[:, None, :] == target[None, :, None], owner[:, None, :], -1), axis=2)
    count = jnp.sum((slots >= 0).astype(jnp.int32), axis=1, keepdims=True)
    flags = jnp.stack([zm_here == g.zm - 1, zv_here == g.zv - 1]).astype(jnp.int32)
    gap = jnp.zeros((ITERS, 120 - found.shape[1]), jnp.int32)
    flags = jnp.broadcast_to(flags[None, :], (ITERS, 2))
    return jnp.concatenate([found, gap, flags, count, jnp.zeros((ITERS, 5), jnp.int32)], axis=1)


def to_all(rows):
    count = lax.axis_size("zm") * lax.axis_size("zv")
    return lax.all_to_all(rows.reshape(count, 1, 128), AXES, 0, 0, tiled=True).reshape(count, 128)


def from_next(value, axis):
    count = lax.axis_size(axis)
    return lax.ppermute(value, axis, [(i, i - 1) for i in range(1, count)])


def shards(table, refined, assign):
    g = Shape(table.shape, assign.shape, lax.axis_size("zm"), lax.axis_size("zv"))
    everyone = g.zm * g.zv
    part = functools.partial
    slots = assign.transpose(0, 2, 1).reshape(ITERS * g.slots, -1)
    views = refined.reshape(ITERS * g.slots, BLOCK_Z // 8, 8, PAIRS, LANES).transpose(0, 1, 3, 2, 4)
    views = views.reshape(ITERS * g.slots, ROWS, LANES)
    vmem = lambda *shape: pltpu.VMEM(shape, F32)
    main, halo = g.main, g.halo

    packed, top = call(
        part(pack_three_body, g), [struct(g.zm, OFFSET[3], LANES), struct(ITERS, *table.shape[1:])], [SMEM, HBM, HBM], [HBM] * 2,
        [pltpu.SMEM((ITERS, g.zm), jnp.int32), vmem(3 * g.slots, ROWS, LANES), vmem(g.zm, OFFSET[3] - 3 * ROWS, LANES),
         vmem(ITERS, *table.shape[1:]), dma(3 * g.slots + 1), dma(3 * g.zm + 4)],
        WHOLE,
    )(slots, views, table)
    below = from_next(top, "zm")
    data = lax.all_to_all(packed, "zm", 0, 0, tiled=True)
    strip = jnp.concatenate([table[:, :8], below[:, :8]], 0)
    strip = from_next(strip, "zv")
    packed = call(
        part(pack_last_body, g), [struct(ROWS, LANES)] * g.zm, [SMEM, HBM], [VMEM] * g.zm,
        [pltpu.SMEM((ITERS, g.zm), jnp.int32), dma(g.zm)], WHOLE,
    )(slots, views)
    last_data = [packed[0]]
    for k in range(1, g.zm):
        last_data.append(lax.ppermute(packed[k], "zm", [(i, i ^ k) for i in range(g.zm)]))
    meta = index_table(g, assign)
    interp, interp_halo = call(
        part(interp_body, g), [struct(*main(LAYERS[0])), struct(*halo(LAYERS[0]))],
        [SMEM] + [VMEM] * 3, [VMEM] * 2, [vmem(*main(DEEP)), vmem(*halo(DEEP))], PART,
    )(meta, table, below, strip)

    strips = call(
        part(strip_body, g), struct(sum(LAYERS[:2]), *TILE), [SMEM] + [HBM] * 3, VMEM,
        [vmem(3 * g.cb, ROWS, LANES), vmem(g.ct, sum(LAYERS[:3]), BLOCK_V, LANES), dma(9 * g.cb)],
        PART,
    )(meta, data, interp_halo, packed[0])
    strips = from_next(strips, "zv")
    own, more, most = struct(*main(BLOCK_Z)), struct(*main(LAYERS[2])), struct(*main(LAYERS[1]))
    a0, a1, a2, totals, peaks0 = call(
        part(local_body, g), [struct(*main(LAYERS[0])), most, more, struct(3, *TILE), struct(g.pairs, *TILE)],
        [SMEM] + [HBM] * 2, [HBM] * 3 + [VMEM] * 2,
        [vmem(*data.shape)] + [vmem(*main(LAYERS[0]))] * 7
        + [vmem(3, 2, g.pairs, *TILE), dma(6 + 2 * g.ct), dma(9 * g.ct)], WHOLE,
    )(meta, data, interp)
    products, ca0, ca1, cb1, halos = call(
        part(middle_body, g), [struct(everyone, 128), more, more, more, struct(3, *halo(LAYERS[1]))],
        [SMEM] + [VMEM] * 3 + [HBM] * 3, [VMEM] + [HBM] * 3 + [VMEM],
        [vmem(*main(LAYERS[0] + 1))] * 7 + [vmem(*halo(LAYERS[0] + 1))] * 3
        + [vmem(2, 2, g.pairs, *TILE), dma(6 * g.ct), dma(9 * g.ct)],
        WHOLE,
    )(meta, strips, interp_halo, totals, a0, a1, a2)
    products = to_all(products)
    change, r3, errors, stats = call(
        part(last_body, g), [own, own, struct(ITERS, 128), struct(everyone, 128)],
        [SMEM] + [VMEM] * 5 + [HBM] * (7 + g.zm), [HBM] * 2 + [VMEM] * 2,
        [vmem(g.zm, ROWS, LANES)] + [vmem(*main(BLOCK_Z))] * 3 + [vmem(*main(LAYERS[2])), vmem(*main(BLOCK_Z))]
        + [vmem(*main(LAYERS[2]))] * 4 + [vmem(*halo(LAYERS[2])), vmem(*main(LAYERS[2]))]
        + [vmem(*main(BLOCK_Z))] * 2
        + [vmem(3, 2, g.pairs, *TILE), vmem(3, g.pairs, *TILE), dma(g.zm + 28 * g.ct), dma(8 * g.ct)],
        WHOLE,
    )(meta, products, strips, interp_halo, halos, peaks0, a0, a1, a2, interp, ca0, ca1, cb1, *last_data)
    stats = to_all(stats)
    table_out, worst = call(
        part(finish_body, g), [struct(*table.shape), struct(ITERS)], [SMEM, VMEM] + [HBM] * 3, [HBM, SMEM],
        [vmem(*table.shape)] + [vmem(*main(BLOCK_Z))] * 2 + [vmem(*table.shape), dma(4 * (1 + 2 * g.ct)), dma(4)],
        WHOLE,
    )(meta, stats, table, change, r3)
    return (table_out, errors[:, : g.blocks], worst)


def solution(mesh):
    in_specs = (P("zm", "zv", None), P(None, ("zm", "zv"), None, None), P())
    out_specs = (P("zm", "zv", None), P(None, ("zm", "zv")), P())

    return jax.shard_map(shards, mesh=mesh, in_specs=in_specs, out_specs=out_specs, check_vma=False)
```

```python
import functools

import jax
import jax.numpy as jnp
from jax import lax
from jax.experimental import pallas as pl
from jax.experimental.pallas import tpu as pltpu
from jax.sharding import PartitionSpec as P


S = 8
BLOCK_Z = 16
BLOCK_V = 16
BLOCK_C = 8
ITERS = 4
HALF = BLOCK_C * S
PAIRS = BLOCK_V // 2
LANES = 2 * HALF
ROWS = BLOCK_Z * PAIRS
DEEP = BLOCK_Z + ITERS
AXES = ("zm", "zv")
F32 = jnp.float32
TILE = (PAIRS, LANES)


def halo_rows(iteration):
    return ITERS - 1 - iteration


LAYERS = [BLOCK_Z + halo_rows(i) for i in range(ITERS)]
OFFSET = [sum(LAYERS[:i]) * PAIRS for i in range(ITERS)]


def lane_ids():
    return lax.broadcasted_iota(jnp.int32, TILE, 1)


def sub_ids():
    return lax.broadcasted_iota(jnp.int32, TILE, 0)


VMEM = pl.BlockSpec(memory_space=pltpu.VMEM)
SMEM = pl.BlockSpec(memory_space=pltpu.SMEM)
HBM = pl.BlockSpec(memory_space=pltpu.HBM)
WHOLE = 53.5
PART = 24


def call(body, outs, in_specs, out_specs, scratch, limit, flops=2000000):
    return pl.pallas_call(
        body,
        out_shape=outs,
        in_specs=in_specs,
        out_specs=out_specs,
        scratch_shapes=list(scratch),
        compiler_params=pltpu.CompilerParams(vmem_limit_bytes=int(limit * (1 << 20))),
        cost_estimate=pl.CostEstimate(flops=flops, bytes_accessed=1 << 20, transcendentals=0),
    )


def struct(*shape, dtype=F32):
    return jax.ShapeDtypeStruct(shape, dtype)


def dma(count):
    return pltpu.SemaphoreType.DMA((count,))


class Shape:
    def __init__(self, table, assign, zm_count, zv_count):
        self.zm, self.zv = zm_count, zv_count
        self.span, self.wide = table[1], table[2]
        self.vb = self.span // BLOCK_V
        self.cb = self.wide // HALF
        self.vt = self.span // 8
        self.ct = self.wide // LANES
        self.blocks = self.vb * self.cb
        self.pairs = self.vb * self.ct
        self.slots = assign[2]
        self.cells = BLOCK_Z * BLOCK_V * BLOCK_C * S

    def main(self, layers):
        return (self.ct, layers, self.span, LANES)

    def halo(self, layers):
        return (self.ct, layers, 8, LANES)


def fill_inverse(g, iterations, assign, inverse):
    me = lax.axis_index("zm") * g.zv + lax.axis_index("zv")
    for t in iterations:
        for peer in range(g.zm):
            inverse[t, peer] = 0
        for slot in range(g.slots):
            block = assign[t * g.slots + slot, me]

            @pl.when(block >= 0)
            def _():
                inverse[t, block // (g.blocks * g.zv)] = slot


def pack_three_body(g, assign, refined, table, out, top, inverse, held, extras, rows_held, sems, out_sems):
    three = range(ITERS - 1)
    reads = [
        pltpu.make_async_copy(refined.at[i], held.at[i], sems.at[i]) for i in range(3 * g.slots)
    ]
    rows_in = pltpu.make_async_copy(table.at[0:ITERS], rows_held, sems.at[3 * g.slots])
    rows_out = pltpu.make_async_copy(rows_held, top, out_sems.at[3 * g.zm + 3])
    rows_in.start()
    for read in reads:
        read.start()
    fill_inverse(g, three, assign, inverse)
    rows_in.wait()
    rows_out.start()
    writes = []
    for t in three:
        for slot in range(g.slots):
            reads[t * g.slots + slot].wait()
        for peer in range(g.zm):
            source = held.at[t * g.slots + inverse[t, peer]]
            target = out.at[peer, OFFSET[t] : OFFSET[t] + ROWS, :]
            writes.append(pltpu.make_async_copy(source, target, out_sems.at[t * g.zm + peer]))
            writes[-1].start()
    for t in three:
        first = OFFSET[t] - t * ROWS
        for peer in range(g.zm):
            after = t * g.slots + inverse[t, min(peer + 1, g.zm - 1)]
            for z in range(halo_rows(t)):
                at = first + z * PAIRS
                extras[peer, at : at + PAIRS, :] = held[after, pl.ds(z, PAIRS, stride=8), :]
        count = halo_rows(t) * PAIRS
        target = out.at[:, OFFSET[t] + ROWS : OFFSET[t + 1], :]
        writes.append(pltpu.make_async_copy(extras.at[:, first : first + count, :], target, out_sems.at[3 * g.zm + t]))
        writes[-1].start()
    for write in writes:
        write.wait()
    rows_out.wait()


def pack_last_body(g, assign, refined, *rest):
    outs, inverse, sems = rest[: g.zm], rest[-2], rest[-1]
    t = ITERS - 1
    fill_inverse(g, [t], assign, inverse)
    here = lax.axis_index("zm")
    copies = []
    for k in range(g.zm):
        source = refined.at[t * g.slots + inverse[t, here ^ k]]
        copies.append(pltpu.make_async_copy(source, outs[k], sems.at[k]))
    for copy in copies:
        copy.start()
    for copy in copies:
        copy.wait()


def pair_tiles(left, first, second):
    even = jnp.where(left, first, pltpu.roll(second, HALF, 1))
    odd = jnp.where(left, pltpu.roll(first, HALF, 1), second)
    return even, odd


def pair_live(meta, iteration, column, left):
    first, second = meta[iteration, column] >= 0, meta[iteration, column + 1] >= 0
    return (left & first) | (~left & second)


def fetch(source, target, sem):
    copy = pltpu.make_async_copy(source, target, sem)
    copy.start()
    return copy


def strip_body(g, meta, data, unused_a, unused_b, out, held, planes, sems):
    three = range(ITERS - 1)
    left, sub = lane_ids() < HALF, sub_ids()
    two = 2 * 8

    def copies(t, c):
        at, mine = t * g.cb + c, jnp.maximum(meta[t, c], 0)
        far = data.at[jnp.maximum(meta[t, g.blocks + c], 0), OFFSET[t] + ROWS : OFFSET[t] + LAYERS[t] * PAIRS, :]
        result = [pltpu.make_async_copy(far, held.at[at, 2 * two : 2 * two + halo_rows(t) * PAIRS, :], sems.at[3 * at])]
        for zt in range(2):
            first = OFFSET[t] + zt * 8 * PAIRS
            source = data.at[mine, first : first + two, :]
            result.append(pltpu.make_async_copy(source, held.at[at, zt * two : zt * two + two, :], sems.at[3 * at + 1 + zt]))
        return result

    for t in three:
        for c in range(g.cb):
            for copy in copies(t, c):
                copy.start()
    for t in three:
        for c in range(g.cb):
            for copy in copies(t, c):
                copy.wait()
        first = sum(LAYERS[:t])
        for z in range(LAYERS[t]):
            for col in range(g.ct):
                tiles = []
                for c in (2 * col, 2 * col + 1):
                    if z < BLOCK_Z:
                        tiles.append(held[t * g.cb + c, pl.ds(z // 8 * two + z % 8, PAIRS, stride=8), :])
                    else:
                        at = 2 * two + (z - BLOCK_Z) * PAIRS
                        tiles.append(held[t * g.cb + c, at : at + PAIRS, :])
                even, odd = pair_tiles(left, *tiles)
                planes[col, first + z, pl.ds(0, PAIRS, stride=2), :] = even
                planes[col, first + z, pl.ds(1, PAIRS, stride=2), :] = odd
        if t == 0:
            for z in range(LAYERS[0]):
                out[z] = jnp.where(sub < 4, planes[0, z, 0:8, :], pltpu.roll(planes[1, z, 0:8, :], 4, 0))
    for z in range(LAYERS[1]):
        one, two_at = LAYERS[0] + z, LAYERS[0] + LAYERS[1] + min(z, LAYERS[2] - 1)
        low = jnp.where(sub < 2, planes[0, one, 0:8, :], pltpu.roll(planes[1, one, 0:8, :], 2, 0))
        high = pltpu.roll(planes[0, two_at, 0:8, :], 4, 0)
        high = jnp.where(sub < 6, high, pltpu.roll(planes[1, two_at, 0:8, :], 6, 0))
        out[LAYERS[0] + z] = jnp.where(sub < 4, low, high)


def strip_tile(strips, t, z, col):
    tile = strips[z] if t == 0 else strips[LAYERS[0] + z]
    shift = (4 * col, 2 * col, 4 + 2 * col)[t]
    return pltpu.roll(tile, 8 - shift, 0) if shift else tile


class Stencil:
    def __init__(self, g, edge):
        self.g = g
        lane, sub = lane_ids(), sub_ids()
        self.inner = lane < LANES - S
        self.above = sub < 7
        self.last = edge & (sub == 7)

    def __call__(self, get, z, low):
        g = self.g
        sums, turned = {}, {}
        for vt in range(g.vt + 1):
            for col in range(g.ct):
                sums[col, vt] = get(col, vt, z) + get(col, vt, low)
                turned[col, vt] = pltpu.roll(sums[col, vt], LANES - S, 1)
        both, up = {}, {}
        for vt in range(g.vt + 1):
            for col in range(g.ct):
                beside = sums[col, vt] if col == g.ct - 1 else turned[col + 1, vt]
                both[col, vt] = sums[col, vt] + jnp.where(self.inner, turned[col, vt], beside)
                up[col, vt] = pltpu.roll(both[col, vt], 7, 0)
        result = {}
        for vt in range(g.vt + 1):
            for col in range(g.ct):
                value = up[col, vt]
                if vt < g.vt:
                    value = jnp.where(self.above, value, up[col, vt + 1])
                if vt == g.vt - 1:
                    value = jnp.where(self.last, both[col, vt], value)
                result[col, vt] = 0.125 * (both[col, vt] + value)
        return result


def edges(meta):
    return meta[0, 120] == 1, meta[0, 121] == 1


def layer_below(z, edge):
    return jnp.where((z == BLOCK_Z - 1) & edge, z, z + 1)


def clip(z, top):
    return jnp.minimum(jnp.maximum(z, 0), top)


def tile_rows(vt):
    return slice(vt * 8, vt * 8 + 8)


def reader(g, main, halo):
    return lambda col, vt, z: halo[col, z] if vt == g.vt else main[col, z, tile_rows(vt), :]


def put(g, main, halo, z, values):
    for (col, vt), value in values.items():
        if vt == g.vt:
            halo[col, z] = value
        else:
            main[col, z, tile_rows(vt), :] = value


def interp_body(g, meta, table, below, strip, interp, interp_halo, nodes, nodes_halo):
    edge_z, edge_v = edges(meta)
    stencil = Stencil(g, edge_v)

    def take(source, z, target):
        for col in range(g.ct):
            lanes = slice(col * LANES, (col + 1) * LANES)
            nodes[col, target] = source[z, :, lanes]
            nodes_halo[col, target] = strip[target, :, lanes]

    @pl.loop(0, BLOCK_Z)
    def _(z):
        take(table, z, z)

    @pl.loop(0, ITERS)
    def _(z):
        take(below, z, BLOCK_Z + z)

    get = reader(g, nodes, nodes_halo)

    @pl.loop(0, LAYERS[0])
    def _(z):
        put(g, interp, interp_halo, z, stencil(get, z, layer_below(z, edge_z)))


PRODUCTS = 14


def spread_rows(values, count):
    rows = [jnp.sum(value, axis=0, keepdims=True) for value in values]
    rows += [jnp.zeros_like(rows[0])] * (-len(rows) % 8)
    column = jnp.sum(jnp.concatenate(rows, 0), axis=1, keepdims=True)
    lane = lax.broadcasted_iota(jnp.int32, (len(rows), 128), 1)
    row = lax.broadcasted_iota(jnp.int32, (len(rows), 128), 0)
    line = jnp.sum(jnp.where(lane == row, column, 0.0), axis=0, keepdims=True)
    return jnp.broadcast_to(line, (count, 128))


def fill_masks(g, meta, masks, iterations, left):
    for at, t in enumerate(iterations):
        for far in range(2):
            for pair in range(g.pairs):
                column = pair // g.ct * g.cb + pair % g.ct * 2 + far * g.blocks
                masks[at, far, pair] = jnp.where(pair_live(meta, t, column, left), 1.0, 0.0)


def halo_live(g, meta, iteration, left):
    first = 2 * g.blocks
    return [[pair_live(meta, iteration, first + far * g.cb + 2 * col, left) for col in range(g.ct)] for far in range(2)]


def segments(top, counts):
    result, high = [], top
    for count in counts:
        result.append((high - count + 1, high))
        high -= count
    return result


def convert(g, meta, t, held, offset, z, out, left):
    row = offset + z // 8 * 8 * PAIRS + z % 8
    for pair in range(g.pairs):
        vb, col = pair // g.ct, pair % g.ct
        tiles = []
        for half in range(2):
            owner = jnp.maximum(meta[t, vb * g.cb + 2 * col + half], 0)
            tiles.append(held[owner, pl.ds(row, PAIRS, stride=8), :])
        even, odd = pair_tiles(left, *tiles)
        out[col, z, pl.ds(vb * BLOCK_V, PAIRS, stride=2), :] = even
        out[col, z, pl.ds(vb * BLOCK_V + 1, PAIRS, stride=2), :] = odd


def between(z):
    return jnp.where((z >= 0) & (z < BLOCK_Z), 1.0, 0.0)


def pair_tile_rows(g, pair):
    return [tile_rows(vt) for vt in (pair // g.ct * 2, pair // g.ct * 2 + 1)]


def local_body(g, meta_in, data, interp_in, a0_out, a1_out, a2_out, totals_out, peaks_out,
               meta, totals, peaks, held, interp, f0, f1, f2, a0, a1, a2, masks, sems, out_sems):
    meta_copy = fetch(meta_in, meta, sems.at[6 + 2 * g.ct])
    f, a, outs = (f0, f1, f2), (a0, a1, a2), (a0_out, a1_out, a2_out)
    split = BLOCK_Z // 2
    groups = ([], [])
    for t in range(3):
        first, middle, end = OFFSET[t], OFFSET[t] + ROWS // 2, OFFSET[t + 1]
        for group, rows in ((0, slice(middle, end)), (1, slice(first, middle))):
            groups[group].append(pltpu.make_async_copy(data.at[:, rows, :], held.at[:, rows, :], sems.at[2 * t + group]))
    for col in range(g.ct):
        for group, layers in ((0, slice(split, LAYERS[0])), (1, slice(0, split))):
            sem = sems.at[6 + 2 * col + group]
            groups[group].append(pltpu.make_async_copy(interp_in.at[col, layers], interp.at[col, layers], sem))
    for group in groups:
        for copy in group:
            copy.start()
    left = lane_ids() < HALF
    peaks[...] = jnp.zeros_like(peaks)
    meta_copy.wait()
    fill_masks(g, meta, masks, (0, 1, 2), left)
    for copy in groups[0]:
        copy.wait()

    @pl.loop(0, g.pairs)
    def _(pair):
        vb, col = pair // g.ct, pair % g.ct
        row = pl.multiple_of(vb * BLOCK_V, BLOCK_V)
        column = g.blocks + vb * g.cb + 2 * col
        for t in range(3):
            owners = [jnp.maximum(meta[t, column + half], 0) for half in range(2)]
            for z in range(BLOCK_Z, LAYERS[t]):
                at = OFFSET[t] + z * PAIRS
                even, odd = pair_tiles(left, *[held[owner, at : at + PAIRS, :] for owner in owners])
                f[t][col, z, pl.ds(row, PAIRS, stride=2), :] = even
                f[t][col, z, pl.ds(row + 1, PAIRS, stride=2), :] = odd
        for t in range(3):
            live = masks[t, 1, pair] > 0.5
            for z in range(BLOCK_Z, LAYERS[t]):
                for half in range(2):
                    rows = pl.ds(row + 8 * half, 8)
                    value = f[t][col, z, rows, :] - interp[col, z, rows, :]
                    a[t][col, z, rows, :] = jnp.where(live, value, 0.0)

    def step(i, carry):
        carry = list(carry)
        base = BLOCK_Z - 1 - i
        at = clip(base + 1, BLOCK_Z - 1)
        inside = jnp.full(TILE, between(base + 1), F32) > 0.5
        for pair in range(g.pairs):
            col = pair % g.ct
            peak = peaks[pair]
            for rows in pair_tile_rows(g, pair):
                mean = interp[col, at, rows, :]
                for t in range(3):
                    live = (masks[t, 0, pair] > 0.5) & inside
                    value = jnp.where(live, f[t][col, at, rows, :] - mean, 0.0)
                    a[t][col, at, rows, :] = value
                    carry[t] = carry[t] + value * value
                    if t == 0:
                        peak = jnp.maximum(peak, jnp.abs(value))
            peaks[pair] = peak
        at = clip(base, BLOCK_Z - 1)
        for t in range(3):
            convert(g, meta, t, held, OFFSET[t], at, f[t], left)
        return tuple(carry)

    carry = (jnp.zeros(TILE, F32),) * 3
    writes, bounds = [], (0, split, split + 5, BLOCK_Z + 1)
    for index in range(3):
        if index == 1:
            for copy in groups[1]:
                copy.wait()
        carry = lax.fori_loop(bounds[index], bounds[index + 1], step, carry)
        lowest = BLOCK_Z - bounds[index + 1] + 1
        for t in range(3):
            highest = BLOCK_Z - bounds[index] if index else LAYERS[t] - 1
            for col in range(g.ct):
                span = slice(lowest, highest + 1)
                sem = out_sems.at[(index * 3 + t) * g.ct + col]
                writes.append(pltpu.make_async_copy(a[t].at[col, span], outs[t].at[col, span], sem))
                writes[-1].start()
    for t in range(3):
        totals[t] = carry[t]
    writes.append(fetch(totals, totals_out, out_sems.at[9 * g.ct]))
    writes.append(fetch(peaks, peaks_out, out_sems.at[9 * g.ct + 1]))
    for write in writes:
        write.wait()


def middle_body(g, meta_in, strips_in, interp_halo_in, totals_in, a0_in, a1_in, a2_in,
                out_hbm, ca0_out, ca1_out, cb1_out, halos_out,
                meta, strips, interp_halo, totals, out, halos, a0, a1, a2, b1, ca0, ca1, cb1, a0_halo, a1_halo, b1_halo, masks, sems, out_sems):
    split = BLOCK_Z // 2
    groups, at = ([], []), 6 * g.ct
    small = []
    for source, target in ((meta_in, meta), (strips_in, strips), (interp_halo_in, interp_halo), (totals_in, totals)):
        small.append(fetch(source, target, sems.at[at]))
        at += 1
    at = 0
    for source, target, layers in ((a0_in, a0, LAYERS[0]), (a1_in, a1, LAYERS[1]), (a2_in, a2, BLOCK_Z)):
        for col in range(g.ct):
            for group, span in ((0, slice(split, layers)), (1, slice(0, split))):
                groups[group].append(pltpu.make_async_copy(source.at[col, span], target.at[col, span], sems.at[at]))
                at += 1
    for group in groups:
        for copy in group:
            copy.start()
    none = LAYERS[0]
    for col in range(g.ct):
        for field in (a1, a2, b1, ca0):
            field[col, none] = jnp.zeros((g.span, LANES), F32)
    for copy in small:
        copy.wait()
    edge_z, edge_v = edges(meta)
    stencil = Stencil(g, edge_v)
    left = lane_ids() < HALF
    live0, live1 = halo_live(g, meta, 0, left), halo_live(g, meta, 1, left)
    fill_masks(g, meta, masks, (1, 2), left)
    for pair in range(g.pairs):
        masks[1, 1, pair] = jnp.zeros(TILE, F32)
    for col in range(g.ct):
        for z in range(LAYERS[0]):
            value = strip_tile(strips, 0, z, col) - interp_halo[col, z]
            a0_halo[col, z] = jnp.where(live0[z >= BLOCK_Z][col], value, 0.0)
        for z in range(LAYERS[1]):
            value = strip_tile(strips, 1, z, col) - interp_halo[col, z]
            a1_halo[col, z] = jnp.where(live1[z >= BLOCK_Z][col], value, 0.0)
    get0, get1, getb = reader(g, a0, a0_halo), reader(g, a1, a1_halo), reader(g, b1, b1_halo)
    top0, top1 = LAYERS[1] - 1, LAYERS[2] - 1
    for copy in groups[0]:
        copy.wait()

    def step(i, carry):
        carry = list(carry)
        base = top0 - i
        z = base + 1
        at = clip(z, top1)
        low = layer_below(at, edge_z)
        after_a = stencil(get1, at, low)
        after_b = stencil(getb, at, low)
        put(g, ca1, halos.at[1], at, after_a)
        put(g, cb1, halos.at[2], at, after_b)
        own = (z >= 0) & (z < BLOCK_Z)
        row, kind = jnp.where(own, z, none), jnp.where(own, 0, 1)
        for pair in range(g.pairs):
            col = pair % g.ct
            live = masks[1, kind, pair] > 0.5
            for half, rows in enumerate(pair_tile_rows(g, pair)):
                vt = pair // g.ct * 2 + half
                one, two = a1[col, row, rows, :], b1[col, row, rows, :]
                carry[0] = carry[0] + one * two
                carry[1] = carry[1] + two * two
                parts = [a2[col, row, rows, :]] + [
                    jnp.where(live, value, 0.0) for value in (ca0[col, row, rows, :], after_a[col, vt], after_b[col, vt])
                ]
                slot = 2
                for m in range(4):
                    for n in range(max(m, 1), 4):
                        carry[slot] = carry[slot] + parts[m] * parts[n]
                        slot += 1
        at = clip(base, top0)
        after = stencil(get0, at, layer_below(at, edge_z))
        put(g, ca0, halos.at[0], at, after)
        far = jnp.where(at >= BLOCK_Z, 1, 0)
        for (col, vt), value in after.items():
            if vt == g.vt:
                live = (live1[0][col] & (at < BLOCK_Z)) | (live1[1][col] & (at >= BLOCK_Z))
                b1_halo[col, at] = jnp.where(live, value, 0.0)
            else:
                mask = masks[0, far, vt // 2 * g.ct + col]
                b1[col, at, tile_rows(vt), :] = jnp.where(mask > 0.5, value, 0.0)
        return tuple(carry)

    carry = (jnp.zeros(TILE, F32),) * 11
    writes = []
    bounds = (0, top0 - split + 1, top0 - split + 6, top0 + 2)
    for index in range(3):
        if index == 1:
            for copy in groups[1]:
                copy.wait()
        carry = lax.fori_loop(bounds[index], bounds[index + 1], step, carry)
        lowest = top0 - bounds[index + 1] + 2
        highest = top0 - bounds[index] + 1 if index else top1
        for which, (source, target) in enumerate(((ca0, ca0_out), (ca1, ca1_out), (cb1, cb1_out))):
            for col in range(g.ct):
                span = slice(lowest, highest + 1)
                sem = out_sems.at[(index * 3 + which) * g.ct + col]
                writes.append(pltpu.make_async_copy(source.at[col, span], target.at[col, span], sem))
                writes[-1].start()
    writes.append(fetch(halos, halos_out, out_sems.at[9 * g.ct]))
    values = [totals[0], totals[1], carry[0], carry[1], totals[2]] + list(carry[2:])
    out[...] = spread_rows(values, out.shape[0])
    writes.append(fetch(out, out_hbm, out_sems.at[9 * g.ct + 1]))
    for write in writes:
        write.wait()


def weight_of(total, count):
    return 1.0 / (1.0 + jnp.sqrt(jnp.maximum(total, 0.0) / count))


def lane_values(line, count):
    lane = lax.broadcasted_iota(jnp.int32, line.shape, 1)
    return [jnp.sum(jnp.where(lane == i, line, 0.0), axis=1, keepdims=True) for i in range(count)]


def live_cells(g, meta, iteration):
    return jnp.full((1, 1), meta[iteration, 122], jnp.int32).astype(F32) * F32(g.cells)


def three_weights(g, meta, parts):
    q = lane_values(jnp.sum(parts[...], axis=0, keepdims=True), PRODUCTS)
    w0 = weight_of(q[0], live_cells(g, meta, 0))
    w1 = weight_of(q[1] - 2.0 * w0 * q[2] + w0 * w0 * q[3], live_cells(g, meta, 1))
    f = [jnp.ones_like(w0), -w0, -w1, w0 * w1]
    total, at = jnp.zeros_like(w0), 4
    for i in range(4):
        for j in range(i, 4):
            total = total + (1.0 if i == j else 2.0) * f[i] * f[j] * q[at]
            at += 1
    return [jnp.broadcast_to(w, TILE) for w in (w0, w1, weight_of(total, live_cells(g, meta, 2)))]


def last_body(g, meta_in, parts, strips_in, interp_halo_in, halos_hbm, peaks0_in, a0_in, a1_in, a2_in, interp_in, ca0_in, ca1_in, cb1_in,
              *rest):
    data, rest = rest[: g.zm], rest[g.zm :]
    (sum_hbm, r3_hbm, errors_out, out,
     meta, strips, interp_halo, halos_in, peaks0, errors, held, f3, a0, a1, a2, interp, ca0, ca1, cb1, r2, r2_halo, change, sum_out, r3, masks, peaks, sems, out_sems) = rest
    top = LAYERS[2] - 1
    small = []
    for source, target in ((meta_in, meta), (strips_in, strips), (interp_halo_in, interp_halo), (halos_hbm, halos_in),
                           (peaks0_in, peaks0)):
        small.append(fetch(source, target, sems.at[g.zm + 28 * g.ct + len(small)]))
    chunks = segments(top, (5, 4, 4, 4))
    reads, at = [], 0
    for lowest, highest in chunks:
        group = []
        if not reads:
            for k in range(g.zm):
                group.append(pltpu.make_async_copy(data[k], held.at[k], sems.at[at]))
                at += 1
        for source, target, layers in ((ca0_in, ca0, BLOCK_Z + 1), (ca1_in, ca1, BLOCK_Z + 1), (cb1_in, cb1, BLOCK_Z + 1),
                                       (a0_in, a0, BLOCK_Z), (a1_in, a1, BLOCK_Z), (a2_in, a2, BLOCK_Z + 1),
                                       (interp_in, interp, BLOCK_Z)):
            for col in range(g.ct):
                span = slice(lowest, min(highest + 1, layers))
                group.append(pltpu.make_async_copy(source.at[col, span], target.at[col, span], sems.at[at]))
                at += 1
        reads.append(group)
    for group in reads:
        for copy in group:
            copy.start()
    peaks[...] = jnp.zeros_like(peaks)
    for copy in small:
        copy.wait()
    edge_z, edge_v = edges(meta)
    stencil = Stencil(g, edge_v)
    left = lane_ids() < HALF
    fill_masks(g, meta, masks, (1, 2, 3), left)
    w0, w1, w2 = three_weights(g, meta, parts)
    w01 = w0 * w1
    live = halo_live(g, meta, 2, left)
    for col in range(g.ct):
        for z in range(LAYERS[2]):
            value = interp_halo[col, z] + w0 * halos_in[0, col, z] + w1 * halos_in[1, col, z] - w01 * halos_in[2, col, z]
            r2_halo[col, z] = jnp.where(live[z >= BLOCK_Z][col], strip_tile(strips, 2, z, col) - value, 0.0)
    get = reader(g, r2, r2_halo)

    def step(i, total):
        base = top - i
        z = base + 1
        at = clip(z, BLOCK_Z - 1)
        counts = between(z)
        after = stencil(get, at, layer_below(at, edge_z))
        for pair in range(g.pairs):
            col = pair % g.ct
            mask = masks[2, 0, pair] * counts > 0.5
            peak = peaks[2, pair]
            for half, rows in enumerate(pair_tile_rows(g, pair)):
                value = f3[col, at, rows, :] - interp[col, at, rows, :] - change[col, at, rows, :]
                value = jnp.where(mask, value - w2 * after[col, pair // g.ct * 2 + half], 0.0)
                r3[col, at, rows, :] = value
                total = total + value * value
                peak = jnp.maximum(peak, jnp.abs(value))
            peaks[2, pair] = peak
        at = clip(base, top)
        far = jnp.where(at >= BLOCK_Z, 1, 0)
        own = jnp.minimum(at, BLOCK_Z - 1)
        inside = jnp.full(TILE, between(at), F32) > 0.5
        for pair in range(g.pairs):
            col = pair % g.ct
            mask1, mask2 = masks[0, 0, pair] > 0.5, masks[1, far, pair] > 0.5
            peak1, peak2 = peaks[0, pair], peaks[1, pair]
            for rows in pair_tile_rows(g, pair):
                zero = w0 * ca0[col, at, rows, :]
                whole = zero + w1 * ca1[col, at, rows, :] - w01 * cb1[col, at, rows, :]
                change[col, at, rows, :] = whole
                value = a2[col, at, rows, :] - jnp.where(mask2, whole, 0.0)
                r2[col, at, rows, :] = value
                peak2 = jnp.maximum(peak2, jnp.where(inside, jnp.abs(value), 0.0))
                one = a1[col, own, rows, :] - jnp.where(mask1, zero, 0.0)
                peak1 = jnp.maximum(peak1, jnp.where(inside, jnp.abs(one), 0.0))
                sum_out[col, own, rows, :] = w0 * a0[col, own, rows, :] + w1 * one + w2 * value
            peaks[0, pair] = peak1
            peaks[1, pair] = peak2
        convert(g, meta, ITERS - 1, held, 0, own, f3, left)
        return total

    total, start, writes = jnp.zeros(TILE, F32), 0, []
    for index, (lowest, highest) in enumerate(chunks):
        for copy in reads[index]:
            copy.wait()
        stop = top - lowest + 1 + (1 if lowest == 0 else 0)
        total = lax.fori_loop(start, stop, step, total)
        start = stop
        below = lowest + 1 if lowest else 0
        above = min((chunks[index - 1][0] if index else BLOCK_Z - 1), BLOCK_Z - 1)
        for which, (source, target, layers) in enumerate(
            ((sum_out, sum_hbm, slice(lowest, min(highest, BLOCK_Z - 1) + 1)), (r3, r3_hbm, slice(below, above + 1)))
        ):
            for col in range(g.ct):
                sem = out_sems.at[(index * 2 + which) * g.ct + col]
                writes.append(pltpu.make_async_copy(source.at[col, layers], target.at[col, layers], sem))
                writes[-1].start()

    line = spread_rows([total], 1)
    lane = lax.broadcasted_iota(jnp.int32, (1, 128), 1)
    lane_p = lax.broadcasted_iota(jnp.int32, (g.pairs, 128), 1)
    row_p = lax.broadcasted_iota(jnp.int32, (g.pairs, 128), 0)
    for i in range(ITERS):
        tiles = [peaks0[pair] if i == 0 else peaks[i - 1, pair] for pair in range(g.pairs)]
        rows = jnp.concatenate([jnp.max(tile, axis=0, keepdims=True) for tile in tiles], 0)
        found = jnp.zeros((1, 128), F32)
        for half in range(2):
            inside = lane_p // HALF == half
            column = jnp.max(jnp.where(inside, rows, 0.0), axis=1, keepdims=True)
            place = row_p // g.ct * g.cb + row_p % g.ct * 2 + half
            found = found + jnp.sum(jnp.where(lane_p == place, column, 0.0), axis=0, keepdims=True)
        errors[i : i + 1, :] = found
        line = jnp.where(lane == 1 + i, jnp.max(found, axis=1, keepdims=True), line)
    writes.append(fetch(errors, errors_out, out_sems.at[8 * g.ct]))
    line = jnp.where(lane == 1 + ITERS, live_cells(g, meta, ITERS - 1), line)
    out[...] = jnp.broadcast_to(line, out.shape)
    for write in writes:
        write.wait()


def finish_body(g, parts, table_in, change_in, r3_in, out_hbm, worst_out, table, change, r3, out, worst, sems, out_sems):
    quarter = BLOCK_Z // 4
    spans = [slice(part * quarter, (part + 1) * quarter) for part in range(4)]
    reads = []
    for part, span in enumerate(spans):
        at = part * (1 + 2 * g.ct)
        group = [pltpu.make_async_copy(table_in.at[span], table.at[span], sems.at[at])]
        for col in range(g.ct):
            at += 2
            group.append(pltpu.make_async_copy(change_in.at[col, span], change.at[col, span], sems.at[at - 1]))
            group.append(pltpu.make_async_copy(r3_in.at[col, span], r3.at[col, span], sems.at[at]))
        reads.append(group)
    for group in reads:
        for read in group:
            read.start()
    total = lane_values(jnp.sum(parts[...], axis=0, keepdims=True), 1)[0]
    largest = lane_values(jnp.max(parts[...], axis=0, keepdims=True), 2 + ITERS)
    w3 = jnp.broadcast_to(weight_of(total, largest[1 + ITERS]), TILE)
    for i in range(ITERS):
        worst[i] = jnp.max(largest[1 + i])
    writes = [fetch(worst, worst_out, out_sems.at[4])]
    for part, span in enumerate(spans):
        for read in reads[part]:
            read.wait()
        for z in range(part * quarter, (part + 1) * quarter):
            for col in range(g.ct):
                lanes = slice(col * LANES, (col + 1) * LANES)
                for vt in range(g.vt):
                    rows = tile_rows(vt)
                    out[z, rows, lanes] = table[z, rows, lanes] + (change[col, z, rows, :] + w3 * r3[col, z, rows, :])
        writes.append(pltpu.make_async_copy(out.at[span], out_hbm.at[span], out_sems.at[part]))
        writes[-1].start()
    for write in writes:
        write.wait()


def index_table(g, assign):
    zm_here, zv_here = lax.axis_index("zm"), lax.axis_index("zv")
    me = zm_here * g.zv + zv_here
    slots = assign.reshape(ITERS, -1)
    owner = jnp.arange(slots.shape[1]) // g.slots // g.zv
    owner = jnp.where(jnp.arange(ITERS)[:, None] == ITERS - 1, owner ^ zm_here, owner)
    column = jnp.arange(2 * g.blocks + 2 * g.cb)
    here = column % g.blocks
    far = jnp.where(column < 2 * g.blocks, column // g.blocks, (column - 2 * g.blocks) // g.cb)
    local = jnp.where(column < 2 * g.blocks, here, (column - 2 * g.blocks) % g.cb)
    side = jnp.where(column < 2 * g.blocks, 0, 1)
    inside = (zm_here + far < g.zm) & (zv_here + side < g.zv)
    target = jnp.where(inside, (me + far * g.zv + side) * g.blocks + local, -2)
    found = jnp.max(jnp.where(slots[:, None, :] == target[None, :, None], owner[:, None, :], -1), axis=2)
    count = jnp.sum((slots >= 0).astype(jnp.int32), axis=1, keepdims=True)
    flags = jnp.stack([zm_here == g.zm - 1, zv_here == g.zv - 1]).astype(jnp.int32)
    gap = jnp.zeros((ITERS, 120 - found.shape[1]), jnp.int32)
    flags = jnp.broadcast_to(flags[None, :], (ITERS, 2))
    return jnp.concatenate([found, gap, flags, count, jnp.zeros((ITERS, 5), jnp.int32)], axis=1)


def to_all(rows):
    count = lax.axis_size("zm") * lax.axis_size("zv")
    return lax.all_to_all(rows.reshape(count, 1, 128), AXES, 0, 0, tiled=True).reshape(count, 128)


def from_next(value, axis):
    count = lax.axis_size(axis)
    return lax.ppermute(value, axis, [(i, i - 1) for i in range(1, count)])


def shards(table, refined, assign):
    g = Shape(table.shape, assign.shape, lax.axis_size("zm"), lax.axis_size("zv"))
    everyone = g.zm * g.zv
    part = functools.partial
    slots = assign.transpose(0, 2, 1).reshape(ITERS * g.slots, -1)
    views = refined.reshape(ITERS * g.slots, BLOCK_Z // 8, 8, PAIRS, LANES).transpose(0, 1, 3, 2, 4)
    views = views.reshape(ITERS * g.slots, ROWS, LANES)
    vmem = lambda *shape: pltpu.VMEM(shape, F32)
    main, halo = g.main, g.halo

    packed, top = call(
        part(pack_three_body, g), [struct(g.zm, OFFSET[3], LANES), struct(ITERS, *table.shape[1:])], [SMEM, HBM, HBM], [HBM] * 2,
        [pltpu.SMEM((ITERS, g.zm), jnp.int32), vmem(3 * g.slots, ROWS, LANES), vmem(g.zm, OFFSET[3] - 3 * ROWS, LANES),
         vmem(ITERS, *table.shape[1:]), dma(3 * g.slots + 1), dma(3 * g.zm + 4)],
        60,
    )(slots, views, table)
    below = from_next(top, "zm")
    data = lax.all_to_all(packed, "zm", 0, 0, tiled=True)
    strip = jnp.concatenate([table[:, :8], below[:, :8]], 0)
    strip = from_next(strip, "zv")
    packed = call(
        part(pack_last_body, g), [struct(ROWS, LANES)] * g.zm, [SMEM, HBM], [VMEM] * g.zm,
        [pltpu.SMEM((ITERS, g.zm), jnp.int32), dma(g.zm)], WHOLE,
    )(slots, views)
    last_data = [packed[0]]
    for k in range(1, g.zm):
        last_data.append(lax.ppermute(packed[k], "zm", [(i, i ^ k) for i in range(g.zm)]))
    meta = index_table(g, assign)
    interp, interp_halo = call(
        part(interp_body, g), [struct(*main(LAYERS[0])), struct(*halo(LAYERS[0]))],
        [SMEM] + [VMEM] * 3, [VMEM] * 2, [vmem(*main(DEEP)), vmem(*halo(DEEP))], PART,
    )(meta, table, below, strip)

    strips = call(
        part(strip_body, g), struct(sum(LAYERS[:2]), *TILE), [SMEM] + [HBM] * 3, VMEM,
        [vmem(3 * g.cb, ROWS, LANES), vmem(g.ct, sum(LAYERS[:3]), BLOCK_V, LANES), dma(9 * g.cb)],
        PART,
    )(meta, data, interp_halo, packed[0])
    strips = from_next(strips, "zv")
    own, more, most = struct(*main(BLOCK_Z)), struct(*main(LAYERS[2])), struct(*main(LAYERS[1]))
    a0, a1, a2, totals, peaks0 = call(
        part(local_body, g), [struct(*main(LAYERS[0])), most, more, struct(3, *TILE), struct(g.pairs, *TILE)],
        [HBM] * 3, [HBM] * 5,
        [pltpu.SMEM(meta.shape, jnp.int32), vmem(3, *TILE), vmem(g.pairs, *TILE), vmem(*data.shape)]
        + [vmem(*main(LAYERS[0]))] * 7
        + [vmem(3, 2, g.pairs, *TILE), dma(7 + 2 * g.ct), dma(9 * g.ct + 2)], WHOLE,
    )(meta, data, interp)
    products, ca0, ca1, cb1, halos = call(
        part(middle_body, g), [struct(everyone, 128), more, more, more, struct(3, *halo(LAYERS[1]))],
        [HBM] * 7, [HBM] * 5,
        [pltpu.SMEM(meta.shape, jnp.int32), vmem(*strips.shape), vmem(*interp_halo.shape), vmem(3, *TILE),
         vmem(everyone, 128), vmem(3, *halo(LAYERS[1]))]
        + [vmem(*main(LAYERS[0] + 1))] * 7 + [vmem(*halo(LAYERS[0] + 1))] * 3
        + [vmem(2, 2, g.pairs, *TILE), dma(6 * g.ct + 4), dma(9 * g.ct + 2)],
        WHOLE,
    )(meta, strips, interp_halo, totals, a0, a1, a2)
    products = to_all(products)
    change, r3, errors, stats = call(
        part(last_body, g), [own, own, struct(ITERS, 128), struct(everyone, 128)],
        [HBM, VMEM] + [HBM] * (11 + g.zm), [HBM] * 3 + [VMEM],
        [pltpu.SMEM(meta.shape, jnp.int32), vmem(*strips.shape), vmem(*interp_halo.shape), vmem(*halos.shape),
         vmem(*peaks0.shape), vmem(ITERS, 128), vmem(g.zm, ROWS, LANES)] + [vmem(*main(BLOCK_Z))] * 3 + [vmem(*main(LAYERS[2])), vmem(*main(BLOCK_Z))]
        + [vmem(*main(LAYERS[2]))] * 4 + [vmem(*halo(LAYERS[2])), vmem(*main(LAYERS[2]))]
        + [vmem(*main(BLOCK_Z))] * 2
        + [vmem(3, 2, g.pairs, *TILE), vmem(3, g.pairs, *TILE), dma(g.zm + 28 * g.ct + 5), dma(8 * g.ct + 1)],
        WHOLE,
    )(meta, products, strips, interp_halo, halos, peaks0, a0, a1, a2, interp, ca0, ca1, cb1, *last_data)
    stats = to_all(stats)
    table_out, worst = call(
        part(finish_body, g), [struct(*table.shape), struct(ITERS)], [VMEM] + [HBM] * 3, [HBM] * 2,
        [vmem(*table.shape)] + [vmem(*main(BLOCK_Z))] * 2
        + [vmem(*table.shape), pltpu.SMEM((ITERS,), F32), dma(4 * (1 + 2 * g.ct)), dma(5)],
        WHOLE,
    )(stats, table, change, r3)
    return (table_out, errors[:, : g.blocks], worst)


def solution(mesh):
    in_specs = (P("zm", "zv", None), P(None, ("zm", "zv"), None, None), P())
    out_specs = (P("zm", "zv", None), P(None, ("zm", "zv")), P())

    return jax.shard_map(shards, mesh=mesh, in_specs=in_specs, out_specs=out_specs, check_vma=False)
```

```python
import functools

import jax
import jax.numpy as jnp
from jax import lax
from jax.experimental import pallas as pl
from jax.experimental.pallas import tpu as pltpu
from jax.sharding import PartitionSpec as P


S = 8
BLOCK_Z = 16
BLOCK_V = 16
BLOCK_C = 8
ITERS = 4
HALF = BLOCK_C * S
PAIRS = BLOCK_V // 2
LANES = 2 * HALF
ROWS = BLOCK_Z * PAIRS
DEEP = BLOCK_Z + ITERS
AXES = ("zm", "zv")
F32 = jnp.float32
TILE = (PAIRS, LANES)


def halo_rows(iteration):
    return ITERS - 1 - iteration


LAYERS = [BLOCK_Z + halo_rows(i) for i in range(ITERS)]
OFFSET = [sum(LAYERS[:i]) * PAIRS for i in range(ITERS)]


def lane_ids():
    return lax.broadcasted_iota(jnp.int32, TILE, 1)


def sub_ids():
    return lax.broadcasted_iota(jnp.int32, TILE, 0)


VMEM = pl.BlockSpec(memory_space=pltpu.VMEM)
SMEM = pl.BlockSpec(memory_space=pltpu.SMEM)
HBM = pl.BlockSpec(memory_space=pltpu.HBM)
WHOLE = 53.5
PART = 24


def call(body, outs, in_specs, out_specs, scratch, limit, flops=2000000):
    return pl.pallas_call(
        body,
        out_shape=outs,
        in_specs=in_specs,
        out_specs=out_specs,
        scratch_shapes=list(scratch),
        compiler_params=pltpu.CompilerParams(vmem_limit_bytes=int(limit * (1 << 20))),
        cost_estimate=pl.CostEstimate(flops=flops, bytes_accessed=1 << 20, transcendentals=0),
    )


def struct(*shape, dtype=F32):
    return jax.ShapeDtypeStruct(shape, dtype)


def dma(count):
    return pltpu.SemaphoreType.DMA((count,))


class Shape:
    def __init__(self, table, assign, zm_count, zv_count):
        self.zm, self.zv = zm_count, zv_count
        self.span, self.wide = table[1], table[2]
        self.vb = self.span // BLOCK_V
        self.cb = self.wide // HALF
        self.vt = self.span // 8
        self.ct = self.wide // LANES
        self.blocks = self.vb * self.cb
        self.pairs = self.vb * self.ct
        self.slots = assign[2]
        self.cells = BLOCK_Z * BLOCK_V * BLOCK_C * S

    def main(self, layers):
        return (self.ct, layers, self.span, LANES)

    def halo(self, layers):
        return (self.ct, layers, 8, LANES)


def fill_inverse(g, iterations, assign, inverse):
    me = lax.axis_index("zm") * g.zv + lax.axis_index("zv")
    for t in iterations:
        for peer in range(g.zm):
            inverse[t, peer] = 0
        for slot in range(g.slots):
            block = assign[t * g.slots + slot, me]

            @pl.when(block >= 0)
            def _():
                inverse[t, block // (g.blocks * g.zv)] = slot


def pack_three_body(g, assign_in, refined, table, out, top, assign, inverse, held, extras, rows_held, sems, out_sems):
    three = range(ITERS - 1)
    reads = [
        pltpu.make_async_copy(refined.at[i], held.at[i], sems.at[i]) for i in range(3 * g.slots)
    ]
    rows_in = pltpu.make_async_copy(table.at[0:ITERS], rows_held, sems.at[3 * g.slots])
    rows_out = pltpu.make_async_copy(rows_held, top, out_sems.at[3 * g.zm + 3])
    numbers = fetch(assign_in, assign, sems.at[3 * g.slots + 1])
    for read in reads:
        read.start()
    rows_in.start()
    numbers.wait()
    fill_inverse(g, three, assign, inverse)
    rows_in.wait()
    rows_out.start()
    writes = []
    for t in three:
        for slot in range(g.slots):
            reads[t * g.slots + slot].wait()
        for peer in range(g.zm):
            source = held.at[t * g.slots + inverse[t, peer]]
            target = out.at[peer, OFFSET[t] : OFFSET[t] + ROWS, :]
            writes.append(pltpu.make_async_copy(source, target, out_sems.at[t * g.zm + peer]))
            writes[-1].start()
    for t in three:
        first = OFFSET[t] - t * ROWS
        for peer in range(g.zm):
            after = t * g.slots + inverse[t, min(peer + 1, g.zm - 1)]
            for z in range(halo_rows(t)):
                at = first + z * PAIRS
                extras[peer, at : at + PAIRS, :] = held[after, pl.ds(z, PAIRS, stride=8), :]
        count = halo_rows(t) * PAIRS
        target = out.at[:, OFFSET[t] + ROWS : OFFSET[t + 1], :]
        writes.append(pltpu.make_async_copy(extras.at[:, first : first + count, :], target, out_sems.at[3 * g.zm + t]))
        writes[-1].start()
    for write in writes:
        write.wait()
    rows_out.wait()


def pack_last_body(g, assign, refined, *rest):
    outs, inverse, sems = rest[: g.zm], rest[-2], rest[-1]
    t = ITERS - 1
    fill_inverse(g, [t], assign, inverse)
    here = lax.axis_index("zm")
    copies = []
    for k in range(g.zm):
        source = refined.at[t * g.slots + inverse[t, here ^ k]]
        copies.append(pltpu.make_async_copy(source, outs[k], sems.at[k]))
    for copy in copies:
        copy.start()
    for copy in copies:
        copy.wait()


def pair_tiles(left, first, second):
    even = jnp.where(left, first, pltpu.roll(second, HALF, 1))
    odd = jnp.where(left, pltpu.roll(first, HALF, 1), second)
    return even, odd


def pair_live(meta, iteration, column, left):
    first, second = meta[iteration, column] >= 0, meta[iteration, column + 1] >= 0
    return (left & first) | (~left & second)


def fetch(source, target, sem):
    copy = pltpu.make_async_copy(source, target, sem)
    copy.start()
    return copy


def strip_body(g, meta, data, unused_a, unused_b, out, held, planes, sems):
    three = range(ITERS - 1)
    left, sub = lane_ids() < HALF, sub_ids()
    two = 2 * 8

    def copies(t, c):
        at, mine = t * g.cb + c, jnp.maximum(meta[t, c], 0)
        far = data.at[jnp.maximum(meta[t, g.blocks + c], 0), OFFSET[t] + ROWS : OFFSET[t] + LAYERS[t] * PAIRS, :]
        result = [pltpu.make_async_copy(far, held.at[at, 2 * two : 2 * two + halo_rows(t) * PAIRS, :], sems.at[3 * at])]
        for zt in range(2):
            first = OFFSET[t] + zt * 8 * PAIRS
            source = data.at[mine, first : first + two, :]
            result.append(pltpu.make_async_copy(source, held.at[at, zt * two : zt * two + two, :], sems.at[3 * at + 1 + zt]))
        return result

    for t in three:
        for c in range(g.cb):
            for copy in copies(t, c):
                copy.start()
    for t in three:
        for c in range(g.cb):
            for copy in copies(t, c):
                copy.wait()
        first = sum(LAYERS[:t])
        for z in range(LAYERS[t]):
            for col in range(g.ct):
                tiles = []
                for c in (2 * col, 2 * col + 1):
                    if z < BLOCK_Z:
                        tiles.append(held[t * g.cb + c, pl.ds(z // 8 * two + z % 8, PAIRS, stride=8), :])
                    else:
                        at = 2 * two + (z - BLOCK_Z) * PAIRS
                        tiles.append(held[t * g.cb + c, at : at + PAIRS, :])
                even, odd = pair_tiles(left, *tiles)
                planes[col, first + z, pl.ds(0, PAIRS, stride=2), :] = even
                planes[col, first + z, pl.ds(1, PAIRS, stride=2), :] = odd
        if t == 0:
            for z in range(LAYERS[0]):
                out[z] = jnp.where(sub < 4, planes[0, z, 0:8, :], pltpu.roll(planes[1, z, 0:8, :], 4, 0))
    for z in range(LAYERS[1]):
        one, two_at = LAYERS[0] + z, LAYERS[0] + LAYERS[1] + min(z, LAYERS[2] - 1)
        low = jnp.where(sub < 2, planes[0, one, 0:8, :], pltpu.roll(planes[1, one, 0:8, :], 2, 0))
        high = pltpu.roll(planes[0, two_at, 0:8, :], 4, 0)
        high = jnp.where(sub < 6, high, pltpu.roll(planes[1, two_at, 0:8, :], 6, 0))
        out[LAYERS[0] + z] = jnp.where(sub < 4, low, high)


def strip_tile(strips, t, z, col):
    tile = strips[z] if t == 0 else strips[LAYERS[0] + z]
    shift = (4 * col, 2 * col, 4 + 2 * col)[t]
    return pltpu.roll(tile, 8 - shift, 0) if shift else tile


class Stencil:
    def __init__(self, g, edge):
        self.g = g
        lane, sub = lane_ids(), sub_ids()
        self.inner = lane < LANES - S
        self.above = sub < 7
        self.last = edge & (sub == 7)

    def __call__(self, get, z, low):
        g = self.g
        sums, turned = {}, {}
        for vt in range(g.vt + 1):
            for col in range(g.ct):
                sums[col, vt] = get(col, vt, z) + get(col, vt, low)
                turned[col, vt] = pltpu.roll(sums[col, vt], LANES - S, 1)
        both, up = {}, {}
        for vt in range(g.vt + 1):
            for col in range(g.ct):
                beside = sums[col, vt] if col == g.ct - 1 else turned[col + 1, vt]
                both[col, vt] = sums[col, vt] + jnp.where(self.inner, turned[col, vt], beside)
                up[col, vt] = pltpu.roll(both[col, vt], 7, 0)
        result = {}
        for vt in range(g.vt + 1):
            for col in range(g.ct):
                value = up[col, vt]
                if vt < g.vt:
                    value = jnp.where(self.above, value, up[col, vt + 1])
                if vt == g.vt - 1:
                    value = jnp.where(self.last, both[col, vt], value)
                result[col, vt] = 0.125 * (both[col, vt] + value)
        return result


def edges(meta):
    return meta[0, 120] == 1, meta[0, 121] == 1


def layer_below(z, edge):
    return jnp.where((z == BLOCK_Z - 1) & edge, z, z + 1)


def clip(z, top):
    return jnp.minimum(jnp.maximum(z, 0), top)


def tile_rows(vt):
    return slice(vt * 8, vt * 8 + 8)


def reader(g, main, halo):
    return lambda col, vt, z: halo[col, z] if vt == g.vt else main[col, z, tile_rows(vt), :]


def put(g, main, halo, z, values):
    for (col, vt), value in values.items():
        if vt == g.vt:
            halo[col, z] = value
        else:
            main[col, z, tile_rows(vt), :] = value


def interp_body(g, meta, table, below, strip, interp, interp_halo, nodes, nodes_halo):
    edge_z, edge_v = edges(meta)
    stencil = Stencil(g, edge_v)

    def take(source, z, target):
        for col in range(g.ct):
            lanes = slice(col * LANES, (col + 1) * LANES)
            nodes[col, target] = source[z, :, lanes]
            nodes_halo[col, target] = strip[target, :, lanes]

    @pl.loop(0, BLOCK_Z)
    def _(z):
        take(table, z, z)

    @pl.loop(0, ITERS)
    def _(z):
        take(below, z, BLOCK_Z + z)

    get = reader(g, nodes, nodes_halo)

    @pl.loop(0, LAYERS[0])
    def _(z):
        put(g, interp, interp_halo, z, stencil(get, z, layer_below(z, edge_z)))


PRODUCTS = 14


def spread_rows(values, count):
    rows = [jnp.sum(value, axis=0, keepdims=True) for value in values]
    rows += [jnp.zeros_like(rows[0])] * (-len(rows) % 8)
    column = jnp.sum(jnp.concatenate(rows, 0), axis=1, keepdims=True)
    lane = lax.broadcasted_iota(jnp.int32, (len(rows), 128), 1)
    row = lax.broadcasted_iota(jnp.int32, (len(rows), 128), 0)
    line = jnp.sum(jnp.where(lane == row, column, 0.0), axis=0, keepdims=True)
    return jnp.broadcast_to(line, (count, 128))


def fill_masks(g, meta, masks, iterations, left):
    for at, t in enumerate(iterations):
        for far in range(2):
            for pair in range(g.pairs):
                column = pair // g.ct * g.cb + pair % g.ct * 2 + far * g.blocks
                masks[at, far, pair] = jnp.where(pair_live(meta, t, column, left), 1.0, 0.0)


def halo_live(g, meta, iteration, left):
    first = 2 * g.blocks
    return [[pair_live(meta, iteration, first + far * g.cb + 2 * col, left) for col in range(g.ct)] for far in range(2)]


def segments(top, counts):
    result, high = [], top
    for count in counts:
        result.append((high - count + 1, high))
        high -= count
    return result


def fill_first_rows(g, meta, iterations, rows, first_rows):
    for t in iterations:
        for block in range(g.blocks):
            first_rows[t, block] = jnp.maximum(meta[t, block], 0) * rows + (OFFSET[t] if t < ITERS - 1 else 0)


def convert(g, first_rows, t, held, z, out, left):
    row = z // 8 * 8 * PAIRS + z % 8
    for pair in range(g.pairs):
        vb, col = pair // g.ct, pair % g.ct
        tiles = []
        for half in range(2):
            tiles.append(held[pl.ds(first_rows[t, vb * g.cb + 2 * col + half] + row, PAIRS, stride=8), :])
        even, odd = pair_tiles(left, *tiles)
        out[col, z, pl.ds(vb * BLOCK_V, PAIRS, stride=2), :] = even
        out[col, z, pl.ds(vb * BLOCK_V + 1, PAIRS, stride=2), :] = odd


def between(z):
    return jnp.where((z >= 0) & (z < BLOCK_Z), 1.0, 0.0)


def pair_tile_rows(g, pair):
    return [tile_rows(vt) for vt in (pair // g.ct * 2, pair // g.ct * 2 + 1)]


def local_body(g, meta_in, data, interp_in, a0_out, a1_out, a2_out, totals_out, peaks_out,
               meta, first_rows, totals, peaks, arrived, interp, f0, f1, f2, a0, a1, a2, masks, sems, out_sems):
    meta_copy = fetch(meta_in, meta, sems.at[8])
    held = arrived.reshape(g.zm * OFFSET[3], LANES)
    f, a, outs = (f0, f1, f2), (a0, a1, a2), (a0_out, a1_out, a2_out)
    split = BLOCK_Z // 2
    groups = ([], [])
    for t in range(3):
        first, middle, end = OFFSET[t], OFFSET[t] + ROWS // 2, OFFSET[t + 1]
        for group, rows in ((0, slice(middle, end)), (1, slice(first, middle))):
            copy = pltpu.make_async_copy(data.at[:, rows, :], arrived.at[:, rows, :], sems.at[2 * t + group])
            groups[group].append(copy)
    for group, layers in ((0, slice(split, LAYERS[0])), (1, slice(0, split))):
        groups[group].append(pltpu.make_async_copy(interp_in.at[:, layers], interp.at[:, layers], sems.at[6 + group]))
    for group in groups:
        for copy in group:
            copy.start()
    left = lane_ids() < HALF
    peaks[...] = jnp.zeros_like(peaks)
    meta_copy.wait()
    fill_first_rows(g, meta, range(3), OFFSET[3], first_rows)
    fill_masks(g, meta, masks, (0, 1, 2), left)
    for copy in groups[0]:
        copy.wait()

    @pl.loop(0, g.pairs)
    def _(pair):
        vb, col = pair // g.ct, pair % g.ct
        row = pl.multiple_of(vb * BLOCK_V, BLOCK_V)
        column = g.blocks + vb * g.cb + 2 * col
        for t in range(3):
            starts = [jnp.maximum(meta[t, column + half], 0) * OFFSET[3] for half in range(2)]
            for z in range(BLOCK_Z, LAYERS[t]):
                at = [pl.multiple_of(start + OFFSET[t] + z * PAIRS, PAIRS) for start in starts]
                even, odd = pair_tiles(left, *[held[pl.ds(row_at, PAIRS), :] for row_at in at])
                f[t][col, z, pl.ds(row, PAIRS, stride=2), :] = even
                f[t][col, z, pl.ds(row + 1, PAIRS, stride=2), :] = odd
        for t in range(3):
            live = masks[t, 1, pair] > 0.5
            for z in range(BLOCK_Z, LAYERS[t]):
                for half in range(2):
                    rows = pl.ds(row + 8 * half, 8)
                    value = f[t][col, z, rows, :] - interp[col, z, rows, :]
                    a[t][col, z, rows, :] = jnp.where(live, value, 0.0)

    def step(i, carry):
        carry = list(carry)
        base = BLOCK_Z - 1 - i
        at = clip(base + 1, BLOCK_Z - 1)
        inside = jnp.full(TILE, between(base + 1), F32) > 0.5
        for pair in range(g.pairs):
            col = pair % g.ct
            peak = peaks[pair]
            for rows in pair_tile_rows(g, pair):
                mean = interp[col, at, rows, :]
                for t in range(3):
                    live = (masks[t, 0, pair] > 0.5) & inside
                    value = jnp.where(live, f[t][col, at, rows, :] - mean, 0.0)
                    a[t][col, at, rows, :] = value
                    carry[t] = carry[t] + value * value
                    if t == 0:
                        peak = jnp.maximum(peak, jnp.abs(value))
            peaks[pair] = peak
        at = clip(base, BLOCK_Z - 1)
        for t in range(3):
            convert(g, first_rows, t, held, at, f[t], left)
        return tuple(carry)

    carry = (jnp.zeros(TILE, F32),) * 3
    writes, bounds = [], (0, split, split + 4, BLOCK_Z - 1, BLOCK_Z + 1)
    for index in range(4):
        if index == 1:
            for copy in groups[1]:
                copy.wait()
        carry = lax.fori_loop(bounds[index], bounds[index + 1], step, carry)
        lowest = BLOCK_Z - bounds[index + 1] + 1
        for t in range(3):
            highest = BLOCK_Z - bounds[index] if index else LAYERS[t] - 1
            span = slice(lowest, highest + 1)
            writes.append(fetch(a[t].at[:, span], outs[t].at[:, span], out_sems.at[index * 3 + t]))
    for t in range(3):
        totals[t] = carry[t]
    writes.append(fetch(totals, totals_out, out_sems.at[12]))
    writes.append(fetch(peaks, peaks_out, out_sems.at[13]))
    for write in writes:
        write.wait()


def middle_body(g, meta_in, strips_in, interp_halo_in, totals_in, a0_in, a1_in, a2_in,
                out, ca0_out, ca1_out, cb1_out, halos_out,
                meta, strips, interp_halo, totals, halos, a0, a1, a2, b1, ca0, ca1, cb1, a0_halo, a1_halo, b1_halo, masks, sems, out_sems):
    cuts = (12, 6, 0)
    groups, at = ([], [], []), 9
    small = []
    for source, target in ((meta_in, meta), (strips_in, strips), (interp_halo_in, interp_halo), (totals_in, totals)):
        small.append(fetch(source, target, sems.at[at]))
        at += 1
    at = 0
    for source, target, layers in ((a0_in, a0, LAYERS[0]), (a1_in, a1, LAYERS[1]), (a2_in, a2, BLOCK_Z)):
        for group, span in enumerate((slice(cuts[0], layers), slice(cuts[1], cuts[0]), slice(0, cuts[1]))):
            groups[group].append(pltpu.make_async_copy(source.at[:, span], target.at[:, span], sems.at[at]))
            at += 1
    for group in groups:
        for copy in group:
            copy.start()
    none = LAYERS[0]
    for col in range(g.ct):
        for field in (a1, a2, b1, ca0):
            field[col, none] = jnp.zeros((g.span, LANES), F32)
    for copy in small:
        copy.wait()
    edge_z, edge_v = edges(meta)
    stencil = Stencil(g, edge_v)
    left = lane_ids() < HALF
    live0, live1 = halo_live(g, meta, 0, left), halo_live(g, meta, 1, left)
    fill_masks(g, meta, masks, (1, 2), left)
    for pair in range(g.pairs):
        masks[1, 1, pair] = jnp.zeros(TILE, F32)
    for col in range(g.ct):
        for z in range(LAYERS[0]):
            value = strip_tile(strips, 0, z, col) - interp_halo[col, z]
            a0_halo[col, z] = jnp.where(live0[z >= BLOCK_Z][col], value, 0.0)
        for z in range(LAYERS[1]):
            value = strip_tile(strips, 1, z, col) - interp_halo[col, z]
            a1_halo[col, z] = jnp.where(live1[z >= BLOCK_Z][col], value, 0.0)
    get0, get1, getb = reader(g, a0, a0_halo), reader(g, a1, a1_halo), reader(g, b1, b1_halo)
    top0, top1 = LAYERS[1] - 1, LAYERS[2] - 1
    for copy in groups[0]:
        copy.wait()

    def step(i, carry):
        carry = list(carry)
        base = top0 - i
        z = base + 1
        at = clip(z, top1)
        low = layer_below(at, edge_z)
        after_a = stencil(get1, at, low)
        after_b = stencil(getb, at, low)
        put(g, ca1, halos.at[1], at, after_a)
        put(g, cb1, halos.at[2], at, after_b)
        own = (z >= 0) & (z < BLOCK_Z)
        row, kind = jnp.where(own, z, none), jnp.where(own, 0, 1)
        for pair in range(g.pairs):
            col = pair % g.ct
            live = masks[1, kind, pair] > 0.5
            for half, rows in enumerate(pair_tile_rows(g, pair)):
                vt = pair // g.ct * 2 + half
                one, two = a1[col, row, rows, :], b1[col, row, rows, :]
                carry[0] = carry[0] + one * two
                carry[1] = carry[1] + two * two
                parts = [a2[col, row, rows, :]] + [
                    jnp.where(live, value, 0.0) for value in (ca0[col, row, rows, :], after_a[col, vt], after_b[col, vt])
                ]
                slot = 2
                for m in range(4):
                    for n in range(max(m, 1), 4):
                        carry[slot] = carry[slot] + parts[m] * parts[n]
                        slot += 1
        at = clip(base, top0)
        after = stencil(get0, at, layer_below(at, edge_z))
        put(g, ca0, halos.at[0], at, after)
        far = jnp.where(at >= BLOCK_Z, 1, 0)
        for (col, vt), value in after.items():
            if vt == g.vt:
                live = (live1[0][col] & (at < BLOCK_Z)) | (live1[1][col] & (at >= BLOCK_Z))
                b1_halo[col, at] = jnp.where(live, value, 0.0)
            else:
                mask = masks[0, far, vt // 2 * g.ct + col]
                b1[col, at, tile_rows(vt), :] = jnp.where(mask > 0.5, value, 0.0)
        return tuple(carry)

    carry = (jnp.zeros(TILE, F32),) * 11
    writes = []
    bounds = (0, top0 - cuts[0] + 1, top0 - cuts[1] + 1, top0, top0 + 2)
    for index in range(4):
        if index in (1, 2):
            for copy in groups[index]:
                copy.wait()
        carry = lax.fori_loop(bounds[index], bounds[index + 1], step, carry)
        lowest = top0 - bounds[index + 1] + 2
        highest = top0 - bounds[index] + 1 if index else top1
        for which, (source, target) in enumerate(((ca0, ca0_out), (ca1, ca1_out), (cb1, cb1_out))):
            span = slice(lowest, highest + 1)
            writes.append(fetch(source.at[:, span], target.at[:, span], out_sems.at[index * 3 + which]))
    writes.append(fetch(halos, halos_out, out_sems.at[12]))
    values = [totals[0], totals[1], carry[0], carry[1], totals[2]] + list(carry[2:])
    out[...] = spread_rows(values, out.shape[0])
    for write in writes:
        write.wait()


def weight_of(total, count):
    return 1.0 / (1.0 + jnp.sqrt(jnp.maximum(total, 0.0) / count))


def lane_values(line, count):
    lane = lax.broadcasted_iota(jnp.int32, line.shape, 1)
    return [jnp.sum(jnp.where(lane == i, line, 0.0), axis=1, keepdims=True) for i in range(count)]


def live_cells(g, meta, iteration):
    return jnp.full((1, 1), meta[iteration, 122], jnp.int32).astype(F32) * F32(g.cells)


def three_weights(g, meta, parts):
    q = lane_values(jnp.sum(parts[...], axis=0, keepdims=True), PRODUCTS)
    w0 = weight_of(q[0], live_cells(g, meta, 0))
    w1 = weight_of(q[1] - 2.0 * w0 * q[2] + w0 * w0 * q[3], live_cells(g, meta, 1))
    f = [jnp.ones_like(w0), -w0, -w1, w0 * w1]
    total, at = jnp.zeros_like(w0), 4
    for i in range(4):
        for j in range(i, 4):
            total = total + (1.0 if i == j else 2.0) * f[i] * f[j] * q[at]
            at += 1
    return [jnp.broadcast_to(w, TILE) for w in (w0, w1, weight_of(total, live_cells(g, meta, 2)))]


def last_body(g, meta_in, parts, strips_in, interp_halo_in, halos_hbm, peaks0_in, a0_in, a1_in, a2_in, interp_in, ca0_in, ca1_in, cb1_in,
              *rest):
    data, rest = rest[: g.zm], rest[g.zm :]
    (sum_hbm, r3_hbm, errors_out, out,
     meta, first_rows, strips, interp_halo, halos_in, peaks0, errors, held, f3, a0, a1, a2, interp, ca0, ca1, cb1, r2, r2_halo, change, sum_out, r3, masks, peaks, sems, out_sems) = rest
    top = LAYERS[2] - 1
    small = []
    for source, target in ((meta_in, meta), (strips_in, strips), (interp_halo_in, interp_halo), (halos_hbm, halos_in),
                           (peaks0_in, peaks0)):
        small.append(fetch(source, target, sems.at[g.zm + 28 + len(small)]))
    chunks = segments(top, (3, 5, 5, 4))
    reads, at = [], 0
    for lowest, highest in chunks:
        group = []
        if not reads:
            for k in range(g.zm):
                group.append(pltpu.make_async_copy(data[k], held.at[k * ROWS : (k + 1) * ROWS, :], sems.at[at]))
                at += 1
        for source, target, layers in ((ca0_in, ca0, BLOCK_Z + 1), (ca1_in, ca1, BLOCK_Z + 1), (cb1_in, cb1, BLOCK_Z + 1),
                                       (a0_in, a0, BLOCK_Z), (a1_in, a1, BLOCK_Z), (a2_in, a2, BLOCK_Z + 1),
                                       (interp_in, interp, BLOCK_Z)):
            span = slice(lowest, min(highest + 1, layers))
            group.append(pltpu.make_async_copy(source.at[:, span], target.at[:, span], sems.at[at]))
            at += 1
        reads.append(group)
    for group in reads:
        for copy in group:
            copy.start()
    peaks[...] = jnp.zeros_like(peaks)
    for copy in small:
        copy.wait()
    edge_z, edge_v = edges(meta)
    stencil = Stencil(g, edge_v)
    left = lane_ids() < HALF
    fill_masks(g, meta, masks, (1, 2, 3), left)
    fill_first_rows(g, meta, [ITERS - 1], ROWS, first_rows)
    w0, w1, w2 = three_weights(g, meta, parts)
    w01 = w0 * w1
    live = halo_live(g, meta, 2, left)
    for col in range(g.ct):
        for z in range(LAYERS[2]):
            value = interp_halo[col, z] + w0 * halos_in[0, col, z] + w1 * halos_in[1, col, z] - w01 * halos_in[2, col, z]
            r2_halo[col, z] = jnp.where(live[z >= BLOCK_Z][col], strip_tile(strips, 2, z, col) - value, 0.0)
    get = reader(g, r2, r2_halo)

    def step(i, total):
        base = top - i
        z = base + 1
        at = clip(z, BLOCK_Z - 1)
        counts = between(z)
        after = stencil(get, at, layer_below(at, edge_z))
        for pair in range(g.pairs):
            col = pair % g.ct
            mask = masks[2, 0, pair] * counts > 0.5
            peak = peaks[2, pair]
            for half, rows in enumerate(pair_tile_rows(g, pair)):
                value = f3[col, at, rows, :] - interp[col, at, rows, :] - change[col, at, rows, :]
                value = jnp.where(mask, value - w2 * after[col, pair // g.ct * 2 + half], 0.0)
                r3[col, at, rows, :] = value
                total = total + value * value
                peak = jnp.maximum(peak, jnp.abs(value))
            peaks[2, pair] = peak
        at = clip(base, top)
        far = jnp.where(at >= BLOCK_Z, 1, 0)
        own = jnp.minimum(at, BLOCK_Z - 1)
        inside = jnp.full(TILE, between(at), F32) > 0.5
        for pair in range(g.pairs):
            col = pair % g.ct
            mask1, mask2 = masks[0, 0, pair] > 0.5, masks[1, far, pair] > 0.5
            peak1, peak2 = peaks[0, pair], peaks[1, pair]
            for rows in pair_tile_rows(g, pair):
                zero = w0 * ca0[col, at, rows, :]
                whole = zero + w1 * ca1[col, at, rows, :] - w01 * cb1[col, at, rows, :]
                change[col, at, rows, :] = whole
                value = a2[col, at, rows, :] - jnp.where(mask2, whole, 0.0)
                r2[col, at, rows, :] = value
                peak2 = jnp.maximum(peak2, jnp.where(inside, jnp.abs(value), 0.0))
                one = a1[col, own, rows, :] - jnp.where(mask1, zero, 0.0)
                peak1 = jnp.maximum(peak1, jnp.where(inside, jnp.abs(one), 0.0))
                sum_out[col, own, rows, :] = w0 * a0[col, own, rows, :] + w1 * one + w2 * value
            peaks[0, pair] = peak1
            peaks[1, pair] = peak2
        convert(g, first_rows, ITERS - 1, held, own, f3, left)
        return total

    total, start, writes = jnp.zeros(TILE, F32), 0, []
    for index, (lowest, highest) in enumerate(chunks):
        for copy in reads[index]:
            copy.wait()
        stop = top - lowest + 1 + (1 if lowest == 0 else 0)
        total = lax.fori_loop(start, stop, step, total)
        start = stop
        below = lowest + 1 if lowest else 0
        above = min((chunks[index - 1][0] if index else BLOCK_Z - 1), BLOCK_Z - 1)
        for which, (source, target, layers) in enumerate(
            ((sum_out, sum_hbm, slice(lowest, min(highest, BLOCK_Z - 1) + 1)), (r3, r3_hbm, slice(below, above + 1)))
        ):
            writes.append(fetch(source.at[:, layers], target.at[:, layers], out_sems.at[index * 2 + which]))

    line = spread_rows([total], 1)
    lane = lax.broadcasted_iota(jnp.int32, (1, 128), 1)
    lane_p = lax.broadcasted_iota(jnp.int32, (g.pairs, 128), 1)
    row_p = lax.broadcasted_iota(jnp.int32, (g.pairs, 128), 0)
    for i in range(ITERS):
        tiles = [peaks0[pair] if i == 0 else peaks[i - 1, pair] for pair in range(g.pairs)]
        rows = jnp.concatenate([jnp.max(tile, axis=0, keepdims=True) for tile in tiles], 0)
        found = jnp.zeros((1, 128), F32)
        for half in range(2):
            inside = lane_p // HALF == half
            column = jnp.max(jnp.where(inside, rows, 0.0), axis=1, keepdims=True)
            place = row_p // g.ct * g.cb + row_p % g.ct * 2 + half
            found = found + jnp.sum(jnp.where(lane_p == place, column, 0.0), axis=0, keepdims=True)
        errors[i : i + 1, :] = found
        line = jnp.where(lane == 1 + i, jnp.max(found, axis=1, keepdims=True), line)
    writes.append(fetch(errors, errors_out, out_sems.at[8]))
    line = jnp.where(lane == 1 + ITERS, live_cells(g, meta, ITERS - 1), line)
    out[...] = jnp.broadcast_to(line, out.shape)
    for write in writes:
        write.wait()


def finish_body(g, parts, table_in, change_in, r3_in, out_hbm, worst_out, table, change, r3, out, worst, sems, out_sems):
    quarter = BLOCK_Z // 4
    spans = [slice(part * quarter, (part + 1) * quarter) for part in range(4)]
    reads = []
    for part, span in enumerate(spans):
        group = [pltpu.make_async_copy(table_in.at[span], table.at[span], sems.at[3 * part])]
        for i, (source, target) in enumerate(((change_in, change), (r3_in, r3))):
            group.append(pltpu.make_async_copy(source.at[:, span], target.at[:, span], sems.at[3 * part + 1 + i]))
        reads.append(group)
    for group in reads:
        for read in group:
            read.start()
    total = lane_values(jnp.sum(parts[...], axis=0, keepdims=True), 1)[0]
    largest = lane_values(jnp.max(parts[...], axis=0, keepdims=True), 2 + ITERS)
    w3 = jnp.broadcast_to(weight_of(total, largest[1 + ITERS]), TILE)
    for i in range(ITERS):
        worst[i] = jnp.max(largest[1 + i])
    writes = [fetch(worst, worst_out, out_sems.at[4])]
    for part, span in enumerate(spans):
        for read in reads[part]:
            read.wait()
        for z in range(part * quarter, (part + 1) * quarter):
            for col in range(g.ct):
                lanes = slice(col * LANES, (col + 1) * LANES)
                for vt in range(g.vt):
                    rows = tile_rows(vt)
                    out[z, rows, lanes] = table[z, rows, lanes] + (change[col, z, rows, :] + w3 * r3[col, z, rows, :])
        writes.append(pltpu.make_async_copy(out.at[span], out_hbm.at[span], out_sems.at[part]))
        writes[-1].start()
    for write in writes:
        write.wait()


def index_table(g, assign):
    zm_here, zv_here = lax.axis_index("zm"), lax.axis_index("zv")
    me = zm_here * g.zv + zv_here
    slots = assign.reshape(ITERS, -1)
    owner = jnp.arange(slots.shape[1]) // g.slots // g.zv
    owner = jnp.where(jnp.arange(ITERS)[:, None] == ITERS - 1, owner ^ zm_here, owner)
    column = jnp.arange(2 * g.blocks + 2 * g.cb)
    here = column % g.blocks
    far = jnp.where(column < 2 * g.blocks, column // g.blocks, (column - 2 * g.blocks) // g.cb)
    local = jnp.where(column < 2 * g.blocks, here, (column - 2 * g.blocks) % g.cb)
    side = jnp.where(column < 2 * g.blocks, 0, 1)
    inside = (zm_here + far < g.zm) & (zv_here + side < g.zv)
    target = jnp.where(inside, (me + far * g.zv + side) * g.blocks + local, -2)
    found = jnp.max(jnp.where(slots[:, None, :] == target[None, :, None], owner[:, None, :], -1), axis=2)
    count = jnp.sum((slots >= 0).astype(jnp.int32), axis=1, keepdims=True)
    flags = jnp.stack([zm_here == g.zm - 1, zv_here == g.zv - 1]).astype(jnp.int32)
    gap = jnp.zeros((ITERS, 120 - found.shape[1]), jnp.int32)
    flags = jnp.broadcast_to(flags[None, :], (ITERS, 2))
    return jnp.concatenate([found, gap, flags, count, jnp.zeros((ITERS, 5), jnp.int32)], axis=1)


def to_all(rows):
    count = lax.axis_size("zm") * lax.axis_size("zv")
    return lax.all_to_all(rows.reshape(count, 1, 128), AXES, 0, 0, tiled=True).reshape(count, 128)


def from_next(value, axis):
    count = lax.axis_size(axis)
    return lax.ppermute(value, axis, [(i, i - 1) for i in range(1, count)])


def shards(table, refined, assign):
    g = Shape(table.shape, assign.shape, lax.axis_size("zm"), lax.axis_size("zv"))
    everyone = g.zm * g.zv
    part = functools.partial
    slots = assign.transpose(0, 2, 1).reshape(ITERS * g.slots, -1)
    views = refined.reshape(ITERS * g.slots, BLOCK_Z // 8, 8, PAIRS, LANES).transpose(0, 1, 3, 2, 4)
    views = views.reshape(ITERS * g.slots, ROWS, LANES)
    vmem = lambda *shape: pltpu.VMEM(shape, F32)
    main, halo = g.main, g.halo

    packed, top = call(
        part(pack_three_body, g), [struct(g.zm, OFFSET[3], LANES), struct(ITERS, *table.shape[1:])], [HBM] * 3, [HBM] * 2,
        [pltpu.SMEM(slots.shape, jnp.int32), pltpu.SMEM((ITERS, g.zm), jnp.int32), vmem(3 * g.slots, ROWS, LANES), vmem(g.zm, OFFSET[3] - 3 * ROWS, LANES),
         vmem(ITERS, *table.shape[1:]), dma(3 * g.slots + 2), dma(3 * g.zm + 4)],
        60,
    )(slots, views, table)
    below = from_next(top, "zm")
    data = lax.all_to_all(packed, "zm", 0, 0, tiled=True)
    strip = jnp.concatenate([table[:, :8], below[:, :8]], 0)
    strip = from_next(strip, "zv")
    packed = call(
        part(pack_last_body, g), [struct(ROWS, LANES)] * g.zm, [SMEM, HBM], [VMEM] * g.zm,
        [pltpu.SMEM((ITERS, g.zm), jnp.int32), dma(g.zm)], WHOLE,
    )(slots, views)
    last_data = [packed[0]]
    for k in range(1, g.zm):
        last_data.append(lax.ppermute(packed[k], "zm", [(i, i ^ k) for i in range(g.zm)]))
    meta = index_table(g, assign)
    interp, interp_halo = call(
        part(interp_body, g), [struct(*main(LAYERS[0])), struct(*halo(LAYERS[0]))],
        [SMEM] + [VMEM] * 3, [VMEM] * 2, [vmem(*main(DEEP)), vmem(*halo(DEEP))], PART,
    )(meta, table, below, strip)

    strips = call(
        part(strip_body, g), struct(sum(LAYERS[:2]), *TILE), [SMEM] + [HBM] * 3, VMEM,
        [vmem(3 * g.cb, ROWS, LANES), vmem(g.ct, sum(LAYERS[:3]), BLOCK_V, LANES), dma(9 * g.cb)],
        PART,
    )(meta, data, interp_halo, packed[0])
    strips = from_next(strips, "zv")
    own, more, most = struct(*main(BLOCK_Z)), struct(*main(LAYERS[2])), struct(*main(LAYERS[1]))
    a0, a1, a2, totals, peaks0 = call(
        part(local_body, g), [struct(*main(LAYERS[0])), most, more, struct(3, *TILE), struct(g.pairs, *TILE)],
        [HBM] * 3, [HBM] * 5,
        [pltpu.SMEM(meta.shape, jnp.int32), pltpu.SMEM((ITERS, g.blocks), jnp.int32), vmem(3, *TILE),
         vmem(g.pairs, *TILE), vmem(*data.shape)]
        + [vmem(*main(LAYERS[0]))] * 7
        + [vmem(3, 2, g.pairs, *TILE), dma(9), dma(14)], WHOLE,
    )(meta, data, interp)
    products, ca0, ca1, cb1, halos = call(
        part(middle_body, g), [struct(everyone, 128), more, more, more, struct(3, *halo(LAYERS[1]))],
        [HBM] * 7, [VMEM] + [HBM] * 4,
        [pltpu.SMEM(meta.shape, jnp.int32), vmem(*strips.shape), vmem(*interp_halo.shape), vmem(3, *TILE),
         vmem(3, *halo(LAYERS[1]))]
        + [vmem(*main(LAYERS[0] + 1))] * 7 + [vmem(*halo(LAYERS[0] + 1))] * 3
        + [vmem(2, 2, g.pairs, *TILE), dma(13), dma(13)],
        WHOLE,
    )(meta, strips, interp_halo, totals, a0, a1, a2)
    products, *last_data = lax.optimization_barrier((products, *last_data))
    products = to_all(products)
    change, r3, errors, stats = call(
        part(last_body, g), [own, own, struct(ITERS, 128), struct(everyone, 128)],
        [HBM, VMEM] + [HBM] * (11 + g.zm), [HBM] * 3 + [VMEM],
        [pltpu.SMEM(meta.shape, jnp.int32), pltpu.SMEM((ITERS, g.blocks), jnp.int32), vmem(*strips.shape),
         vmem(*interp_halo.shape), vmem(*halos.shape), vmem(*peaks0.shape), vmem(ITERS, 128), vmem(g.zm * ROWS, LANES)] + [vmem(*main(BLOCK_Z))] * 3 + [vmem(*main(LAYERS[2])), vmem(*main(BLOCK_Z))]
        + [vmem(*main(LAYERS[2]))] * 4 + [vmem(*halo(LAYERS[2])), vmem(*main(LAYERS[2]))]
        + [vmem(*main(BLOCK_Z))] * 2
        + [vmem(3, 2, g.pairs, *TILE), vmem(3, g.pairs, *TILE), dma(g.zm + 33), dma(9)],
        WHOLE,
    )(meta, products, strips, interp_halo, halos, peaks0, a0, a1, a2, interp, ca0, ca1, cb1, *last_data)
    stats = to_all(stats)
    table_out, worst = call(
        part(finish_body, g), [struct(*table.shape), struct(ITERS)], [VMEM] + [HBM] * 3, [HBM] * 2,
        [vmem(*table.shape)] + [vmem(*main(BLOCK_Z))] * 2
        + [vmem(*table.shape), pltpu.SMEM((ITERS,), F32), dma(12), dma(5)],
        WHOLE,
    )(stats, table, change, r3)
    return (table_out, errors[:, : g.blocks], worst)


def solution(mesh):
    in_specs = (P("zm", "zv", None), P(None, ("zm", "zv"), None, None), P())
    out_specs = (P("zm", "zv", None), P(None, ("zm", "zv")), P())

    return jax.shard_map(shards, mesh=mesh, in_specs=in_specs, out_specs=out_specs, check_vma=False)
```

```python
import functools

import jax
import jax.numpy as jnp
from jax import lax
from jax.experimental import pallas as pl
from jax.experimental.pallas import tpu as pltpu
from jax.sharding import PartitionSpec as P


S = 8
BLOCK_Z = 16
BLOCK_V = 16
BLOCK_C = 8
ITERS = 4
HALF = BLOCK_C * S
PAIRS = BLOCK_V // 2
LANES = 2 * HALF
ROWS = BLOCK_Z * PAIRS
DEEP = BLOCK_Z + ITERS
AXES = ("zm", "zv")
F32 = jnp.float32
TILE = (PAIRS, LANES)


def halo_rows(iteration):
    return ITERS - 1 - iteration


LAYERS = [BLOCK_Z + halo_rows(i) for i in range(ITERS)]
OFFSET = [sum(LAYERS[:i]) * PAIRS for i in range(ITERS)]


def lane_ids():
    return lax.broadcasted_iota(jnp.int32, TILE, 1)


def sub_ids():
    return lax.broadcasted_iota(jnp.int32, TILE, 0)


VMEM = pl.BlockSpec(memory_space=pltpu.VMEM)
SMEM = pl.BlockSpec(memory_space=pltpu.SMEM)
HBM = pl.BlockSpec(memory_space=pltpu.HBM)
WHOLE = 53.5
PART = 24


def call(body, outs, in_specs, out_specs, scratch, limit, flops=2000000):
    return pl.pallas_call(
        body,
        out_shape=outs,
        in_specs=in_specs,
        out_specs=out_specs,
        scratch_shapes=list(scratch),
        compiler_params=pltpu.CompilerParams(vmem_limit_bytes=int(limit * (1 << 20))),
        cost_estimate=pl.CostEstimate(flops=flops, bytes_accessed=1 << 20, transcendentals=0),
    )


def struct(*shape, dtype=F32):
    return jax.ShapeDtypeStruct(shape, dtype)


def dma(count):
    return pltpu.SemaphoreType.DMA((count,))


class Shape:
    def __init__(self, table, assign, zm_count, zv_count):
        self.zm, self.zv = zm_count, zv_count
        self.span, self.wide = table[1], table[2]
        self.vb = self.span // BLOCK_V
        self.cb = self.wide // HALF
        self.vt = self.span // 8
        self.ct = self.wide // LANES
        self.blocks = self.vb * self.cb
        self.pairs = self.vb * self.ct
        self.slots = assign[2]
        self.cells = BLOCK_Z * BLOCK_V * BLOCK_C * S

    def main(self, layers):
        return (self.ct, layers, self.span, LANES)

    def wide_main(self, layers):
        return (self.ct, layers, self.span + 8, LANES)

    def halo(self, layers):
        return (self.ct, layers, 8, LANES)


def fill_inverse(g, iterations, assign, inverse):
    me = lax.axis_index("zm") * g.zv + lax.axis_index("zv")
    for t in iterations:
        for peer in range(g.zm):
            inverse[t, peer] = 0
        for slot in range(g.slots):
            block = assign[t * g.slots + slot, me]

            @pl.when(block >= 0)
            def _():
                inverse[t, block // (g.blocks * g.zv)] = slot


def pack_three_body(g, assign_in, refined, table, out, top, assign, inverse, held, extras, rows_held, sems, out_sems):
    three = range(ITERS - 1)
    spans = [slice(t * g.slots, (t + 1) * g.slots) for t in three]
    reads = [pltpu.make_async_copy(refined.at[span], held.at[span], sems.at[t]) for t, span in enumerate(spans)]
    rows_in = pltpu.make_async_copy(table.at[0:ITERS], rows_held, sems.at[3])
    rows_out = pltpu.make_async_copy(rows_held, top, out_sems.at[3 * g.zm + 3])
    numbers = fetch(assign_in, assign, sems.at[4])
    for read in reads:
        read.start()
    rows_in.start()
    numbers.wait()
    fill_inverse(g, three, assign, inverse)
    rows_in.wait()
    rows_out.start()
    writes = []
    for t in three:
        reads[t].wait()
        for peer in range(g.zm):
            source = held.at[t * g.slots + inverse[t, peer]]
            target = out.at[peer, OFFSET[t] : OFFSET[t] + ROWS, :]
            writes.append(pltpu.make_async_copy(source, target, out_sems.at[t * g.zm + peer]))
            writes[-1].start()
    for t in three:
        first = OFFSET[t] - t * ROWS
        for peer in range(g.zm):
            after = t * g.slots + inverse[t, min(peer + 1, g.zm - 1)]
            for z in range(halo_rows(t)):
                at = first + z * PAIRS
                extras[peer, at : at + PAIRS, :] = held[after, pl.ds(z, PAIRS, stride=8), :]
        count = halo_rows(t) * PAIRS
        target = out.at[:, OFFSET[t] + ROWS : OFFSET[t + 1], :]
        writes.append(pltpu.make_async_copy(extras.at[:, first : first + count, :], target, out_sems.at[3 * g.zm + t]))
        writes[-1].start()
    for write in writes:
        write.wait()
    rows_out.wait()


def pack_last_body(g, assign, refined, *rest):
    outs, inverse, sems = rest[: g.zm], rest[-2], rest[-1]
    t = ITERS - 1
    fill_inverse(g, [t], assign, inverse)
    here = lax.axis_index("zm")
    copies = []
    for k in range(g.zm):
        source = refined.at[t * g.slots + inverse[t, here ^ k]]
        copies.append(pltpu.make_async_copy(source, outs[k], sems.at[k]))
    for copy in copies:
        copy.start()
    for copy in copies:
        copy.wait()


def pair_tiles(left, first, second):
    even = jnp.where(left, first, pltpu.roll(second, HALF, 1))
    odd = jnp.where(left, pltpu.roll(first, HALF, 1), second)
    return even, odd


def pair_live(meta, iteration, column, left):
    first, second = meta[iteration, column] >= 0, meta[iteration, column + 1] >= 0
    return (left & first) | (~left & second)


def fetch(source, target, sem):
    copy = pltpu.make_async_copy(source, target, sem)
    copy.start()
    return copy


def strip_body(g, meta, data, unused_a, unused_b, out, held, planes, sems):
    three = range(ITERS - 1)
    left, sub = lane_ids() < HALF, sub_ids()
    two = 2 * 8

    def copies(t, c):
        at, mine = t * g.cb + c, jnp.maximum(meta[t, c], 0)
        far = data.at[jnp.maximum(meta[t, g.blocks + c], 0), OFFSET[t] + ROWS : OFFSET[t] + LAYERS[t] * PAIRS, :]
        result = [pltpu.make_async_copy(far, held.at[at, 2 * two : 2 * two + halo_rows(t) * PAIRS, :], sems.at[3 * at])]
        for zt in range(2):
            first = OFFSET[t] + zt * 8 * PAIRS
            source = data.at[mine, first : first + two, :]
            result.append(pltpu.make_async_copy(source, held.at[at, zt * two : zt * two + two, :], sems.at[3 * at + 1 + zt]))
        return result

    for t in three:
        for c in range(g.cb):
            for copy in copies(t, c):
                copy.start()
    for t in three:
        for c in range(g.cb):
            for copy in copies(t, c):
                copy.wait()
        first = sum(LAYERS[:t])
        for z in range(LAYERS[t]):
            for col in range(g.ct):
                tiles = []
                for c in (2 * col, 2 * col + 1):
                    if z < BLOCK_Z:
                        tiles.append(held[t * g.cb + c, pl.ds(z // 8 * two + z % 8, PAIRS, stride=8), :])
                    else:
                        at = 2 * two + (z - BLOCK_Z) * PAIRS
                        tiles.append(held[t * g.cb + c, at : at + PAIRS, :])
                even, odd = pair_tiles(left, *tiles)
                planes[col, first + z, pl.ds(0, PAIRS, stride=2), :] = even
                planes[col, first + z, pl.ds(1, PAIRS, stride=2), :] = odd
        if t == 0:
            for z in range(LAYERS[0]):
                out[z] = jnp.where(sub < 4, planes[0, z, 0:8, :], pltpu.roll(planes[1, z, 0:8, :], 4, 0))
    for z in range(LAYERS[1]):
        one, two_at = LAYERS[0] + z, LAYERS[0] + LAYERS[1] + min(z, LAYERS[2] - 1)
        low = jnp.where(sub < 2, planes[0, one, 0:8, :], pltpu.roll(planes[1, one, 0:8, :], 2, 0))
        high = pltpu.roll(planes[0, two_at, 0:8, :], 4, 0)
        high = jnp.where(sub < 6, high, pltpu.roll(planes[1, two_at, 0:8, :], 6, 0))
        out[LAYERS[0] + z] = jnp.where(sub < 4, low, high)


def strip_tile(strips, t, z, col):
    tile = strips[z] if t == 0 else strips[LAYERS[0] + z]
    shift = (4 * col, 2 * col, 4 + 2 * col)[t]
    return pltpu.roll(tile, 8 - shift, 0) if shift else tile


class Stencil:
    def __init__(self, g, edge):
        self.g = g
        lane, sub = lane_ids(), sub_ids()
        self.inner = lane < LANES - S
        self.above = sub < 7
        self.last = edge & (sub == 7)

    def __call__(self, get, z, low):
        g = self.g
        sums, turned = {}, {}
        for vt in range(g.vt + 1):
            for col in range(g.ct):
                sums[col, vt] = get(col, vt, z) + get(col, vt, low)
                turned[col, vt] = pltpu.roll(sums[col, vt], LANES - S, 1)
        both, up = {}, {}
        for vt in range(g.vt + 1):
            for col in range(g.ct):
                beside = sums[col, vt] if col == g.ct - 1 else turned[col + 1, vt]
                both[col, vt] = sums[col, vt] + jnp.where(self.inner, turned[col, vt], beside)
                up[col, vt] = pltpu.roll(both[col, vt], 7, 0)
        result = {}
        for vt in range(g.vt + 1):
            for col in range(g.ct):
                value = up[col, vt]
                if vt < g.vt:
                    value = jnp.where(self.above, value, up[col, vt + 1])
                if vt == g.vt - 1:
                    value = jnp.where(self.last, both[col, vt], value)
                result[col, vt] = 0.125 * (both[col, vt] + value)
        return result


def edges(meta):
    return meta[0, 120] == 1, meta[0, 121] == 1


def layer_below(z, edge):
    return jnp.where((z == BLOCK_Z - 1) & edge, z, z + 1)


def clip(z, top):
    return jnp.minimum(jnp.maximum(z, 0), top)


def tile_rows(vt):
    return slice(vt * 8, vt * 8 + 8)


def reader(g, main, halo):
    return lambda col, vt, z: halo[col, z] if vt == g.vt else main[col, z, tile_rows(vt), :]


def put(g, main, halo, z, values):
    for (col, vt), value in values.items():
        if vt == g.vt:
            halo[col, z] = value
        else:
            main[col, z, tile_rows(vt), :] = value


def put_wide(main, z, values):
    for (col, vt), value in values.items():
        main[col, z, tile_rows(vt), :] = value


def interp_body(g, meta, table, below, strip, interp, interp_halo, nodes, nodes_halo):
    edge_z, edge_v = edges(meta)
    stencil = Stencil(g, edge_v)

    def take(source, z, target):
        for col in range(g.ct):
            lanes = slice(col * LANES, (col + 1) * LANES)
            nodes[col, target] = source[z, :, lanes]
            nodes_halo[col, target] = strip[target, :, lanes]

    @pl.loop(0, BLOCK_Z)
    def _(z):
        take(table, z, z)

    @pl.loop(0, ITERS)
    def _(z):
        take(below, z, BLOCK_Z + z)

    get = reader(g, nodes, nodes_halo)

    @pl.loop(0, LAYERS[0])
    def _(z):
        put(g, interp, interp_halo, z, stencil(get, z, layer_below(z, edge_z)))


PRODUCTS = 14


def spread_rows(values, count):
    rows = [jnp.sum(value, axis=0, keepdims=True) for value in values]
    rows += [jnp.zeros_like(rows[0])] * (-len(rows) % 8)
    column = jnp.sum(jnp.concatenate(rows, 0), axis=1, keepdims=True)
    lane = lax.broadcasted_iota(jnp.int32, (len(rows), 128), 1)
    row = lax.broadcasted_iota(jnp.int32, (len(rows), 128), 0)
    line = jnp.sum(jnp.where(lane == row, column, 0.0), axis=0, keepdims=True)
    return jnp.broadcast_to(line, (count, 128))


def fill_masks(g, meta, masks, iterations, left):
    for at, t in enumerate(iterations):
        for far in range(2):
            for pair in range(g.pairs):
                column = pair // g.ct * g.cb + pair % g.ct * 2 + far * g.blocks
                masks[at, far, pair] = jnp.where(pair_live(meta, t, column, left), 1.0, 0.0)


def halo_live(g, meta, iteration, left):
    first = 2 * g.blocks
    return [[pair_live(meta, iteration, first + far * g.cb + 2 * col, left) for col in range(g.ct)] for far in range(2)]


def segments(top, counts):
    result, high = [], top
    for count in counts:
        result.append((high - count + 1, high))
        high -= count
    return result


def fill_first_rows(g, meta, iterations, rows, first_rows):
    for t in iterations:
        for block in range(g.blocks):
            first_rows[t, block] = jnp.maximum(meta[t, block], 0) * rows + (OFFSET[t] if t < ITERS - 1 else 0)


def convert(g, first_rows, t, held, z, out, left):
    row = z // 8 * 8 * PAIRS + z % 8
    for pair in range(g.pairs):
        vb, col = pair // g.ct, pair % g.ct
        tiles = []
        for half in range(2):
            tiles.append(held[pl.ds(first_rows[t, vb * g.cb + 2 * col + half] + row, PAIRS, stride=8), :])
        even, odd = pair_tiles(left, *tiles)
        out[col, z, pl.ds(vb * BLOCK_V, PAIRS, stride=2), :] = even
        out[col, z, pl.ds(vb * BLOCK_V + 1, PAIRS, stride=2), :] = odd


def between(z):
    return jnp.where((z >= 0) & (z < BLOCK_Z), 1.0, 0.0)


def pair_tile_rows(g, pair):
    return [tile_rows(vt) for vt in (pair // g.ct * 2, pair // g.ct * 2 + 1)]


def local_body(g, meta_in, data, interp_in, a0_out, a1_out, a2_out, totals_out, peaks_out,
               meta, first_rows, totals, peaks, arrived, interp, f0, f1, f2, a0, a1, a2, masks, sems, out_sems):
    meta_copy = fetch(meta_in, meta, sems.at[8])
    held = arrived.reshape(g.zm * OFFSET[3], LANES)
    f, a, outs = (f0, f1, f2), (a0, a1, a2), (a0_out, a1_out, a2_out)
    split = BLOCK_Z // 2
    groups = ([], [])
    for t in range(3):
        first, middle, end = OFFSET[t], OFFSET[t] + ROWS // 2, OFFSET[t + 1]
        for group, rows in ((0, slice(middle, end)), (1, slice(first, middle))):
            copy = pltpu.make_async_copy(data.at[:, rows, :], arrived.at[:, rows, :], sems.at[2 * t + group])
            groups[group].append(copy)
    for group, layers in ((0, slice(split, LAYERS[0])), (1, slice(0, split))):
        groups[group].append(pltpu.make_async_copy(interp_in.at[:, layers], interp.at[:, layers], sems.at[6 + group]))
    for group in groups:
        for copy in group:
            copy.start()
    left = lane_ids() < HALF
    peaks[...] = jnp.zeros_like(peaks)
    meta_copy.wait()
    fill_first_rows(g, meta, range(3), OFFSET[3], first_rows)
    fill_masks(g, meta, masks, (0, 1, 2), left)
    for copy in groups[0]:
        copy.wait()

    @pl.loop(0, g.pairs)
    def _(pair):
        vb, col = pair // g.ct, pair % g.ct
        row = pl.multiple_of(vb * BLOCK_V, BLOCK_V)
        column = g.blocks + vb * g.cb + 2 * col
        for t in range(3):
            starts = [jnp.maximum(meta[t, column + half], 0) * OFFSET[3] for half in range(2)]
            for z in range(BLOCK_Z, LAYERS[t]):
                at = [pl.multiple_of(start + OFFSET[t] + z * PAIRS, PAIRS) for start in starts]
                even, odd = pair_tiles(left, *[held[pl.ds(row_at, PAIRS), :] for row_at in at])
                f[t][col, z, pl.ds(row, PAIRS, stride=2), :] = even
                f[t][col, z, pl.ds(row + 1, PAIRS, stride=2), :] = odd
        for t in range(3):
            live = masks[t, 1, pair] > 0.5
            for z in range(BLOCK_Z, LAYERS[t]):
                for half in range(2):
                    rows = pl.ds(row + 8 * half, 8)
                    value = f[t][col, z, rows, :] - interp[col, z, rows, :]
                    a[t][col, z, rows, :] = jnp.where(live, value, 0.0)

    def step(i, carry):
        carry = list(carry)
        base = BLOCK_Z - 1 - i
        at = clip(base + 1, BLOCK_Z - 1)
        inside = jnp.full(TILE, between(base + 1), F32) > 0.5
        for pair in range(g.pairs):
            col = pair % g.ct
            peak = peaks[pair]
            for rows in pair_tile_rows(g, pair):
                mean = interp[col, at, rows, :]
                for t in range(3):
                    live = (masks[t, 0, pair] > 0.5) & inside
                    value = jnp.where(live, f[t][col, at, rows, :] - mean, 0.0)
                    a[t][col, at, rows, :] = value
                    carry[t] = carry[t] + value * value
                    if t == 0:
                        peak = jnp.maximum(peak, jnp.abs(value))
            peaks[pair] = peak
        at = clip(base, BLOCK_Z - 1)
        for t in range(3):
            convert(g, first_rows, t, held, at, f[t], left)
        return tuple(carry)

    carry = (jnp.zeros(TILE, F32),) * 3
    writes, bounds = [], (0, split, split + 4, BLOCK_Z - 1, BLOCK_Z + 1)
    for index in range(4):
        if index == 1:
            for copy in groups[1]:
                copy.wait()
        carry = lax.fori_loop(bounds[index], bounds[index + 1], step, carry)
        lowest = BLOCK_Z - bounds[index + 1] + 1
        for t in range(3):
            highest = BLOCK_Z - bounds[index] if index else LAYERS[t] - 1
            span = slice(lowest, highest + 1)
            writes.append(fetch(a[t].at[:, span], outs[t].at[:, span], out_sems.at[index * 3 + t]))
    for t in range(3):
        totals[t] = carry[t]
    writes.append(fetch(totals, totals_out, out_sems.at[12]))
    writes.append(fetch(peaks, peaks_out, out_sems.at[13]))
    for write in writes:
        write.wait()


def middle_body(g, meta_in, strips_in, interp_halo_in, totals_in, a0_in, a1_in, a2_in,
                out, ca0_out, ca1_out, cb1_out,
                meta, strips, interp_halo, totals, a0, a1, a2, b1, ca0, ca1, cb1, a0_halo, a1_halo, b1_halo, masks, sems, out_sems):
    cuts = (12, 6, 0)
    groups, at = ([], [], []), 9
    small = []
    for source, target in ((meta_in, meta), (strips_in, strips), (interp_halo_in, interp_halo), (totals_in, totals)):
        small.append(fetch(source, target, sems.at[at]))
        at += 1
    at = 0
    for source, target, layers in ((a0_in, a0, LAYERS[0]), (a1_in, a1, LAYERS[1]), (a2_in, a2, BLOCK_Z)):
        for group, span in enumerate((slice(cuts[0], layers), slice(cuts[1], cuts[0]), slice(0, cuts[1]))):
            groups[group].append(pltpu.make_async_copy(source.at[:, span], target.at[:, span], sems.at[at]))
            at += 1
    for group in groups:
        for copy in group:
            copy.start()
    none = LAYERS[0]
    for col in range(g.ct):
        for field in (a1, a2, b1):
            field[col, none] = jnp.zeros((g.span, LANES), F32)
        ca0[col, none] = jnp.zeros((g.span + 8, LANES), F32)
    for copy in small:
        copy.wait()
    edge_z, edge_v = edges(meta)
    stencil = Stencil(g, edge_v)
    left = lane_ids() < HALF
    live0, live1 = halo_live(g, meta, 0, left), halo_live(g, meta, 1, left)
    fill_masks(g, meta, masks, (1, 2), left)
    for pair in range(g.pairs):
        masks[1, 1, pair] = jnp.zeros(TILE, F32)
    for col in range(g.ct):
        for z in range(LAYERS[0]):
            value = strip_tile(strips, 0, z, col) - interp_halo[col, z]
            a0_halo[col, z] = jnp.where(live0[z >= BLOCK_Z][col], value, 0.0)
        for z in range(LAYERS[1]):
            value = strip_tile(strips, 1, z, col) - interp_halo[col, z]
            a1_halo[col, z] = jnp.where(live1[z >= BLOCK_Z][col], value, 0.0)
    get0, get1, getb = reader(g, a0, a0_halo), reader(g, a1, a1_halo), reader(g, b1, b1_halo)
    top0, top1 = LAYERS[1] - 1, LAYERS[2] - 1
    for copy in groups[0]:
        copy.wait()

    def step(i, carry):
        carry = list(carry)
        base = top0 - i
        z = base + 1
        at = clip(z, top1)
        low = layer_below(at, edge_z)
        after_a = stencil(get1, at, low)
        after_b = stencil(getb, at, low)
        put_wide(ca1, at, after_a)
        put_wide(cb1, at, after_b)
        own = (z >= 0) & (z < BLOCK_Z)
        row, kind = jnp.where(own, z, none), jnp.where(own, 0, 1)
        for pair in range(g.pairs):
            col = pair % g.ct
            live = masks[1, kind, pair] > 0.5
            for half, rows in enumerate(pair_tile_rows(g, pair)):
                vt = pair // g.ct * 2 + half
                one, two = a1[col, row, rows, :], b1[col, row, rows, :]
                carry[0] = carry[0] + one * two
                carry[1] = carry[1] + two * two
                parts = [a2[col, row, rows, :]] + [
                    jnp.where(live, value, 0.0) for value in (ca0[col, row, rows, :], after_a[col, vt], after_b[col, vt])
                ]
                slot = 2
                for m in range(4):
                    for n in range(max(m, 1), 4):
                        carry[slot] = carry[slot] + parts[m] * parts[n]
                        slot += 1
        at = clip(base, top0)
        after = stencil(get0, at, layer_below(at, edge_z))
        put_wide(ca0, at, after)
        far = jnp.where(at >= BLOCK_Z, 1, 0)
        for (col, vt), value in after.items():
            if vt == g.vt:
                live = (live1[0][col] & (at < BLOCK_Z)) | (live1[1][col] & (at >= BLOCK_Z))
                b1_halo[col, at] = jnp.where(live, value, 0.0)
            else:
                mask = masks[0, far, vt // 2 * g.ct + col]
                b1[col, at, tile_rows(vt), :] = jnp.where(mask > 0.5, value, 0.0)
        return tuple(carry)

    carry = (jnp.zeros(TILE, F32),) * 11
    writes = []
    bounds = (0, top0 - cuts[0] + 1, top0 - cuts[1] + 1, top0, top0 + 2)
    for index in range(4):
        if index in (1, 2):
            for copy in groups[index]:
                copy.wait()
        carry = lax.fori_loop(bounds[index], bounds[index + 1], step, carry)
        lowest = top0 - bounds[index + 1] + 2
        highest = top0 - bounds[index] + 1 if index else top1
        for which, (source, target) in enumerate(((ca0, ca0_out), (ca1, ca1_out), (cb1, cb1_out))):
            span = slice(lowest, highest + 1)
            writes.append(fetch(source.at[:, span], target.at[:, span], out_sems.at[index * 3 + which]))
    values = [totals[0], totals[1], carry[0], carry[1], totals[2]] + list(carry[2:])
    out[...] = spread_rows(values, out.shape[0])
    for write in writes:
        write.wait()


def weight_of(total, count):
    return 1.0 / (1.0 + jnp.sqrt(jnp.maximum(total, 0.0) / count))


def lane_values(line, count):
    lane = lax.broadcasted_iota(jnp.int32, line.shape, 1)
    return [jnp.sum(jnp.where(lane == i, line, 0.0), axis=1, keepdims=True) for i in range(count)]


def live_cells(g, meta, iteration):
    return jnp.full((1, 1), meta[iteration, 122], jnp.int32).astype(F32) * F32(g.cells)


def three_weights(g, meta, parts):
    q = lane_values(jnp.sum(parts[...], axis=0, keepdims=True), PRODUCTS)
    w0 = weight_of(q[0], live_cells(g, meta, 0))
    w1 = weight_of(q[1] - 2.0 * w0 * q[2] + w0 * w0 * q[3], live_cells(g, meta, 1))
    f = [jnp.ones_like(w0), -w0, -w1, w0 * w1]
    total, at = jnp.zeros_like(w0), 4
    for i in range(4):
        for j in range(i, 4):
            total = total + (1.0 if i == j else 2.0) * f[i] * f[j] * q[at]
            at += 1
    return [jnp.broadcast_to(w, TILE) for w in (w0, w1, weight_of(total, live_cells(g, meta, 2)))]


def last_body(g, meta_in, parts, strips_in, interp_halo_in, peaks0_in, a0_in, a1_in, a2_in, interp_in, ca0_in, ca1_in, cb1_in,
              *rest):
    data, rest = rest[: g.zm], rest[g.zm :]
    (sum_out, r3, errors_out, out,
     meta, first_rows, strips, interp_halo, peaks0, errors, held, f3, a0, a1, a2, interp, ca0, ca1, cb1, r2, r2_halo, change, masks, peaks, sems, out_sems) = rest
    top = LAYERS[2] - 1
    small = []
    for source, target in ((meta_in, meta), (strips_in, strips), (interp_halo_in, interp_halo), (peaks0_in, peaks0)):
        small.append(fetch(source, target, sems.at[g.zm + 28 + len(small)]))
    chunks = segments(top, (3, 5, 5, 4))
    reads, at = [], 0
    for lowest, highest in chunks:
        group = []
        if not reads:
            for k in range(g.zm):
                group.append(pltpu.make_async_copy(data[k], held.at[k * ROWS : (k + 1) * ROWS, :], sems.at[at]))
                at += 1
        for source, target, layers in ((ca0_in, ca0, BLOCK_Z + 1), (ca1_in, ca1, BLOCK_Z + 1), (cb1_in, cb1, BLOCK_Z + 1),
                                       (a0_in, a0, BLOCK_Z), (a1_in, a1, BLOCK_Z), (a2_in, a2, BLOCK_Z + 1),
                                       (interp_in, interp, BLOCK_Z)):
            span = slice(lowest, min(highest + 1, layers))
            group.append(pltpu.make_async_copy(source.at[:, span], target.at[:, span], sems.at[at]))
            at += 1
        reads.append(group)
    for group in reads:
        for copy in group:
            copy.start()
    peaks[...] = jnp.zeros_like(peaks)
    for copy in small:
        copy.wait()
    edge_z, edge_v = edges(meta)
    stencil = Stencil(g, edge_v)
    left = lane_ids() < HALF
    fill_masks(g, meta, masks, (1, 2, 3), left)
    fill_first_rows(g, meta, [ITERS - 1], ROWS, first_rows)
    w0, w1, w2 = three_weights(g, meta, parts)
    w01 = w0 * w1
    live = halo_live(g, meta, 2, left)
    get = reader(g, r2, r2_halo)

    def step(i, total):
        base = top - i
        z = base + 1
        at = clip(z, BLOCK_Z - 1)
        counts = between(z)
        after = stencil(get, at, layer_below(at, edge_z))
        for pair in range(g.pairs):
            col = pair % g.ct
            mask = masks[2, 0, pair] * counts > 0.5
            peak = peaks[2, pair]
            for half, rows in enumerate(pair_tile_rows(g, pair)):
                value = f3[col, at, rows, :] - interp[col, at, rows, :] - change[col, at, rows, :]
                value = jnp.where(mask, value - w2 * after[col, pair // g.ct * 2 + half], 0.0)
                r3[col, at, rows, :] = value
                total = total + value * value
                peak = jnp.maximum(peak, jnp.abs(value))
            peaks[2, pair] = peak
        at = clip(base, top)
        edge = tile_rows(g.vt)
        for col in range(g.ct):
            value = strip_tile(strips, 2, at, col) - interp_halo[col, at] - w0 * ca0[col, at, edge, :]
            value = value - w1 * ca1[col, at, edge, :] + w01 * cb1[col, at, edge, :]
            there = (live[0][col] & (at < BLOCK_Z)) | (live[1][col] & (at >= BLOCK_Z))
            r2_halo[col, at] = jnp.where(there, value, 0.0)
        far = jnp.where(at >= BLOCK_Z, 1, 0)
        own = jnp.minimum(at, BLOCK_Z - 1)
        inside = jnp.full(TILE, between(at), F32) > 0.5
        for pair in range(g.pairs):
            col = pair % g.ct
            mask1, mask2 = masks[0, 0, pair] > 0.5, masks[1, far, pair] > 0.5
            peak1, peak2 = peaks[0, pair], peaks[1, pair]
            for rows in pair_tile_rows(g, pair):
                zero = w0 * ca0[col, at, rows, :]
                whole = zero + w1 * ca1[col, at, rows, :] - w01 * cb1[col, at, rows, :]
                change[col, at, rows, :] = whole
                value = a2[col, at, rows, :] - jnp.where(mask2, whole, 0.0)
                r2[col, at, rows, :] = value
                peak2 = jnp.maximum(peak2, jnp.where(inside, jnp.abs(value), 0.0))
                one = a1[col, own, rows, :] - jnp.where(mask1, zero, 0.0)
                peak1 = jnp.maximum(peak1, jnp.where(inside, jnp.abs(one), 0.0))
                sum_out[col, own, rows, :] = w0 * a0[col, own, rows, :] + w1 * one + w2 * value
            peaks[0, pair] = peak1
            peaks[1, pair] = peak2
        convert(g, first_rows, ITERS - 1, held, own, f3, left)
        return total

    total, start, writes = jnp.zeros(TILE, F32), 0, []
    for index, (lowest, highest) in enumerate(chunks):
        for copy in reads[index]:
            copy.wait()
        stop = top - lowest + 1 + (1 if lowest == 0 else 0)
        total = lax.fori_loop(start, stop, step, total)
        start = stop

    line = spread_rows([total], 1)
    lane = lax.broadcasted_iota(jnp.int32, (1, 128), 1)
    lane_p = lax.broadcasted_iota(jnp.int32, (g.pairs, 128), 1)
    row_p = lax.broadcasted_iota(jnp.int32, (g.pairs, 128), 0)
    for i in range(ITERS):
        tiles = [peaks0[pair] if i == 0 else peaks[i - 1, pair] for pair in range(g.pairs)]
        rows = jnp.concatenate([jnp.max(tile, axis=0, keepdims=True) for tile in tiles], 0)
        found = jnp.zeros((1, 128), F32)
        for half in range(2):
            inside = lane_p // HALF == half
            column = jnp.max(jnp.where(inside, rows, 0.0), axis=1, keepdims=True)
            place = row_p // g.ct * g.cb + row_p % g.ct * 2 + half
            found = found + jnp.sum(jnp.where(lane_p == place, column, 0.0), axis=0, keepdims=True)
        errors[i : i + 1, :] = found
        line = jnp.where(lane == 1 + i, jnp.max(found, axis=1, keepdims=True), line)
    writes.append(fetch(errors, errors_out, out_sems.at[0]))
    line = jnp.where(lane == 1 + ITERS, live_cells(g, meta, ITERS - 1), line)
    out[...] = jnp.broadcast_to(line, out.shape)
    for write in writes:
        write.wait()


def finish_body(g, parts, table_in, change, r3, out_hbm, worst_out, table, out, worst, sems, out_sems):
    quarter = BLOCK_Z // 4
    spans = [slice(part * quarter, (part + 1) * quarter) for part in range(4)]
    reads = []
    for part, span in enumerate(spans):
        group = [pltpu.make_async_copy(table_in.at[span], table.at[span], sems.at[3 * part])]
        reads.append(group)
    for group in reads:
        for read in group:
            read.start()
    total = lane_values(jnp.sum(parts[...], axis=0, keepdims=True), 1)[0]
    largest = lane_values(jnp.max(parts[...], axis=0, keepdims=True), 2 + ITERS)
    w3 = jnp.broadcast_to(weight_of(total, largest[1 + ITERS]), TILE)
    for i in range(ITERS):
        worst[i] = jnp.max(largest[1 + i])
    writes = [fetch(worst, worst_out, out_sems.at[4])]
    for part, span in enumerate(spans):
        for read in reads[part]:
            read.wait()
        for z in range(part * quarter, (part + 1) * quarter):
            for col in range(g.ct):
                lanes = slice(col * LANES, (col + 1) * LANES)
                for vt in range(g.vt):
                    rows = tile_rows(vt)
                    out[z, rows, lanes] = table[z, rows, lanes] + (change[col, z, rows, :] + w3 * r3[col, z, rows, :])
        writes.append(pltpu.make_async_copy(out.at[span], out_hbm.at[span], out_sems.at[part]))
        writes[-1].start()
    for write in writes:
        write.wait()


def index_table(g, assign):
    zm_here, zv_here = lax.axis_index("zm"), lax.axis_index("zv")
    me = zm_here * g.zv + zv_here
    slots = assign.reshape(ITERS, -1)
    owner = jnp.arange(slots.shape[1]) // g.slots // g.zv
    owner = jnp.where(jnp.arange(ITERS)[:, None] == ITERS - 1, owner ^ zm_here, owner)
    column = jnp.arange(2 * g.blocks + 2 * g.cb)
    here = column % g.blocks
    far = jnp.where(column < 2 * g.blocks, column // g.blocks, (column - 2 * g.blocks) // g.cb)
    local = jnp.where(column < 2 * g.blocks, here, (column - 2 * g.blocks) % g.cb)
    side = jnp.where(column < 2 * g.blocks, 0, 1)
    inside = (zm_here + far < g.zm) & (zv_here + side < g.zv)
    target = jnp.where(inside, (me + far * g.zv + side) * g.blocks + local, -2)
    found = jnp.max(jnp.where(slots[:, None, :] == target[None, :, None], owner[:, None, :], -1), axis=2)
    count = jnp.sum((slots >= 0).astype(jnp.int32), axis=1, keepdims=True)
    flags = jnp.stack([zm_here == g.zm - 1, zv_here == g.zv - 1]).astype(jnp.int32)
    gap = jnp.zeros((ITERS, 120 - found.shape[1]), jnp.int32)
    flags = jnp.broadcast_to(flags[None, :], (ITERS, 2))
    return jnp.concatenate([found, gap, flags, count, jnp.zeros((ITERS, 5), jnp.int32)], axis=1)


def to_all(rows):
    count = lax.axis_size("zm") * lax.axis_size("zv")
    return lax.all_to_all(rows.reshape(count, 1, 128), AXES, 0, 0, tiled=True).reshape(count, 128)


def from_next(value, axis):
    count = lax.axis_size(axis)
    return lax.ppermute(value, axis, [(i, i - 1) for i in range(1, count)])


def shards(table, refined, assign):
    g = Shape(table.shape, assign.shape, lax.axis_size("zm"), lax.axis_size("zv"))
    everyone = g.zm * g.zv
    part = functools.partial
    slots = assign.transpose(0, 2, 1).reshape(ITERS * g.slots, -1)
    views = refined.reshape(ITERS * g.slots, BLOCK_Z // 8, 8, PAIRS, LANES).transpose(0, 1, 3, 2, 4)
    views = views.reshape(ITERS * g.slots, ROWS, LANES)
    vmem = lambda *shape: pltpu.VMEM(shape, F32)
    main, halo = g.main, g.halo

    packed, top = call(
        part(pack_three_body, g), [struct(g.zm, OFFSET[3], LANES), struct(ITERS, *table.shape[1:])], [HBM] * 3, [HBM] * 2,
        [pltpu.SMEM(slots.shape, jnp.int32), pltpu.SMEM((ITERS, g.zm), jnp.int32), vmem(3 * g.slots, ROWS, LANES), vmem(g.zm, OFFSET[3] - 3 * ROWS, LANES),
         vmem(ITERS, *table.shape[1:]), dma(5), dma(3 * g.zm + 4)],
        60,
    )(slots, views, table)
    below = from_next(top, "zm")
    data = lax.all_to_all(packed, "zm", 0, 0, tiled=True)
    strip = jnp.concatenate([table[:, :8], below[:, :8]], 0)
    strip = from_next(strip, "zv")
    packed = call(
        part(pack_last_body, g), [struct(ROWS, LANES)] * g.zm, [SMEM, HBM], [VMEM] * g.zm,
        [pltpu.SMEM((ITERS, g.zm), jnp.int32), dma(g.zm)], WHOLE,
    )(slots, views)
    last_data = [packed[0]]
    for k in range(1, g.zm):
        last_data.append(lax.ppermute(packed[k], "zm", [(i, i ^ k) for i in range(g.zm)]))
    meta = index_table(g, assign)
    interp, interp_halo = call(
        part(interp_body, g), [struct(*main(LAYERS[0])), struct(*halo(LAYERS[0]))],
        [SMEM] + [VMEM] * 3, [VMEM] * 2, [vmem(*main(DEEP)), vmem(*halo(DEEP))], PART,
    )(meta, table, below, strip)

    strips = call(
        part(strip_body, g), struct(sum(LAYERS[:2]), *TILE), [SMEM] + [HBM] * 3, VMEM,
        [vmem(3 * g.cb, ROWS, LANES), vmem(g.ct, sum(LAYERS[:3]), BLOCK_V, LANES), dma(9 * g.cb)],
        PART,
    )(meta, data, interp_halo, packed[0])
    strips = from_next(strips, "zv")
    own, more, most = struct(*main(BLOCK_Z)), struct(*main(LAYERS[2])), struct(*main(LAYERS[1]))
    a0, a1, a2, totals, peaks0 = call(
        part(local_body, g), [struct(*main(LAYERS[0])), most, more, struct(3, *TILE), struct(g.pairs, *TILE)],
        [HBM] * 3, [HBM] * 5,
        [pltpu.SMEM(meta.shape, jnp.int32), pltpu.SMEM((ITERS, g.blocks), jnp.int32), vmem(3, *TILE),
         vmem(g.pairs, *TILE), vmem(*data.shape)]
        + [vmem(*main(LAYERS[0]))] * 7
        + [vmem(3, 2, g.pairs, *TILE), dma(9), dma(14)], WHOLE,
    )(meta, data, interp)
    wide = struct(*g.wide_main(LAYERS[2]))
    products, ca0, ca1, cb1 = call(
        part(middle_body, g), [struct(everyone, 128), wide, wide, wide],
        [HBM] * 7, [VMEM] + [HBM] * 3,
        [pltpu.SMEM(meta.shape, jnp.int32), vmem(*strips.shape), vmem(*interp_halo.shape), vmem(3, *TILE)]
        + [vmem(*main(LAYERS[0] + 1))] * 4 + [vmem(*g.wide_main(LAYERS[0] + 1))] * 3 + [vmem(*halo(LAYERS[0] + 1))] * 3
        + [vmem(2, 2, g.pairs, *TILE), dma(13), dma(13)],
        WHOLE,
    )(meta, strips, interp_halo, totals, a0, a1, a2)
    products, *last_data = lax.optimization_barrier((products, *last_data))
    products = to_all(products)
    change, r3, errors, stats = call(
        part(last_body, g), [own, own, struct(ITERS, 128), struct(everyone, 128)],
        [HBM, VMEM] + [HBM] * (10 + g.zm), [VMEM] * 2 + [HBM, VMEM],
        [pltpu.SMEM(meta.shape, jnp.int32), pltpu.SMEM((ITERS, g.blocks), jnp.int32), vmem(*strips.shape),
         vmem(*interp_halo.shape), vmem(*peaks0.shape), vmem(ITERS, 128), vmem(g.zm * ROWS, LANES)] + [vmem(*main(BLOCK_Z))] * 3 + [vmem(*main(LAYERS[2])), vmem(*main(BLOCK_Z))]
        + [vmem(*g.wide_main(LAYERS[2]))] * 3 + [vmem(*main(LAYERS[2])), vmem(*halo(LAYERS[2])), vmem(*main(LAYERS[2]))]
        + [vmem(3, 2, g.pairs, *TILE), vmem(3, g.pairs, *TILE), dma(g.zm + 33), dma(1)],
        50.5,
    )(meta, products, strips, interp_halo, peaks0, a0, a1, a2, interp, ca0, ca1, cb1, *last_data)
    stats = to_all(stats)
    table_out, worst = call(
        part(finish_body, g), [struct(*table.shape), struct(ITERS)], [VMEM, HBM, VMEM, VMEM], [HBM] * 2,
        [vmem(*table.shape), vmem(*table.shape), pltpu.SMEM((ITERS,), F32), dma(12), dma(5)],
        30,
    )(stats, table, change, r3)
    return (table_out, errors[:, : g.blocks], worst)


def solution(mesh):
    in_specs = (P("zm", "zv", None), P(None, ("zm", "zv"), None, None), P())
    out_specs = (P("zm", "zv", None), P(None, ("zm", "zv")), P())

    return jax.shard_map(shards, mesh=mesh, in_specs=in_specs, out_specs=out_specs, check_vma=False)
```

```python
import functools

import jax
import jax.numpy as jnp
from jax import lax
from jax.experimental import pallas as pl
from jax.experimental.pallas import tpu as pltpu
from jax.sharding import PartitionSpec as P


S = 8
BLOCK_Z = 16
BLOCK_V = 16
BLOCK_C = 8
ITERS = 4
HALF = BLOCK_C * S
PAIRS = BLOCK_V // 2
LANES = 2 * HALF
ROWS = BLOCK_Z * PAIRS
DEEP = BLOCK_Z + ITERS
AXES = ("zm", "zv")
F32 = jnp.float32
TILE = (PAIRS, LANES)


def halo_rows(iteration):
    return ITERS - 1 - iteration


LAYERS = [BLOCK_Z + halo_rows(i) for i in range(ITERS)]
OFFSET = [sum(LAYERS[:i]) * PAIRS for i in range(ITERS)]


def lane_ids():
    return lax.broadcasted_iota(jnp.int32, TILE, 1)


def sub_ids():
    return lax.broadcasted_iota(jnp.int32, TILE, 0)


VMEM = pl.BlockSpec(memory_space=pltpu.VMEM)
SMEM = pl.BlockSpec(memory_space=pltpu.SMEM)
HBM = pl.BlockSpec(memory_space=pltpu.HBM)
WHOLE = 53.5
PART = 24


def call(body, outs, in_specs, out_specs, scratch, limit, flops=2000000):
    return pl.pallas_call(
        body,
        out_shape=outs,
        in_specs=in_specs,
        out_specs=out_specs,
        scratch_shapes=list(scratch),
        compiler_params=pltpu.CompilerParams(vmem_limit_bytes=int(limit * (1 << 20))),
        cost_estimate=pl.CostEstimate(flops=flops, bytes_accessed=1 << 20, transcendentals=0),
    )


def struct(*shape, dtype=F32):
    return jax.ShapeDtypeStruct(shape, dtype)


def dma(count):
    return pltpu.SemaphoreType.DMA((count,))


class Shape:
    def __init__(self, table, assign, zm_count, zv_count):
        self.zm, self.zv = zm_count, zv_count
        self.span, self.wide = table[1], table[2]
        self.vb = self.span // BLOCK_V
        self.cb = self.wide // HALF
        self.vt = self.span // 8
        self.ct = self.wide // LANES
        self.blocks = self.vb * self.cb
        self.pairs = self.vb * self.ct
        self.slots = assign[2]
        self.cells = BLOCK_Z * BLOCK_V * BLOCK_C * S

    def main(self, layers):
        return (self.ct, layers, self.span, LANES)

    def wide_main(self, layers):
        return (self.ct, layers, self.span + 8, LANES)

    def halo(self, layers):
        return (self.ct, layers, 8, LANES)


def fill_inverse(g, iterations, assign, inverse):
    me = lax.axis_index("zm") * g.zv + lax.axis_index("zv")
    for t in iterations:
        for peer in range(g.zm):
            inverse[t, peer] = 0
        for slot in range(g.slots):
            block = assign[t * g.slots + slot, me]

            @pl.when(block >= 0)
            def _():
                inverse[t, block // (g.blocks * g.zv)] = slot


def pack_three_body(g, assign_in, refined, table, out, top, assign, inverse, held, extras, rows_held, sems, out_sems):
    three = range(ITERS - 1)
    spans = [slice(t * g.slots, (t + 1) * g.slots) for t in three]
    reads = [pltpu.make_async_copy(refined.at[span], held.at[span], sems.at[t]) for t, span in enumerate(spans)]
    rows_in = pltpu.make_async_copy(table.at[0:ITERS], rows_held, sems.at[3])
    rows_out = pltpu.make_async_copy(rows_held, top, out_sems.at[3 * g.zm + 3])
    numbers = fetch(assign_in, assign, sems.at[4])
    for read in reads:
        read.start()
    rows_in.start()
    numbers.wait()
    fill_inverse(g, three, assign, inverse)
    rows_in.wait()
    rows_out.start()
    writes = []
    for t in three:
        reads[t].wait()
        for peer in range(g.zm):
            source = held.at[t * g.slots + inverse[t, peer]]
            target = out.at[peer, OFFSET[t] : OFFSET[t] + ROWS, :]
            writes.append(pltpu.make_async_copy(source, target, out_sems.at[t * g.zm + peer]))
            writes[-1].start()
    for t in three:
        first = OFFSET[t] - t * ROWS
        for peer in range(g.zm):
            after = t * g.slots + inverse[t, min(peer + 1, g.zm - 1)]
            for z in range(halo_rows(t)):
                at = first + z * PAIRS
                extras[peer, at : at + PAIRS, :] = held[after, pl.ds(z, PAIRS, stride=8), :]
        count = halo_rows(t) * PAIRS
        target = out.at[:, OFFSET[t] + ROWS : OFFSET[t + 1], :]
        writes.append(pltpu.make_async_copy(extras.at[:, first : first + count, :], target, out_sems.at[3 * g.zm + t]))
        writes[-1].start()
    for write in writes:
        write.wait()
    rows_out.wait()


def pack_last_body(g, assign, refined, *rest):
    outs, inverse, sems = rest[: g.zm], rest[-2], rest[-1]
    t = ITERS - 1
    fill_inverse(g, [t], assign, inverse)
    here = lax.axis_index("zm")
    copies = []
    for k in range(g.zm):
        source = refined.at[t * g.slots + inverse[t, here ^ k]]
        copies.append(pltpu.make_async_copy(source, outs[k], sems.at[k]))
    for copy in copies:
        copy.start()
    for copy in copies:
        copy.wait()


def pair_tiles(left, first, second):
    even = jnp.where(left, first, pltpu.roll(second, HALF, 1))
    odd = jnp.where(left, pltpu.roll(first, HALF, 1), second)
    return even, odd


def pair_live(meta, iteration, column, left):
    first, second = meta[iteration, column] >= 0, meta[iteration, column + 1] >= 0
    return (left & first) | (~left & second)


def fetch(source, target, sem):
    copy = pltpu.make_async_copy(source, target, sem)
    copy.start()
    return copy


def strip_body(g, meta, data, unused_a, unused_b, out):
    left = lane_ids() < HALF
    for t in range(ITERS - 1):
        columns = (4, 2, 2)[t]
        base = (0, LAYERS[0] * 8, LAYERS[0] * 8 + 4)[t]
        for col in range(g.ct):
            mine = [jnp.maximum(meta[t, 2 * col + half], 0) for half in range(2)]
            far = [jnp.maximum(meta[t, g.blocks + 2 * col + half], 0) for half in range(2)]
            row = base + col * columns
            for zt in range(2):
                for j in range(columns // 2):
                    at = OFFSET[t] + zt * 8 * PAIRS + j * 8
                    even, odd = pair_tiles(left, *[data[owner, at : at + 8, :] for owner in mine])
                    out[pl.ds(row + zt * 64 + 2 * j, 8, stride=8), :] = even
                    out[pl.ds(row + zt * 64 + 2 * j + 1, 8, stride=8), :] = odd
            for z in range(BLOCK_Z, LAYERS[t]):
                at = OFFSET[t] + z * PAIRS
                even, odd = pair_tiles(left, *[data[owner, at : at + PAIRS, :] for owner in far])
                for j in range(columns // 2):
                    first = row + z * 8 + 2 * j
                    out[first : first + 1, :] = even[j : j + 1, :]
                    out[first + 1 : first + 2, :] = odd[j : j + 1, :]


def strip_tile(strips, t, z, col):
    tile = strips[z] if t == 0 else strips[LAYERS[0] + z]
    shift = (4 * col, 2 * col, 4 + 2 * col)[t]
    return pltpu.roll(tile, 8 - shift, 0) if shift else tile


class Stencil:
    def __init__(self, g, edge):
        self.g = g
        lane, sub = lane_ids(), sub_ids()
        self.inner = lane < LANES - S
        self.above = sub < 7
        self.last = edge & (sub == 7)

    def __call__(self, get, z, low):
        g = self.g
        sums, turned = {}, {}
        for vt in range(g.vt + 1):
            for col in range(g.ct):
                sums[col, vt] = get(col, vt, z) + get(col, vt, low)
                turned[col, vt] = pltpu.roll(sums[col, vt], LANES - S, 1)
        both, up = {}, {}
        for vt in range(g.vt + 1):
            for col in range(g.ct):
                beside = sums[col, vt] if col == g.ct - 1 else turned[col + 1, vt]
                both[col, vt] = sums[col, vt] + jnp.where(self.inner, turned[col, vt], beside)
                up[col, vt] = pltpu.roll(both[col, vt], 7, 0)
        result = {}
        for vt in range(g.vt + 1):
            for col in range(g.ct):
                value = up[col, vt]
                if vt < g.vt:
                    value = jnp.where(self.above, value, up[col, vt + 1])
                if vt == g.vt - 1:
                    value = jnp.where(self.last, both[col, vt], value)
                result[col, vt] = 0.125 * (both[col, vt] + value)
        return result


def edges(meta):
    return meta[0, 120] == 1, meta[0, 121] == 1


def layer_below(z, edge):
    return jnp.where((z == BLOCK_Z - 1) & edge, z, z + 1)


def clip(z, top):
    return jnp.minimum(jnp.maximum(z, 0), top)


def tile_rows(vt):
    return slice(vt * 8, vt * 8 + 8)


def reader(g, main, halo):
    return lambda col, vt, z: halo[col, z] if vt == g.vt else main[col, z, tile_rows(vt), :]


def put(g, main, halo, z, values):
    for (col, vt), value in values.items():
        if vt == g.vt:
            halo[col, z] = value
        else:
            main[col, z, tile_rows(vt), :] = value


def put_wide(main, z, values):
    for (col, vt), value in values.items():
        main[col, z, tile_rows(vt), :] = value


def interp_body(g, meta, table, below, strip, interp, interp_halo, nodes, nodes_halo):
    edge_z, edge_v = edges(meta)
    stencil = Stencil(g, edge_v)

    def take(source, z, target):
        for col in range(g.ct):
            lanes = slice(col * LANES, (col + 1) * LANES)
            nodes[col, target] = source[z, :, lanes]
            nodes_halo[col, target] = strip[target, :, lanes]

    @pl.loop(0, BLOCK_Z)
    def _(z):
        take(table, z, z)

    @pl.loop(0, ITERS)
    def _(z):
        take(below, z, BLOCK_Z + z)

    get = reader(g, nodes, nodes_halo)

    @pl.loop(0, LAYERS[0])
    def _(z):
        put(g, interp, interp_halo, z, stencil(get, z, layer_below(z, edge_z)))


PRODUCTS = 14


def spread_rows(values, count):
    rows = [jnp.sum(value, axis=0, keepdims=True) for value in values]
    rows += [jnp.zeros_like(rows[0])] * (-len(rows) % 8)
    column = jnp.sum(jnp.concatenate(rows, 0), axis=1, keepdims=True)
    lane = lax.broadcasted_iota(jnp.int32, (len(rows), 128), 1)
    row = lax.broadcasted_iota(jnp.int32, (len(rows), 128), 0)
    line = jnp.sum(jnp.where(lane == row, column, 0.0), axis=0, keepdims=True)
    return jnp.broadcast_to(line, (count, 128))


def fill_masks(g, meta, masks, iterations, left):
    for at, t in enumerate(iterations):
        for far in range(2):
            for pair in range(g.pairs):
                column = pair // g.ct * g.cb + pair % g.ct * 2 + far * g.blocks
                masks[at, far, pair] = jnp.where(pair_live(meta, t, column, left), 1.0, 0.0)


def halo_live(g, meta, iteration, left):
    first = 2 * g.blocks
    return [[pair_live(meta, iteration, first + far * g.cb + 2 * col, left) for col in range(g.ct)] for far in range(2)]


def segments(top, counts):
    result, high = [], top
    for count in counts:
        result.append((high - count + 1, high))
        high -= count
    return result


def fill_first_rows(g, meta, iterations, rows, first_rows):
    for t in iterations:
        for block in range(g.blocks):
            first_rows[t, block] = jnp.maximum(meta[t, block], 0) * rows + (OFFSET[t] if t < ITERS - 1 else 0)


def convert(g, first_rows, t, held, z, out, left):
    row = z // 8 * 8 * PAIRS + z % 8
    for pair in range(g.pairs):
        vb, col = pair // g.ct, pair % g.ct
        tiles = []
        for half in range(2):
            tiles.append(held[pl.ds(first_rows[t, vb * g.cb + 2 * col + half] + row, PAIRS, stride=8), :])
        even, odd = pair_tiles(left, *tiles)
        out[col, z, pl.ds(vb * BLOCK_V, PAIRS, stride=2), :] = even
        out[col, z, pl.ds(vb * BLOCK_V + 1, PAIRS, stride=2), :] = odd


def between(z):
    return jnp.where((z >= 0) & (z < BLOCK_Z), 1.0, 0.0)


def pair_tile_rows(g, pair):
    return [tile_rows(vt) for vt in (pair // g.ct * 2, pair // g.ct * 2 + 1)]


def local_body(g, meta_in, data, interp_in, a0_out, a1_out, a2_out, totals_out, peaks_out,
               meta, first_rows, totals, peaks, arrived, interp, f0, f1, f2, a0, a1, a2, masks, sems, out_sems):
    meta_copy = fetch(meta_in, meta, sems.at[8])
    held = arrived.reshape(g.zm * OFFSET[3], LANES)
    f, a, outs = (f0, f1, f2), (a0, a1, a2), (a0_out, a1_out, a2_out)
    split = BLOCK_Z // 2
    groups = ([], [])
    for t in range(3):
        first, middle, end = OFFSET[t], OFFSET[t] + ROWS // 2, OFFSET[t + 1]
        for group, rows in ((0, slice(middle, end)), (1, slice(first, middle))):
            copy = pltpu.make_async_copy(data.at[:, rows, :], arrived.at[:, rows, :], sems.at[2 * t + group])
            groups[group].append(copy)
    for group, layers in ((0, slice(split, LAYERS[0])), (1, slice(0, split))):
        groups[group].append(pltpu.make_async_copy(interp_in.at[:, layers], interp.at[:, layers], sems.at[6 + group]))
    for group in groups:
        for copy in group:
            copy.start()
    left = lane_ids() < HALF
    peaks[...] = jnp.zeros_like(peaks)
    meta_copy.wait()
    fill_first_rows(g, meta, range(3), OFFSET[3], first_rows)
    fill_masks(g, meta, masks, (0, 1, 2), left)
    for copy in groups[0]:
        copy.wait()

    for pair in range(g.pairs):
        vb, col = pair // g.ct, pair % g.ct
        row = vb * BLOCK_V
        column = g.blocks + vb * g.cb + 2 * col
        for t in range(3):
            starts = [jnp.maximum(meta[t, column + half], 0) * OFFSET[3] for half in range(2)]
            for z in range(BLOCK_Z, LAYERS[t]):
                at = [pl.multiple_of(start + OFFSET[t] + z * PAIRS, PAIRS) for start in starts]
                even, odd = pair_tiles(left, *[held[pl.ds(row_at, PAIRS), :] for row_at in at])
                f[t][col, z, pl.ds(row, PAIRS, stride=2), :] = even
                f[t][col, z, pl.ds(row + 1, PAIRS, stride=2), :] = odd
        for t in range(3):
            live = masks[t, 1, pair] > 0.5
            for z in range(BLOCK_Z, LAYERS[t]):
                for half in range(2):
                    rows = pl.ds(row + 8 * half, 8)
                    value = f[t][col, z, rows, :] - interp[col, z, rows, :]
                    a[t][col, z, rows, :] = jnp.where(live, value, 0.0)

    def step(i, carry):
        carry = list(carry)
        base = BLOCK_Z - 1 - i
        at = clip(base + 1, BLOCK_Z - 1)
        inside = jnp.full(TILE, between(base + 1), F32) > 0.5
        for pair in range(g.pairs):
            col = pair % g.ct
            peak = peaks[pair]
            for rows in pair_tile_rows(g, pair):
                mean = interp[col, at, rows, :]
                for t in range(3):
                    live = (masks[t, 0, pair] > 0.5) & inside
                    value = jnp.where(live, f[t][col, at, rows, :] - mean, 0.0)
                    a[t][col, at, rows, :] = value
                    carry[t] = carry[t] + value * value
                    if t == 0:
                        peak = jnp.maximum(peak, jnp.abs(value))
            peaks[pair] = peak
        at = clip(base, BLOCK_Z - 1)
        for t in range(3):
            convert(g, first_rows, t, held, at, f[t], left)
        return tuple(carry)

    carry = (jnp.zeros(TILE, F32),) * 3
    writes, bounds = [], (0, split, split + 4, BLOCK_Z - 1, BLOCK_Z + 1)
    for index in range(4):
        if index == 1:
            for copy in groups[1]:
                copy.wait()
        carry = lax.fori_loop(bounds[index], bounds[index + 1], step, carry)
        lowest = BLOCK_Z - bounds[index + 1] + 1
        for t in range(3):
            highest = BLOCK_Z - bounds[index] if index else LAYERS[t] - 1
            span = slice(lowest, highest + 1)
            writes.append(fetch(a[t].at[:, span], outs[t].at[:, span], out_sems.at[index * 3 + t]))
    for t in range(3):
        totals[t] = carry[t]
    writes.append(fetch(totals, totals_out, out_sems.at[12]))
    writes.append(fetch(peaks, peaks_out, out_sems.at[13]))
    for write in writes:
        write.wait()


def middle_body(g, meta_in, strips_in, interp_halo_in, totals_in, a0_in, a1_in, a2_in,
                out, ca0_out, ca1_out, cb1_out,
                meta, strips, interp_halo, totals, a0, a1, a2, b1, ca0, ca1, cb1, a0_halo, a1_halo, b1_halo, masks, sems, out_sems):
    cuts = (12, 6, 0)
    groups, at = ([], [], []), 9
    small = []
    for source, target in ((meta_in, meta), (strips_in, strips), (interp_halo_in, interp_halo), (totals_in, totals)):
        small.append(fetch(source, target, sems.at[at]))
        at += 1
    at = 0
    for source, target, layers in ((a0_in, a0, LAYERS[0]), (a1_in, a1, LAYERS[1]), (a2_in, a2, BLOCK_Z)):
        for group, span in enumerate((slice(cuts[0], layers), slice(cuts[1], cuts[0]), slice(0, cuts[1]))):
            groups[group].append(pltpu.make_async_copy(source.at[:, span], target.at[:, span], sems.at[at]))
            at += 1
    for group in groups:
        for copy in group:
            copy.start()
    none = LAYERS[0]
    for col in range(g.ct):
        for field in (a1, a2, b1):
            field[col, none] = jnp.zeros((g.span, LANES), F32)
        ca0[col, none] = jnp.zeros((g.span + 8, LANES), F32)
    for copy in small:
        copy.wait()
    edge_z, edge_v = edges(meta)
    stencil = Stencil(g, edge_v)
    left = lane_ids() < HALF
    live0, live1 = halo_live(g, meta, 0, left), halo_live(g, meta, 1, left)
    fill_masks(g, meta, masks, (1, 2), left)
    for pair in range(g.pairs):
        masks[1, 1, pair] = jnp.zeros(TILE, F32)
    for col in range(g.ct):
        for z in range(LAYERS[0]):
            value = strip_tile(strips, 0, z, col) - interp_halo[col, z]
            a0_halo[col, z] = jnp.where(live0[z >= BLOCK_Z][col], value, 0.0)
        for z in range(LAYERS[1]):
            value = strip_tile(strips, 1, z, col) - interp_halo[col, z]
            a1_halo[col, z] = jnp.where(live1[z >= BLOCK_Z][col], value, 0.0)
    get0, get1, getb = reader(g, a0, a0_halo), reader(g, a1, a1_halo), reader(g, b1, b1_halo)
    top0, top1 = LAYERS[1] - 1, LAYERS[2] - 1
    for copy in groups[0]:
        copy.wait()

    def step(i, carry):
        carry = list(carry)
        base = top0 - i
        z = base + 1
        at = clip(z, top1)
        low = layer_below(at, edge_z)
        after_a = stencil(get1, at, low)
        after_b = stencil(getb, at, low)
        put_wide(ca1, at, after_a)
        put_wide(cb1, at, after_b)
        own = (z >= 0) & (z < BLOCK_Z)
        row, kind = jnp.where(own, z, none), jnp.where(own, 0, 1)
        for pair in range(g.pairs):
            col = pair % g.ct
            live = masks[1, kind, pair] > 0.5
            for half, rows in enumerate(pair_tile_rows(g, pair)):
                vt = pair // g.ct * 2 + half
                one, two = a1[col, row, rows, :], b1[col, row, rows, :]
                carry[0] = carry[0] + one * two
                carry[1] = carry[1] + two * two
                parts = [a2[col, row, rows, :]] + [
                    jnp.where(live, value, 0.0) for value in (ca0[col, row, rows, :], after_a[col, vt], after_b[col, vt])
                ]
                slot = 2
                for m in range(4):
                    for n in range(max(m, 1), 4):
                        carry[slot] = carry[slot] + parts[m] * parts[n]
                        slot += 1
        at = clip(base, top0)
        after = stencil(get0, at, layer_below(at, edge_z))
        put_wide(ca0, at, after)
        far = jnp.where(at >= BLOCK_Z, 1, 0)
        for (col, vt), value in after.items():
            if vt == g.vt:
                live = (live1[0][col] & (at < BLOCK_Z)) | (live1[1][col] & (at >= BLOCK_Z))
                b1_halo[col, at] = jnp.where(live, value, 0.0)
            else:
                mask = masks[0, far, vt // 2 * g.ct + col]
                b1[col, at, tile_rows(vt), :] = jnp.where(mask > 0.5, value, 0.0)
        return tuple(carry)

    carry = (jnp.zeros(TILE, F32),) * 11
    writes = []
    bounds = (0, top0 - cuts[0] + 1, top0 - cuts[1] + 1, top0, top0 + 2)
    for index in range(4):
        if index in (1, 2):
            for copy in groups[index]:
                copy.wait()
        carry = lax.fori_loop(bounds[index], bounds[index + 1], step, carry)
        lowest = top0 - bounds[index + 1] + 2
        highest = top0 - bounds[index] + 1 if index else top1
        for which, (source, target) in enumerate(((ca0, ca0_out), (ca1, ca1_out), (cb1, cb1_out))):
            span = slice(lowest, highest + 1)
            writes.append(fetch(source.at[:, span], target.at[:, span], out_sems.at[index * 3 + which]))
    values = [totals[0], totals[1], carry[0], carry[1], totals[2]] + list(carry[2:])
    out[...] = spread_rows(values, out.shape[0])
    for write in writes:
        write.wait()


def weight_of(total, count):
    return 1.0 / (1.0 + jnp.sqrt(jnp.maximum(total, 0.0) / count))


def lane_values(line, count):
    lane = lax.broadcasted_iota(jnp.int32, line.shape, 1)
    return [jnp.sum(jnp.where(lane == i, line, 0.0), axis=1, keepdims=True) for i in range(count)]


def live_cells(g, meta, iteration):
    return jnp.full((1, 1), meta[iteration, 122], jnp.int32).astype(F32) * F32(g.cells)


def three_weights(g, meta, parts):
    q = lane_values(jnp.sum(parts[...], axis=0, keepdims=True), PRODUCTS)
    w0 = weight_of(q[0], live_cells(g, meta, 0))
    w1 = weight_of(q[1] - 2.0 * w0 * q[2] + w0 * w0 * q[3], live_cells(g, meta, 1))
    f = [jnp.ones_like(w0), -w0, -w1, w0 * w1]
    total, at = jnp.zeros_like(w0), 4
    for i in range(4):
        for j in range(i, 4):
            total = total + (1.0 if i == j else 2.0) * f[i] * f[j] * q[at]
            at += 1
    return [jnp.broadcast_to(w, TILE) for w in (w0, w1, weight_of(total, live_cells(g, meta, 2)))]


def last_body(g, meta_in, parts, strips_in, interp_halo_in, peaks0_in, a0_in, a1_in, a2_in, interp_in, ca0_in, ca1_in, cb1_in,
              *rest):
    data, rest = rest[: g.zm], rest[g.zm :]
    (sum_out, r3, errors_out, out,
     meta, first_rows, strips, interp_halo, peaks0, errors, held, f3, a0, a1, a2, interp, ca0, ca1, cb1, r2, r2_halo, change, masks, peaks, sems, out_sems) = rest
    top = LAYERS[2] - 1
    small = []
    for source, target in ((meta_in, meta), (strips_in, strips), (interp_halo_in, interp_halo), (peaks0_in, peaks0)):
        small.append(fetch(source, target, sems.at[g.zm + 28 + len(small)]))
    chunks = segments(top, (3, 5, 5, 4))
    reads, at = [], 0
    for lowest, highest in chunks:
        group = []
        if not reads:
            for k in range(g.zm):
                group.append(pltpu.make_async_copy(data[k], held.at[k * ROWS : (k + 1) * ROWS, :], sems.at[at]))
                at += 1
        for source, target, layers in ((ca0_in, ca0, BLOCK_Z + 1), (ca1_in, ca1, BLOCK_Z + 1), (cb1_in, cb1, BLOCK_Z + 1),
                                       (a0_in, a0, BLOCK_Z), (a1_in, a1, BLOCK_Z), (a2_in, a2, BLOCK_Z + 1),
                                       (interp_in, interp, BLOCK_Z)):
            span = slice(lowest, min(highest + 1, layers))
            group.append(pltpu.make_async_copy(source.at[:, span], target.at[:, span], sems.at[at]))
            at += 1
        reads.append(group)
    for group in reads:
        for copy in group:
            copy.start()
    peaks[...] = jnp.zeros_like(peaks)
    for copy in small:
        copy.wait()
    edge_z, edge_v = edges(meta)
    stencil = Stencil(g, edge_v)
    left = lane_ids() < HALF
    fill_masks(g, meta, masks, (1, 2, 3), left)
    fill_first_rows(g, meta, [ITERS - 1], ROWS, first_rows)
    w0, w1, w2 = three_weights(g, meta, parts)
    w01 = w0 * w1
    live = halo_live(g, meta, 2, left)
    get = reader(g, r2, r2_halo)

    def step(i, total):
        base = top - i
        z = base + 1
        at = clip(z, BLOCK_Z - 1)
        counts = between(z)
        after = stencil(get, at, layer_below(at, edge_z))
        for pair in range(g.pairs):
            col = pair % g.ct
            mask = masks[2, 0, pair] * counts > 0.5
            peak = peaks[2, pair]
            for half, rows in enumerate(pair_tile_rows(g, pair)):
                value = f3[col, at, rows, :] - interp[col, at, rows, :] - change[col, at, rows, :]
                value = jnp.where(mask, value - w2 * after[col, pair // g.ct * 2 + half], 0.0)
                r3[col, at, rows, :] = value
                total = total + value * value
                peak = jnp.maximum(peak, jnp.abs(value))
            peaks[2, pair] = peak
        at = clip(base, top)
        edge = tile_rows(g.vt)
        for col in range(g.ct):
            value = strip_tile(strips, 2, at, col) - interp_halo[col, at] - w0 * ca0[col, at, edge, :]
            value = value - w1 * ca1[col, at, edge, :] + w01 * cb1[col, at, edge, :]
            there = (live[0][col] & (at < BLOCK_Z)) | (live[1][col] & (at >= BLOCK_Z))
            r2_halo[col, at] = jnp.where(there, value, 0.0)
        far = jnp.where(at >= BLOCK_Z, 1, 0)
        own = jnp.minimum(at, BLOCK_Z - 1)
        inside = jnp.full(TILE, between(at), F32) > 0.5
        for pair in range(g.pairs):
            col = pair % g.ct
            mask1, mask2 = masks[0, 0, pair] > 0.5, masks[1, far, pair] > 0.5
            peak1, peak2 = peaks[0, pair], peaks[1, pair]
            for rows in pair_tile_rows(g, pair):
                zero = w0 * ca0[col, at, rows, :]
                whole = zero + w1 * ca1[col, at, rows, :] - w01 * cb1[col, at, rows, :]
                change[col, at, rows, :] = whole
                value = a2[col, at, rows, :] - jnp.where(mask2, whole, 0.0)
                r2[col, at, rows, :] = value
                peak2 = jnp.maximum(peak2, jnp.where(inside, jnp.abs(value), 0.0))
                one = a1[col, own, rows, :] - jnp.where(mask1, zero, 0.0)
                peak1 = jnp.maximum(peak1, jnp.where(inside, jnp.abs(one), 0.0))
                sum_out[col, own, rows, :] = w0 * a0[col, own, rows, :] + w1 * one + w2 * value
            peaks[0, pair] = peak1
            peaks[1, pair] = peak2
        convert(g, first_rows, ITERS - 1, held, own, f3, left)
        return total

    total, start, writes = jnp.zeros(TILE, F32), 0, []
    for index, (lowest, highest) in enumerate(chunks):
        for copy in reads[index]:
            copy.wait()
        stop = top - lowest + 1 + (1 if lowest == 0 else 0)
        total = lax.fori_loop(start, stop, step, total)
        start = stop

    line = spread_rows([total], 1)
    lane = lax.broadcasted_iota(jnp.int32, (1, 128), 1)
    lane_p = lax.broadcasted_iota(jnp.int32, (g.pairs, 128), 1)
    row_p = lax.broadcasted_iota(jnp.int32, (g.pairs, 128), 0)
    for i in range(ITERS):
        tiles = [peaks0[pair] if i == 0 else peaks[i - 1, pair] for pair in range(g.pairs)]
        rows = jnp.concatenate([jnp.max(tile, axis=0, keepdims=True) for tile in tiles], 0)
        found = jnp.zeros((1, 128), F32)
        for half in range(2):
            inside = lane_p // HALF == half
            column = jnp.max(jnp.where(inside, rows, 0.0), axis=1, keepdims=True)
            place = row_p // g.ct * g.cb + row_p % g.ct * 2 + half
            found = found + jnp.sum(jnp.where(lane_p == place, column, 0.0), axis=0, keepdims=True)
        errors[i : i + 1, :] = found
        line = jnp.where(lane == 1 + i, jnp.max(found, axis=1, keepdims=True), line)
    writes.append(fetch(errors, errors_out, out_sems.at[0]))
    line = jnp.where(lane == 1 + ITERS, live_cells(g, meta, ITERS - 1), line)
    out[...] = jnp.broadcast_to(line, out.shape)
    for write in writes:
        write.wait()


def finish_body(g, parts, table_in, change, r3, out_hbm, worst_out, table, out, worst, sems, out_sems):
    quarter = BLOCK_Z // 4
    spans = [slice(part * quarter, (part + 1) * quarter) for part in range(4)]
    reads = []
    for part, span in enumerate(spans):
        group = [pltpu.make_async_copy(table_in.at[span], table.at[span], sems.at[3 * part])]
        reads.append(group)
    for group in reads:
        for read in group:
            read.start()
    total = lane_values(jnp.sum(parts[...], axis=0, keepdims=True), 1)[0]
    largest = lane_values(jnp.max(parts[...], axis=0, keepdims=True), 2 + ITERS)
    w3 = jnp.broadcast_to(weight_of(total, largest[1 + ITERS]), TILE)
    for i in range(ITERS):
        worst[i] = jnp.max(largest[1 + i])
    writes = [fetch(worst, worst_out, out_sems.at[4])]
    for part, span in enumerate(spans):
        for read in reads[part]:
            read.wait()
        for z in range(part * quarter, (part + 1) * quarter):
            for col in range(g.ct):
                lanes = slice(col * LANES, (col + 1) * LANES)
                for vt in range(g.vt):
                    rows = tile_rows(vt)
                    out[z, rows, lanes] = table[z, rows, lanes] + (change[col, z, rows, :] + w3 * r3[col, z, rows, :])
        writes.append(pltpu.make_async_copy(out.at[span], out_hbm.at[span], out_sems.at[part]))
        writes[-1].start()
    for write in writes:
        write.wait()


def index_table(g, assign):
    zm_here, zv_here = lax.axis_index("zm"), lax.axis_index("zv")
    me = zm_here * g.zv + zv_here
    slots = assign.reshape(ITERS, -1)
    owner = jnp.arange(slots.shape[1]) // g.slots // g.zv
    owner = jnp.where(jnp.arange(ITERS)[:, None] == ITERS - 1, owner ^ zm_here, owner)
    column = jnp.arange(2 * g.blocks + 2 * g.cb)
    here = column % g.blocks
    far = jnp.where(column < 2 * g.blocks, column // g.blocks, (column - 2 * g.blocks) // g.cb)
    local = jnp.where(column < 2 * g.blocks, here, (column - 2 * g.blocks) % g.cb)
    side = jnp.where(column < 2 * g.blocks, 0, 1)
    inside = (zm_here + far < g.zm) & (zv_here + side < g.zv)
    target = jnp.where(inside, (me + far * g.zv + side) * g.blocks + local, -2)
    found = jnp.max(jnp.where(slots[:, None, :] == target[None, :, None], owner[:, None, :], -1), axis=2)
    count = jnp.sum((slots >= 0).astype(jnp.int32), axis=1, keepdims=True)
    flags = jnp.stack([zm_here == g.zm - 1, zv_here == g.zv - 1]).astype(jnp.int32)
    gap = jnp.zeros((ITERS, 120 - found.shape[1]), jnp.int32)
    flags = jnp.broadcast_to(flags[None, :], (ITERS, 2))
    return jnp.concatenate([found, gap, flags, count, jnp.zeros((ITERS, 5), jnp.int32)], axis=1)


def to_all(rows):
    count = lax.axis_size("zm") * lax.axis_size("zv")
    return lax.all_to_all(rows.reshape(count, 1, 128), AXES, 0, 0, tiled=True).reshape(count, 128)


def from_next(value, axis):
    count = lax.axis_size(axis)
    return lax.ppermute(value, axis, [(i, i - 1) for i in range(1, count)])


def shards(table, refined, assign):
    g = Shape(table.shape, assign.shape, lax.axis_size("zm"), lax.axis_size("zv"))
    everyone = g.zm * g.zv
    part = functools.partial
    slots = assign.transpose(0, 2, 1).reshape(ITERS * g.slots, -1)
    views = refined.reshape(ITERS * g.slots, BLOCK_Z // 8, 8, PAIRS, LANES).transpose(0, 1, 3, 2, 4)
    views = views.reshape(ITERS * g.slots, ROWS, LANES)
    vmem = lambda *shape: pltpu.VMEM(shape, F32)
    main, halo = g.main, g.halo

    packed, top = call(
        part(pack_three_body, g), [struct(g.zm, OFFSET[3], LANES), struct(ITERS, *table.shape[1:])], [HBM] * 3, [HBM] * 2,
        [pltpu.SMEM(slots.shape, jnp.int32), pltpu.SMEM((ITERS, g.zm), jnp.int32), vmem(3 * g.slots, ROWS, LANES), vmem(g.zm, OFFSET[3] - 3 * ROWS, LANES),
         vmem(ITERS, *table.shape[1:]), dma(5), dma(3 * g.zm + 4)],
        60,
    )(slots, views, table)
    below = from_next(top, "zm")
    data = lax.all_to_all(packed, "zm", 0, 0, tiled=True)
    strip = jnp.concatenate([table[:, :8], below[:, :8]], 0)
    strip = from_next(strip, "zv")
    packed = call(
        part(pack_last_body, g), [struct(ROWS, LANES)] * g.zm, [SMEM, HBM], [VMEM] * g.zm,
        [pltpu.SMEM((ITERS, g.zm), jnp.int32), dma(g.zm)], WHOLE,
    )(slots, views)
    last_data = [packed[0]]
    for k in range(1, g.zm):
        last_data.append(lax.ppermute(packed[k], "zm", [(i, i ^ k) for i in range(g.zm)]))
    meta = index_table(g, assign)
    interp, interp_halo = call(
        part(interp_body, g), [struct(*main(LAYERS[0])), struct(*halo(LAYERS[0]))],
        [SMEM] + [VMEM] * 3, [VMEM] * 2, [vmem(*main(DEEP)), vmem(*halo(DEEP))], PART,
    )(meta, table, below, strip)

    strips = call(
        part(strip_body, g), struct(sum(LAYERS[:2]) * 8, LANES), [SMEM, VMEM, HBM, HBM], VMEM,
        [],
        PART,
    )(meta, data, interp_halo, packed[0])
    strips = from_next(strips, "zv").reshape(sum(LAYERS[:2]), *TILE)
    own, more, most = struct(*main(BLOCK_Z)), struct(*main(LAYERS[2])), struct(*main(LAYERS[1]))
    a0, a1, a2, totals, peaks0 = call(
        part(local_body, g), [struct(*main(LAYERS[0])), most, more, struct(3, *TILE), struct(g.pairs, *TILE)],
        [HBM] * 3, [HBM] * 5,
        [pltpu.SMEM(meta.shape, jnp.int32), pltpu.SMEM((ITERS, g.blocks), jnp.int32), vmem(3, *TILE),
         vmem(g.pairs, *TILE), vmem(*data.shape)]
        + [vmem(*main(LAYERS[0]))] * 7
        + [vmem(3, 2, g.pairs, *TILE), dma(9), dma(14)], WHOLE,
    )(meta, data, interp)
    wide = struct(*g.wide_main(LAYERS[2]))
    products, ca0, ca1, cb1 = call(
        part(middle_body, g), [struct(everyone, 128), wide, wide, wide],
        [HBM] * 7, [VMEM] + [HBM] * 3,
        [pltpu.SMEM(meta.shape, jnp.int32), vmem(*strips.shape), vmem(*interp_halo.shape), vmem(3, *TILE)]
        + [vmem(*main(LAYERS[0] + 1))] * 4 + [vmem(*g.wide_main(LAYERS[0] + 1))] * 3 + [vmem(*halo(LAYERS[0] + 1))] * 3
        + [vmem(2, 2, g.pairs, *TILE), dma(13), dma(13)],
        WHOLE,
    )(meta, strips, interp_halo, totals, a0, a1, a2)
    products, *last_data = lax.optimization_barrier((products, *last_data))
    products = to_all(products)
    change, r3, errors, stats = call(
        part(last_body, g), [own, own, struct(ITERS, 128), struct(everyone, 128)],
        [HBM, VMEM] + [HBM] * (10 + g.zm), [VMEM] * 2 + [HBM, VMEM],
        [pltpu.SMEM(meta.shape, jnp.int32), pltpu.SMEM((ITERS, g.blocks), jnp.int32), vmem(*strips.shape),
         vmem(*interp_halo.shape), vmem(*peaks0.shape), vmem(ITERS, 128), vmem(g.zm * ROWS, LANES)] + [vmem(*main(BLOCK_Z))] * 3 + [vmem(*main(LAYERS[2])), vmem(*main(BLOCK_Z))]
        + [vmem(*g.wide_main(LAYERS[2]))] * 3 + [vmem(*main(LAYERS[2])), vmem(*halo(LAYERS[2])), vmem(*main(LAYERS[2]))]
        + [vmem(3, 2, g.pairs, *TILE), vmem(3, g.pairs, *TILE), dma(g.zm + 33), dma(1)],
        50.5,
    )(meta, products, strips, interp_halo, peaks0, a0, a1, a2, interp, ca0, ca1, cb1, *last_data)
    stats = to_all(stats)
    table_out, worst = call(
        part(finish_body, g), [struct(*table.shape), struct(ITERS)], [VMEM, HBM, VMEM, VMEM], [HBM] * 2,
        [vmem(*table.shape), vmem(*table.shape), pltpu.SMEM((ITERS,), F32), dma(12), dma(5)],
        30,
    )(stats, table, change, r3)
    return (table_out, errors[:, : g.blocks], worst)


def solution(mesh):
    in_specs = (P("zm", "zv", None), P(None, ("zm", "zv"), None, None), P())
    out_specs = (P("zm", "zv", None), P(None, ("zm", "zv")), P())

    return jax.shard_map(shards, mesh=mesh, in_specs=in_specs, out_specs=out_specs, check_vma=False)
```

```python
import functools

import jax
import jax.numpy as jnp
from jax import lax
from jax.experimental import pallas as pl
from jax.experimental.pallas import tpu as pltpu
from jax.sharding import PartitionSpec as P


S = 8
BLOCK_Z = 16
BLOCK_V = 16
BLOCK_C = 8
ITERS = 4
HALF = BLOCK_C * S
PAIRS = BLOCK_V // 2
LANES = 2 * HALF
ROWS = BLOCK_Z * PAIRS
DEEP = BLOCK_Z + ITERS
AXES = ("zm", "zv")
F32 = jnp.float32
TILE = (PAIRS, LANES)


def halo_rows(iteration):
    return ITERS - 1 - iteration


LAYERS = [BLOCK_Z + halo_rows(i) for i in range(ITERS)]
OFFSET = [sum(LAYERS[:i]) * PAIRS for i in range(ITERS)]


def lane_ids():
    return lax.broadcasted_iota(jnp.int32, TILE, 1)


def sub_ids():
    return lax.broadcasted_iota(jnp.int32, TILE, 0)


VMEM = pl.BlockSpec(memory_space=pltpu.VMEM)
SMEM = pl.BlockSpec(memory_space=pltpu.SMEM)
HBM = pl.BlockSpec(memory_space=pltpu.HBM)
WHOLE = 53.5
PART = 24


def call(body, outs, in_specs, out_specs, scratch, limit, flops=2000000):
    return pl.pallas_call(
        body,
        out_shape=outs,
        in_specs=in_specs,
        out_specs=out_specs,
        scratch_shapes=list(scratch),
        compiler_params=pltpu.CompilerParams(vmem_limit_bytes=int(limit * (1 << 20))),
        cost_estimate=pl.CostEstimate(flops=flops, bytes_accessed=1 << 20, transcendentals=0),
    )


def struct(*shape, dtype=F32):
    return jax.ShapeDtypeStruct(shape, dtype)


def dma(count):
    return pltpu.SemaphoreType.DMA((count,))


class Shape:
    def __init__(self, table, assign, zm_count, zv_count):
        self.zm, self.zv = zm_count, zv_count
        self.span, self.wide = table[1], table[2]
        self.vb = self.span // BLOCK_V
        self.cb = self.wide // HALF
        self.vt = self.span // 8
        self.ct = self.wide // LANES
        self.blocks = self.vb * self.cb
        self.pairs = self.vb * self.ct
        self.slots = assign[2]
        self.cells = BLOCK_Z * BLOCK_V * BLOCK_C * S

    def main(self, layers):
        return (self.ct, layers, self.span, LANES)

    def wide_main(self, layers):
        return (self.ct, layers, self.span + 8, LANES)

    def halo(self, layers):
        return (self.ct, layers, 8, LANES)


def fill_inverse(g, iterations, assign, inverse):
    me = lax.axis_index("zm") * g.zv + lax.axis_index("zv")
    for t in iterations:
        for peer in range(g.zm):
            inverse[t, peer] = 0
        for slot in range(g.slots):
            block = assign[t * g.slots + slot, me]

            @pl.when(block >= 0)
            def _():
                inverse[t, block // (g.blocks * g.zv)] = slot


def pack_three_body(g, assign_in, refined, table, out, top, assign, inverse, held, extras, rows_held, sems, out_sems):
    three = range(ITERS - 1)
    spans = [slice(t * g.slots, (t + 1) * g.slots) for t in three]
    reads = [pltpu.make_async_copy(refined.at[span], held.at[span], sems.at[t]) for t, span in enumerate(spans)]
    rows_in = pltpu.make_async_copy(table.at[0:ITERS], rows_held, sems.at[3])
    rows_out = pltpu.make_async_copy(rows_held, top, out_sems.at[3 * g.zm + 3])
    numbers = fetch(assign_in, assign, sems.at[4])
    for read in reads:
        read.start()
    rows_in.start()
    numbers.wait()
    fill_inverse(g, three, assign, inverse)
    rows_in.wait()
    rows_out.start()
    writes = []
    for t in three:
        reads[t].wait()
        for peer in range(g.zm):
            source = held.at[t * g.slots + inverse[t, peer]]
            target = out.at[peer, OFFSET[t] : OFFSET[t] + ROWS, :]
            writes.append(pltpu.make_async_copy(source, target, out_sems.at[t * g.zm + peer]))
            writes[-1].start()
    for t in three:
        first = OFFSET[t] - t * ROWS
        for peer in range(g.zm):
            after = t * g.slots + inverse[t, min(peer + 1, g.zm - 1)]
            for z in range(halo_rows(t)):
                at = first + z * PAIRS
                extras[peer, at : at + PAIRS, :] = held[after, pl.ds(z, PAIRS, stride=8), :]
        count = halo_rows(t) * PAIRS
        target = out.at[:, OFFSET[t] + ROWS : OFFSET[t + 1], :]
        writes.append(pltpu.make_async_copy(extras.at[:, first : first + count, :], target, out_sems.at[3 * g.zm + t]))
        writes[-1].start()
    for write in writes:
        write.wait()
    rows_out.wait()


def pack_last_body(g, assign, refined, *rest):
    outs, inverse, sems = rest[: g.zm], rest[-2], rest[-1]
    t = ITERS - 1
    fill_inverse(g, [t], assign, inverse)
    here = lax.axis_index("zm")
    copies = []
    for k in range(g.zm):
        source = refined.at[t * g.slots + inverse[t, here ^ k]]
        copies.append(pltpu.make_async_copy(source, outs[k], sems.at[k]))
    for copy in copies:
        copy.start()
    for copy in copies:
        copy.wait()


def pair_tiles(left, first, second):
    even = jnp.where(left, first, pltpu.roll(second, HALF, 1))
    odd = jnp.where(left, pltpu.roll(first, HALF, 1), second)
    return even, odd


def pair_live(meta, iteration, column, left):
    first, second = meta[iteration, column] >= 0, meta[iteration, column + 1] >= 0
    return (left & first) | (~left & second)


def fetch(source, target, sem):
    copy = pltpu.make_async_copy(source, target, sem)
    copy.start()
    return copy


def strip_body(g, meta, data, unused_a, unused_b, out):
    left = lane_ids() < HALF
    for t in range(ITERS - 1):
        columns = (4, 2, 2)[t]
        base = (0, LAYERS[0] * 8, LAYERS[0] * 8 + 4)[t]
        for col in range(g.ct):
            mine = [jnp.maximum(meta[t, 2 * col + half], 0) for half in range(2)]
            far = [jnp.maximum(meta[t, g.blocks + 2 * col + half], 0) for half in range(2)]
            row = base + col * columns
            for zt in range(2):
                for j in range(columns // 2):
                    at = OFFSET[t] + zt * 8 * PAIRS + j * 8
                    even, odd = pair_tiles(left, *[data[owner, at : at + 8, :] for owner in mine])
                    out[pl.ds(row + zt * 64 + 2 * j, 8, stride=8), :] = even
                    out[pl.ds(row + zt * 64 + 2 * j + 1, 8, stride=8), :] = odd
            for z in range(BLOCK_Z, LAYERS[t]):
                at = OFFSET[t] + z * PAIRS
                even, odd = pair_tiles(left, *[data[owner, at : at + PAIRS, :] for owner in far])
                for j in range(columns // 2):
                    first = row + z * 8 + 2 * j
                    out[first : first + 1, :] = even[j : j + 1, :]
                    out[first + 1 : first + 2, :] = odd[j : j + 1, :]


def strip_tile(strips, t, z, col):
    tile = strips[z] if t == 0 else strips[LAYERS[0] + z]
    shift = (4 * col, 2 * col, 4 + 2 * col)[t]
    return pltpu.roll(tile, 8 - shift, 0) if shift else tile


class Stencil:
    def __init__(self, g, edge):
        self.g = g
        lane, sub = lane_ids(), sub_ids()
        self.inner = lane < LANES - S
        self.above = sub < 7
        self.last = edge & (sub == 7)

    def __call__(self, get, z, low):
        g = self.g
        sums, turned = {}, {}
        for vt in range(g.vt + 1):
            for col in range(g.ct):
                sums[col, vt] = get(col, vt, z) + get(col, vt, low)
                turned[col, vt] = pltpu.roll(sums[col, vt], LANES - S, 1)
        both, up = {}, {}
        for vt in range(g.vt + 1):
            for col in range(g.ct):
                beside = sums[col, vt] if col == g.ct - 1 else turned[col + 1, vt]
                both[col, vt] = sums[col, vt] + jnp.where(self.inner, turned[col, vt], beside)
                up[col, vt] = pltpu.roll(both[col, vt], 7, 0)
        result = {}
        for vt in range(g.vt + 1):
            for col in range(g.ct):
                value = up[col, vt]
                if vt < g.vt:
                    value = jnp.where(self.above, value, up[col, vt + 1])
                if vt == g.vt - 1:
                    value = jnp.where(self.last, both[col, vt], value)
                result[col, vt] = 0.125 * (both[col, vt] + value)
        return result


def edges(meta):
    return meta[0, 120] == 1, meta[0, 121] == 1


def layer_below(z, edge):
    return jnp.where((z == BLOCK_Z - 1) & edge, z, z + 1)


def clip(z, top):
    return jnp.minimum(jnp.maximum(z, 0), top)


def tile_rows(vt):
    return slice(vt * 8, vt * 8 + 8)


def reader(g, main, halo):
    return lambda col, vt, z: halo[col, z] if vt == g.vt else main[col, z, tile_rows(vt), :]


def put(g, main, halo, z, values):
    for (col, vt), value in values.items():
        if vt == g.vt:
            halo[col, z] = value
        else:
            main[col, z, tile_rows(vt), :] = value


def put_wide(main, z, values):
    for (col, vt), value in values.items():
        main[col, z, tile_rows(vt), :] = value


def interp_body(g, meta, table, below, strip, interp, interp_halo, nodes, nodes_halo):
    edge_z, edge_v = edges(meta)
    stencil = Stencil(g, edge_v)

    def take(source, z, target):
        for col in range(g.ct):
            lanes = slice(col * LANES, (col + 1) * LANES)
            nodes[col, target] = source[z, :, lanes]
            nodes_halo[col, target] = strip[target, :, lanes]

    @pl.loop(0, BLOCK_Z)
    def _(z):
        take(table, z, z)

    @pl.loop(0, ITERS)
    def _(z):
        take(below, z, BLOCK_Z + z)

    get = reader(g, nodes, nodes_halo)

    @pl.loop(0, LAYERS[0])
    def _(z):
        put(g, interp, interp_halo, z, stencil(get, z, layer_below(z, edge_z)))


PRODUCTS = 14


def spread_rows(values, count):
    rows = [jnp.sum(value, axis=0, keepdims=True) for value in values]
    rows += [jnp.zeros_like(rows[0])] * (-len(rows) % 8)
    column = jnp.sum(jnp.concatenate(rows, 0), axis=1, keepdims=True)
    lane = lax.broadcasted_iota(jnp.int32, (len(rows), 128), 1)
    row = lax.broadcasted_iota(jnp.int32, (len(rows), 128), 0)
    line = jnp.sum(jnp.where(lane == row, column, 0.0), axis=0, keepdims=True)
    return jnp.broadcast_to(line, (count, 128))


def fill_masks(g, meta, masks, iterations, left):
    for at, t in enumerate(iterations):
        for far in range(2):
            for pair in range(g.pairs):
                column = pair // g.ct * g.cb + pair % g.ct * 2 + far * g.blocks
                masks[at, far, pair] = jnp.where(pair_live(meta, t, column, left), 1.0, 0.0)


def halo_live(g, meta, iteration, left):
    first = 2 * g.blocks
    return [[pair_live(meta, iteration, first + far * g.cb + 2 * col, left) for col in range(g.ct)] for far in range(2)]


def segments(top, counts):
    result, high = [], top
    for count in counts:
        result.append((high - count + 1, high))
        high -= count
    return result


def fill_first_rows(g, meta, iterations, rows, first_rows):
    for t in iterations:
        for block in range(g.blocks):
            first_rows[t, block] = jnp.maximum(meta[t, block], 0) * rows + (OFFSET[t] if t < ITERS - 1 else 0)


def convert(g, first_rows, t, held, z, out, left):
    row = z // 8 * 8 * PAIRS + z % 8
    for pair in range(g.pairs):
        vb, col = pair // g.ct, pair % g.ct
        tiles = []
        for half in range(2):
            tiles.append(held[pl.ds(first_rows[t, vb * g.cb + 2 * col + half] + row, PAIRS, stride=8), :])
        even, odd = pair_tiles(left, *tiles)
        out[col, z, pl.ds(vb * BLOCK_V, PAIRS, stride=2), :] = even
        out[col, z, pl.ds(vb * BLOCK_V + 1, PAIRS, stride=2), :] = odd


def between(z):
    return jnp.where((z >= 0) & (z < BLOCK_Z), 1.0, 0.0)


def pair_tile_rows(g, pair):
    return [tile_rows(vt) for vt in (pair // g.ct * 2, pair // g.ct * 2 + 1)]


def local_body(g, meta_in, data, interp_in, a0_out, a1_out, a2_out, totals_out, peaks_out,
               meta, first_rows, totals, peaks, arrived, interp, f0, f1, f2, a0, a1, a2, masks, sems, out_sems):
    meta_copy = fetch(meta_in, meta, sems.at[8])
    held = arrived.reshape(g.zm * OFFSET[3], LANES)
    f, a, outs = (f0, f1, f2), (a0, a1, a2), (a0_out, a1_out, a2_out)
    split = BLOCK_Z // 2
    groups = ([], [])
    for t in range(3):
        first, middle, end = OFFSET[t], OFFSET[t] + ROWS // 2, OFFSET[t + 1]
        for group, rows in ((0, slice(middle, end)), (1, slice(first, middle))):
            copy = pltpu.make_async_copy(data.at[:, rows, :], arrived.at[:, rows, :], sems.at[2 * t + group])
            groups[group].append(copy)
    for group, layers in ((0, slice(split, LAYERS[0])), (1, slice(0, split))):
        groups[group].append(pltpu.make_async_copy(interp_in.at[:, layers], interp.at[:, layers], sems.at[6 + group]))
    for group in groups:
        for copy in group:
            copy.start()
    left = lane_ids() < HALF
    peaks[...] = jnp.zeros_like(peaks)
    meta_copy.wait()
    fill_first_rows(g, meta, range(3), OFFSET[3], first_rows)
    fill_masks(g, meta, masks, (0, 1, 2), left)
    for copy in groups[0]:
        copy.wait()

    for pair in range(g.pairs):
        vb, col = pair // g.ct, pair % g.ct
        row = vb * BLOCK_V
        column = g.blocks + vb * g.cb + 2 * col
        for t in range(3):
            starts = [jnp.maximum(meta[t, column + half], 0) * OFFSET[3] for half in range(2)]
            for z in range(BLOCK_Z, LAYERS[t]):
                at = [pl.multiple_of(start + OFFSET[t] + z * PAIRS, PAIRS) for start in starts]
                even, odd = pair_tiles(left, *[held[pl.ds(row_at, PAIRS), :] for row_at in at])
                f[t][col, z, pl.ds(row, PAIRS, stride=2), :] = even
                f[t][col, z, pl.ds(row + 1, PAIRS, stride=2), :] = odd
        for t in range(3):
            live = masks[t, 1, pair] > 0.5
            for z in range(BLOCK_Z, LAYERS[t]):
                for half in range(2):
                    rows = pl.ds(row + 8 * half, 8)
                    value = f[t][col, z, rows, :] - interp[col, z, rows, :]
                    a[t][col, z, rows, :] = jnp.where(live, value, 0.0)

    def step(i, carry):
        carry = list(carry)
        base = BLOCK_Z - 1 - i
        at = clip(base + 1, BLOCK_Z - 1)
        inside = jnp.full(TILE, between(base + 1), F32) > 0.5
        for pair in range(g.pairs):
            col = pair % g.ct
            peak = peaks[pair]
            for rows in pair_tile_rows(g, pair):
                mean = interp[col, at, rows, :]
                for t in range(3):
                    live = (masks[t, 0, pair] > 0.5) & inside
                    value = jnp.where(live, f[t][col, at, rows, :] - mean, 0.0)
                    a[t][col, at, rows, :] = value
                    carry[t] = carry[t] + value * value
                    if t == 0:
                        peak = jnp.maximum(peak, jnp.abs(value))
            peaks[pair] = peak
        at = clip(base, BLOCK_Z - 1)
        for t in range(3):
            convert(g, first_rows, t, held, at, f[t], left)
        return tuple(carry)

    carry = (jnp.zeros(TILE, F32),) * 3
    writes, bounds = [], (0, split, split + 4, BLOCK_Z - 1, BLOCK_Z + 1)
    for index in range(4):
        if index == 1:
            for copy in groups[1]:
                copy.wait()
        carry = lax.fori_loop(bounds[index], bounds[index + 1], step, carry)
        lowest = BLOCK_Z - bounds[index + 1] + 1
        for t in range(3):
            highest = BLOCK_Z - bounds[index] if index else LAYERS[t] - 1
            span = slice(lowest, highest + 1)
            writes.append(fetch(a[t].at[:, span], outs[t].at[:, span], out_sems.at[index * 3 + t]))
    for t in range(3):
        totals[t] = carry[t]
    writes.append(fetch(totals, totals_out, out_sems.at[12]))
    writes.append(fetch(peaks, peaks_out, out_sems.at[13]))
    for write in writes:
        write.wait()


def middle_body(g, meta_in, strips_in, interp_halo_in, totals_in, a0_in, a1_in, a2_in,
                out, ca0_out, ca1_out, cb1_out,
                meta, strips, interp_halo, totals, a0, a1, a2, b1, ca0, ca1, cb1, a0_halo, a1_halo, b1_halo, masks, sems, out_sems):
    cuts = (12, 6, 0)
    groups, at = ([], [], []), 9
    small = []
    for source, target in ((meta_in, meta), (strips_in, strips), (interp_halo_in, interp_halo), (totals_in, totals)):
        small.append(fetch(source, target, sems.at[at]))
        at += 1
    at = 0
    for source, target, layers in ((a0_in, a0, LAYERS[0]), (a1_in, a1, LAYERS[1]), (a2_in, a2, BLOCK_Z)):
        for group, span in enumerate((slice(cuts[0], layers), slice(cuts[1], cuts[0]), slice(0, cuts[1]))):
            groups[group].append(pltpu.make_async_copy(source.at[:, span], target.at[:, span], sems.at[at]))
            at += 1
    for group in groups:
        for copy in group:
            copy.start()
    none = LAYERS[0]
    for col in range(g.ct):
        for field in (a1, a2, b1):
            field[col, none] = jnp.zeros((g.span, LANES), F32)
        ca0[col, none] = jnp.zeros((g.span + 8, LANES), F32)
    for copy in small:
        copy.wait()
    edge_z, edge_v = edges(meta)
    stencil = Stencil(g, edge_v)
    left = lane_ids() < HALF
    live0, live1 = halo_live(g, meta, 0, left), halo_live(g, meta, 1, left)
    fill_masks(g, meta, masks, (1, 2), left)
    for pair in range(g.pairs):
        masks[1, 1, pair] = jnp.zeros(TILE, F32)
    for col in range(g.ct):
        for z in range(LAYERS[0]):
            value = strip_tile(strips, 0, z, col) - interp_halo[col, z]
            a0_halo[col, z] = jnp.where(live0[z >= BLOCK_Z][col], value, 0.0)
        for z in range(LAYERS[1]):
            value = strip_tile(strips, 1, z, col) - interp_halo[col, z]
            a1_halo[col, z] = jnp.where(live1[z >= BLOCK_Z][col], value, 0.0)
    get0, get1, getb = reader(g, a0, a0_halo), reader(g, a1, a1_halo), reader(g, b1, b1_halo)
    top0, top1 = LAYERS[1] - 1, LAYERS[2] - 1
    for copy in groups[0]:
        copy.wait()

    def first_stage(i, carry):
        base = top0 - i
        at = clip(base, top0)
        after = stencil(get0, at, layer_below(at, edge_z))
        put_wide(ca0, at, after)
        far = jnp.where(at >= BLOCK_Z, 1, 0)
        for (col, vt), value in after.items():
            if vt == g.vt:
                live = (live1[0][col] & (at < BLOCK_Z)) | (live1[1][col] & (at >= BLOCK_Z))
                b1_halo[col, at] = jnp.where(live, value, 0.0)
            else:
                mask = masks[0, far, vt // 2 * g.ct + col]
                b1[col, at, tile_rows(vt), :] = jnp.where(mask > 0.5, value, 0.0)
        return carry

    def second_stage(i, carry):
        carry = list(carry)
        z = top0 - i + 1
        at = clip(z, top1)
        low = layer_below(at, edge_z)
        after_a = stencil(get1, at, low)
        after_b = stencil(getb, at, low)
        put_wide(ca1, at, after_a)
        put_wide(cb1, at, after_b)
        own = (z >= 0) & (z < BLOCK_Z)
        row, kind = jnp.where(own, z, none), jnp.where(own, 0, 1)
        for pair in range(g.pairs):
            col = pair % g.ct
            live = masks[1, kind, pair] > 0.5
            for half, rows in enumerate(pair_tile_rows(g, pair)):
                vt = pair // g.ct * 2 + half
                one, two = a1[col, row, rows, :], b1[col, row, rows, :]
                carry[0] = carry[0] + one * two
                carry[1] = carry[1] + two * two
                parts = [a2[col, row, rows, :]] + [
                    jnp.where(live, value, 0.0) for value in (ca0[col, row, rows, :], after_a[col, vt], after_b[col, vt])
                ]
                slot = 2
                for m in range(4):
                    for n in range(max(m, 1), 4):
                        carry[slot] = carry[slot] + parts[m] * parts[n]
                        slot += 1
        return tuple(carry)

    def step(i, carry):
        return first_stage(i, second_stage(i, carry))

    carry = (jnp.zeros(TILE, F32),) * 11
    writes = []
    bounds = (0, top0 - cuts[0] + 1, top0 - cuts[1] + 1, top0, top0 + 2)
    for index in range(4):
        if index in (1, 2):
            for copy in groups[index]:
                copy.wait()
        start, stop = bounds[index], bounds[index + 1]
        if index == 0:
            carry = lax.fori_loop(start, start + 2, first_stage, carry)
            start += 2
        if index == 3:
            stop -= 1
        carry = lax.fori_loop(start, stop, step, carry)
        if index == 3:
            carry = second_stage(stop, carry)
        lowest = top0 - bounds[index + 1] + 2
        highest = top0 - bounds[index] + 1 if index else top1
        for which, (source, target) in enumerate(((ca0, ca0_out), (ca1, ca1_out), (cb1, cb1_out))):
            span = slice(lowest, highest + 1)
            writes.append(fetch(source.at[:, span], target.at[:, span], out_sems.at[index * 3 + which]))
    values = [totals[0], totals[1], carry[0], carry[1], totals[2]] + list(carry[2:])
    out[...] = spread_rows(values, out.shape[0])
    for write in writes:
        write.wait()


def weight_of(total, count):
    return 1.0 / (1.0 + jnp.sqrt(jnp.maximum(total, 0.0) / count))


def lane_values(line, count):
    lane = lax.broadcasted_iota(jnp.int32, line.shape, 1)
    return [jnp.sum(jnp.where(lane == i, line, 0.0), axis=1, keepdims=True) for i in range(count)]


def live_cells(g, meta, iteration):
    return jnp.full((1, 1), meta[iteration, 122], jnp.int32).astype(F32) * F32(g.cells)


def three_weights(g, meta, parts):
    q = lane_values(jnp.sum(parts[...], axis=0, keepdims=True), PRODUCTS)
    w0 = weight_of(q[0], live_cells(g, meta, 0))
    w1 = weight_of(q[1] - 2.0 * w0 * q[2] + w0 * w0 * q[3], live_cells(g, meta, 1))
    f = [jnp.ones_like(w0), -w0, -w1, w0 * w1]
    total, at = jnp.zeros_like(w0), 4
    for i in range(4):
        for j in range(i, 4):
            total = total + (1.0 if i == j else 2.0) * f[i] * f[j] * q[at]
            at += 1
    return [jnp.broadcast_to(w, TILE) for w in (w0, w1, weight_of(total, live_cells(g, meta, 2)))]


def last_body(g, meta_in, parts, strips_in, interp_halo_in, peaks0_in, a0_in, a1_in, a2_in, interp_in, ca0_in, ca1_in, cb1_in,
              *rest):
    data, rest = rest[: g.zm], rest[g.zm :]
    (sum_out, r3, errors, out,
     meta, first_rows, strips, interp_halo, peaks0, held, f3, a0, a1, a2, interp, ca0, ca1, cb1, r2, r2_halo, change, masks, peaks, sems) = rest
    top = LAYERS[2] - 1
    small = []
    for source, target in ((meta_in, meta), (strips_in, strips), (interp_halo_in, interp_halo), (peaks0_in, peaks0)):
        small.append(fetch(source, target, sems.at[g.zm + 28 + len(small)]))
    chunks = segments(top, (3, 5, 6, 3))
    reads, at = [], 0
    for lowest, highest in chunks:
        group = []
        if not reads:
            for k in range(g.zm):
                group.append(pltpu.make_async_copy(data[k], held.at[k * ROWS : (k + 1) * ROWS, :], sems.at[at]))
                at += 1
        for source, target, layers in ((ca0_in, ca0, BLOCK_Z + 1), (ca1_in, ca1, BLOCK_Z + 1), (cb1_in, cb1, BLOCK_Z + 1),
                                       (a0_in, a0, BLOCK_Z), (a1_in, a1, BLOCK_Z), (a2_in, a2, BLOCK_Z + 1),
                                       (interp_in, interp, BLOCK_Z)):
            span = slice(lowest, min(highest + 1, layers))
            group.append(pltpu.make_async_copy(source.at[:, span], target.at[:, span], sems.at[at]))
            at += 1
        reads.append(group)
    for group in reads:
        for copy in group:
            copy.start()
    peaks[...] = jnp.zeros_like(peaks)
    for copy in small:
        copy.wait()
    edge_z, edge_v = edges(meta)
    stencil = Stencil(g, edge_v)
    left = lane_ids() < HALF
    fill_masks(g, meta, masks, (1, 2, 3), left)
    fill_first_rows(g, meta, [ITERS - 1], ROWS, first_rows)
    w0, w1, w2 = three_weights(g, meta, parts)
    w01 = w0 * w1
    live = halo_live(g, meta, 2, left)
    get = reader(g, r2, r2_halo)

    def above_stage(i, total):
        base = top - i
        z = base + 1
        at = clip(z, BLOCK_Z - 1)
        counts = between(z)
        after = stencil(get, at, layer_below(at, edge_z))
        for pair in range(g.pairs):
            col = pair % g.ct
            mask = masks[2, 0, pair] * counts > 0.5
            peak = peaks[2, pair]
            for half, rows in enumerate(pair_tile_rows(g, pair)):
                value = f3[col, at, rows, :] - interp[col, at, rows, :] - change[col, at, rows, :]
                value = jnp.where(mask, value - w2 * after[col, pair // g.ct * 2 + half], 0.0)
                r3[col, at, rows, :] = value
                total = total + value * value
                peak = jnp.maximum(peak, jnp.abs(value))
            peaks[2, pair] = peak
        return total

    def layer_stage(i, total):
        base = top - i
        at = clip(base, top)
        edge = tile_rows(g.vt)
        for col in range(g.ct):
            value = strip_tile(strips, 2, at, col) - interp_halo[col, at] - w0 * ca0[col, at, edge, :]
            value = value - w1 * ca1[col, at, edge, :] + w01 * cb1[col, at, edge, :]
            there = (live[0][col] & (at < BLOCK_Z)) | (live[1][col] & (at >= BLOCK_Z))
            r2_halo[col, at] = jnp.where(there, value, 0.0)
        far = jnp.where(at >= BLOCK_Z, 1, 0)
        own = jnp.minimum(at, BLOCK_Z - 1)
        inside = jnp.full(TILE, between(at), F32) > 0.5
        for pair in range(g.pairs):
            col = pair % g.ct
            mask1, mask2 = masks[0, 0, pair] > 0.5, masks[1, far, pair] > 0.5
            peak1, peak2 = peaks[0, pair], peaks[1, pair]
            for rows in pair_tile_rows(g, pair):
                zero = w0 * ca0[col, at, rows, :]
                whole = zero + w1 * ca1[col, at, rows, :] - w01 * cb1[col, at, rows, :]
                change[col, at, rows, :] = whole
                value = a2[col, at, rows, :] - jnp.where(mask2, whole, 0.0)
                r2[col, at, rows, :] = value
                peak2 = jnp.maximum(peak2, jnp.where(inside, jnp.abs(value), 0.0))
                one = a1[col, own, rows, :] - jnp.where(mask1, zero, 0.0)
                peak1 = jnp.maximum(peak1, jnp.where(inside, jnp.abs(one), 0.0))
                sum_out[col, own, rows, :] = w0 * a0[col, own, rows, :] + w1 * one + w2 * value
            peaks[0, pair] = peak1
            peaks[1, pair] = peak2
        convert(g, first_rows, ITERS - 1, held, own, f3, left)
        return total

    def step(i, total):
        return layer_stage(i, above_stage(i, total))

    total, start = jnp.zeros(TILE, F32), 0
    for index, (lowest, highest) in enumerate(chunks):
        for copy in reads[index]:
            copy.wait()
        stop = top - lowest + 1
        if index == 0:
            total = lax.fori_loop(start, start + 2, layer_stage, total)
            start += 2
        total = lax.fori_loop(start, stop, step, total)
        start = stop
        if lowest == 0:
            total = above_stage(stop, total)

    line = spread_rows([total], 1)
    lane = lax.broadcasted_iota(jnp.int32, (1, 128), 1)
    lane_p = lax.broadcasted_iota(jnp.int32, (g.pairs, 128), 1)
    row_p = lax.broadcasted_iota(jnp.int32, (g.pairs, 128), 0)
    for i in range(ITERS):
        tiles = [peaks0[pair] if i == 0 else peaks[i - 1, pair] for pair in range(g.pairs)]
        rows = jnp.concatenate([jnp.max(tile, axis=0, keepdims=True) for tile in tiles], 0)
        found = jnp.zeros((1, 128), F32)
        for half in range(2):
            inside = lane_p // HALF == half
            column = jnp.max(jnp.where(inside, rows, 0.0), axis=1, keepdims=True)
            place = row_p // g.ct * g.cb + row_p % g.ct * 2 + half
            found = found + jnp.sum(jnp.where(lane_p == place, column, 0.0), axis=0, keepdims=True)
        errors[i : i + 1, :] = found
        line = jnp.where(lane == 1 + i, jnp.max(found, axis=1, keepdims=True), line)
    line = jnp.where(lane == 1 + ITERS, live_cells(g, meta, ITERS - 1), line)
    out[...] = jnp.broadcast_to(line, out.shape)


def finish_body(g, parts, table_in, change, r3, errors, out_hbm, worst_out, errors_out, table, out, worst, sems, out_sems):
    quarter = BLOCK_Z // 4
    spans = [slice(part * quarter, (part + 1) * quarter) for part in range(4)]
    reads = []
    for part, span in enumerate(spans):
        group = [pltpu.make_async_copy(table_in.at[span], table.at[span], sems.at[3 * part])]
        reads.append(group)
    for group in reads:
        for read in group:
            read.start()
    total = lane_values(jnp.sum(parts[...], axis=0, keepdims=True), 1)[0]
    largest = lane_values(jnp.max(parts[...], axis=0, keepdims=True), 2 + ITERS)
    w3 = jnp.broadcast_to(weight_of(total, largest[1 + ITERS]), TILE)
    for i in range(ITERS):
        worst[i] = jnp.max(largest[1 + i])
    writes = [fetch(worst, worst_out, out_sems.at[4]), fetch(errors, errors_out, out_sems.at[5])]
    for part, span in enumerate(spans):
        for read in reads[part]:
            read.wait()
        for z in range(part * quarter, (part + 1) * quarter):
            for col in range(g.ct):
                lanes = slice(col * LANES, (col + 1) * LANES)
                for vt in range(g.vt):
                    rows = tile_rows(vt)
                    out[z, rows, lanes] = table[z, rows, lanes] + (change[col, z, rows, :] + w3 * r3[col, z, rows, :])
        writes.append(pltpu.make_async_copy(out.at[span], out_hbm.at[span], out_sems.at[part]))
        writes[-1].start()
    for write in writes:
        write.wait()


def index_table(g, assign):
    zm_here, zv_here = lax.axis_index("zm"), lax.axis_index("zv")
    me = zm_here * g.zv + zv_here
    slots = assign.reshape(ITERS, -1)
    owner = jnp.arange(slots.shape[1]) // g.slots // g.zv
    owner = jnp.where(jnp.arange(ITERS)[:, None] == ITERS - 1, owner ^ zm_here, owner)
    column = jnp.arange(2 * g.blocks + 2 * g.cb)
    here = column % g.blocks
    far = jnp.where(column < 2 * g.blocks, column // g.blocks, (column - 2 * g.blocks) // g.cb)
    local = jnp.where(column < 2 * g.blocks, here, (column - 2 * g.blocks) % g.cb)
    side = jnp.where(column < 2 * g.blocks, 0, 1)
    inside = (zm_here + far < g.zm) & (zv_here + side < g.zv)
    target = jnp.where(inside, (me + far * g.zv + side) * g.blocks + local, -2)
    found = jnp.max(jnp.where(slots[:, None, :] == target[None, :, None], owner[:, None, :], -1), axis=2)
    count = jnp.sum((slots >= 0).astype(jnp.int32), axis=1, keepdims=True)
    flags = jnp.stack([zm_here == g.zm - 1, zv_here == g.zv - 1]).astype(jnp.int32)
    gap = jnp.zeros((ITERS, 120 - found.shape[1]), jnp.int32)
    flags = jnp.broadcast_to(flags[None, :], (ITERS, 2))
    return jnp.concatenate([found, gap, flags, count, jnp.zeros((ITERS, 5), jnp.int32)], axis=1)


def to_all(rows):
    count = lax.axis_size("zm") * lax.axis_size("zv")
    return lax.all_to_all(rows.reshape(count, 1, 128), AXES, 0, 0, tiled=True).reshape(count, 128)


def from_next(value, axis):
    count = lax.axis_size(axis)
    return lax.ppermute(value, axis, [(i, i - 1) for i in range(1, count)])


def shards(table, refined, assign):
    g = Shape(table.shape, assign.shape, lax.axis_size("zm"), lax.axis_size("zv"))
    everyone = g.zm * g.zv
    part = functools.partial
    slots = assign.transpose(0, 2, 1).reshape(ITERS * g.slots, -1)
    views = refined.reshape(ITERS * g.slots, BLOCK_Z // 8, 8, PAIRS, LANES).transpose(0, 1, 3, 2, 4)
    views = views.reshape(ITERS * g.slots, ROWS, LANES)
    vmem = lambda *shape: pltpu.VMEM(shape, F32)
    main, halo = g.main, g.halo

    packed, top = call(
        part(pack_three_body, g), [struct(g.zm, OFFSET[3], LANES), struct(ITERS, *table.shape[1:])], [HBM] * 3, [HBM] * 2,
        [pltpu.SMEM(slots.shape, jnp.int32), pltpu.SMEM((ITERS, g.zm), jnp.int32), vmem(3 * g.slots, ROWS, LANES), vmem(g.zm, OFFSET[3] - 3 * ROWS, LANES),
         vmem(ITERS, *table.shape[1:]), dma(5), dma(3 * g.zm + 4)],
        60,
    )(slots, views, table)
    below = from_next(top, "zm")
    data = lax.all_to_all(packed, "zm", 0, 0, tiled=True)
    strip = jnp.concatenate([table[:, :8], below[:, :8]], 0)
    strip = from_next(strip, "zv")
    packed = call(
        part(pack_last_body, g), [struct(ROWS, LANES)] * g.zm, [SMEM, HBM], [VMEM] * g.zm,
        [pltpu.SMEM((ITERS, g.zm), jnp.int32), dma(g.zm)], WHOLE,
    )(slots, views)
    last_data = [packed[0]]
    for k in range(1, g.zm):
        last_data.append(lax.ppermute(packed[k], "zm", [(i, i ^ k) for i in range(g.zm)]))
    meta = index_table(g, assign)
    interp, interp_halo = call(
        part(interp_body, g), [struct(*main(LAYERS[0])), struct(*halo(LAYERS[0]))],
        [SMEM] + [VMEM] * 3, [VMEM] * 2, [vmem(*main(DEEP)), vmem(*halo(DEEP))], PART,
    )(meta, table, below, strip)

    strips = call(
        part(strip_body, g), struct(sum(LAYERS[:2]) * 8, LANES), [SMEM, VMEM, HBM, HBM], VMEM,
        [],
        PART,
    )(meta, data, interp_halo, packed[0])
    strips = from_next(strips, "zv").reshape(sum(LAYERS[:2]), *TILE)
    own, more, most = struct(*main(BLOCK_Z)), struct(*main(LAYERS[2])), struct(*main(LAYERS[1]))
    a0, a1, a2, totals, peaks0 = call(
        part(local_body, g), [struct(*main(LAYERS[0])), most, more, struct(3, *TILE), struct(g.pairs, *TILE)],
        [HBM] * 3, [HBM] * 5,
        [pltpu.SMEM(meta.shape, jnp.int32), pltpu.SMEM((ITERS, g.blocks), jnp.int32), vmem(3, *TILE),
         vmem(g.pairs, *TILE), vmem(*data.shape)]
        + [vmem(*main(LAYERS[0]))] * 7
        + [vmem(3, 2, g.pairs, *TILE), dma(9), dma(14)], WHOLE,
    )(meta, data, interp)
    wide = struct(*g.wide_main(LAYERS[2]))
    products, ca0, ca1, cb1 = call(
        part(middle_body, g), [struct(everyone, 128), wide, wide, wide],
        [HBM] * 7, [VMEM] + [HBM] * 3,
        [pltpu.SMEM(meta.shape, jnp.int32), vmem(*strips.shape), vmem(*interp_halo.shape), vmem(3, *TILE)]
        + [vmem(*main(LAYERS[0] + 1))] * 4 + [vmem(*g.wide_main(LAYERS[0] + 1))] * 3 + [vmem(*halo(LAYERS[0] + 1))] * 3
        + [vmem(2, 2, g.pairs, *TILE), dma(13), dma(13)],
        WHOLE,
    )(meta, strips, interp_halo, totals, a0, a1, a2)
    products, *last_data = lax.optimization_barrier((products, *last_data))
    products = to_all(products)
    change, r3, errors, stats = call(
        part(last_body, g), [own, own, struct(ITERS, 128), struct(everyone, 128)],
        [HBM, VMEM] + [HBM] * (10 + g.zm), [VMEM] * 4,
        [pltpu.SMEM(meta.shape, jnp.int32), pltpu.SMEM((ITERS, g.blocks), jnp.int32), vmem(*strips.shape),
         vmem(*interp_halo.shape), vmem(*peaks0.shape), vmem(g.zm * ROWS, LANES)] + [vmem(*main(BLOCK_Z))] * 3 + [vmem(*main(LAYERS[2])), vmem(*main(BLOCK_Z))]
        + [vmem(*g.wide_main(LAYERS[2]))] * 3 + [vmem(*main(LAYERS[2])), vmem(*halo(LAYERS[2])), vmem(*main(LAYERS[2]))]
        + [vmem(3, 2, g.pairs, *TILE), vmem(3, g.pairs, *TILE), dma(g.zm + 33)],
        50.5,
    )(meta, products, strips, interp_halo, peaks0, a0, a1, a2, interp, ca0, ca1, cb1, *last_data)
    stats = to_all(stats)
    table_out, worst, errors = call(
        part(finish_body, g), [struct(*table.shape), struct(ITERS), struct(ITERS, 128)], [VMEM, HBM] + [VMEM] * 3, [HBM] * 3,
        [vmem(*table.shape), vmem(*table.shape), pltpu.SMEM((ITERS,), F32), dma(12), dma(6)],
        30,
    )(stats, table, change, r3, errors)
    return (table_out, errors[:, : g.blocks], worst)


def solution(mesh):
    in_specs = (P("zm", "zv", None), P(None, ("zm", "zv"), None, None), P())
    out_specs = (P("zm", "zv", None), P(None, ("zm", "zv")), P())

    return jax.shard_map(shards, mesh=mesh, in_specs=in_specs, out_specs=out_specs, check_vma=False)
```
